32 devices in a mesh: shot: 8 (over z, y), grp: 4 (over x, core).
Axes of the slice: x: 2, y: 2, z: 4, core: 2. Of those that a mesh axis runs over, the one named last changes fastest.
Arguments:
- offsets: bfloat16 [6144, 32, 512], P(('shot', 'grp')), may hold values from -500 to 500
- slant_weights: bfloat16 [64, 32], replicated, may hold values from -1 to 1
- live: int32 [6144, 64], P(('shot', 'grp')), may hold values from 0 to 1, as said below
- block_tile: int32 [3072, 1], P(('shot', 'grp')), may hold values from 0 to 7; in each aligned block of 96 rows (0 to 95, 96 to 191, ...) at most 13 rows name the same one
- image_slot: int32 [3072], P(('shot', 'grp')), may hold values from 0 to 15
Outputs:
- image: bfloat16 [128, 128, 512], P(('shot', 'grp'))
The draws below stay inside these ranges and needn't reach their ends.
Inputs may be any that keep to these rules, and one draw needn't show every extreme that they name: Each position's live angles are 0 up to a cutoff minus 1, the cutoff at least 16; the first position of every 192 positions keeps all 64 angles. `block_tile`: among the 96 blocks of one device no tile is named more than 13 times.
All inputs are finite; a program needn't handle non-finite values.
Results may differ from the reference program's by a relative error of at most 0.0049.
Values may be sent and summed in bfloat16 or wider, within the bound.
A program may use at most 192 MiB of HBM per device.

```python
import math
import jax
import jax.numpy as jnp
import numpy as np
from jax import lax

ANG = 64
H = 32
Z = 512
TRB = 128
BLK_DEV = 96
IMG_DEV = 4
CAP = 13
POS_DEV = 192
POSITIONS = 6144
BLOCKS = 3072
IT = 16
IMAGE_BLOCKS = 128
N_SHOT = 8
N_GRP = 4
DEVICES = 32


def draw_offsets(key, part):
    keys = jax.random.split(jax.random.fold_in(key, 11), 3)
    row_scale = jnp.exp(jax.random.uniform(keys[1], (POSITIONS, 1, 1), jnp.float32) * jnp.log(10.0))
    depth_scale = jnp.exp(jax.random.uniform(keys[2], (1, 1, Z), jnp.float32) * jnp.log(10.0))
    place = jnp.arange(POSITIONS, dtype=jnp.float32) / max(POSITIONS - 1, 1)
    base = jnp.clip(jax.random.normal(keys[0], (POSITIONS, H, Z), jnp.float32), -6.0, 6.0)
    ramp = 1.0 + 2.0 * place
    values = 0.1 * base * row_scale * depth_scale * ramp[:, None, None]
    return values.astype(jnp.bfloat16)


def draw_live(key, part):
    cutoff = jax.random.randint(jax.random.fold_in(key, 23), (POSITIONS,), ANG // 4, ANG + 1)
    first = jnp.arange(POSITIONS) % POS_DEV == 0
    cutoff = jnp.where(first, ANG, cutoff)
    return (jnp.arange(ANG)[None, :] < cutoff[:, None]).astype(jnp.int32)


def place_ends(drawn, key, low, top_value):
    spot = [jax.random.randint(jax.random.fold_in(key, axis), (), 0, length) for axis, length in enumerate(drawn.shape)]
    longest = drawn.shape.index(max(drawn.shape))
    next_to = spot[:longest] + [(spot[longest] + 1) % drawn.shape[longest]] + spot[longest + 1:]
    return drawn.at[tuple(spot)].set(low).at[tuple(next_to)].set(top_value)


def deal_out(key, own, number, rows, number_of, top, most, lean):
    order = jax.random.permutation(key, number_of)
    crowded, usual = shares(number_of, rows * top, most, lean, True), shares(number_of, rows * top, most, lean, False)
    places = jnp.arange(number_of)

    def named(lengths, rotation):
        used = int((lengths > 0).sum())
        fixed = max(1, used // 4)
        moved = fixed + (places - fixed + rotation * (used - fixed)) % max(1, number_of - fixed)
        return jnp.zeros((number_of,), jnp.int32).at[order[jnp.where(places < fixed, places, moved)]].set(jnp.asarray(lengths, jnp.int32))

    lengths = jnp.where(number % 4 == 0, named(crowded, number // 4), named(usual, number - number // 4 - 1))
    mixed = jax.random.permutation(jax.random.fold_in(own, 3), number_of)
    giver, receiver = mixed[0:number_of // 2 * 2:2], mixed[1:number_of // 2 * 2:2]
    margin = jnp.minimum(lengths[giver] - 1, most - lengths[receiver]) // 2
    margin = jnp.where((giver == order[0]) | (receiver == order[0]) | (lengths[receiver] == 0), 0, jnp.maximum(margin, 0))
    moved = jax.random.randint(jax.random.fold_in(own, 4), (number_of // 2,), 0, 1 << 20) % (margin + 1)
    lengths = lengths.at[giver].add(-moved).at[receiver].add(moved)
    labels = jnp.searchsorted(jnp.cumsum(lengths), jnp.arange(rows * top), side="right").astype(jnp.int32)
    table = labels.reshape(top, rows).T
    table = table[jax.random.permutation(jax.random.fold_in(own, 1), rows)]
    rotation = jax.random.randint(jax.random.fold_in(own, 2), (rows, 1), 0, top)
    return jnp.take_along_axis(table, (jnp.arange(top)[None, :] + rotation) % top, axis=1)


def shares(number_of, total, reach, lean, full):
    weights = [(1 << 20) // math.isqrt(standing ** lean) + 1 for standing in range(1, number_of + 1)]
    largest = reach if full else min(reach, max(-(-total // number_of), total * weights[0] // sum(weights)))
    least = 1 if total - largest >= number_of - 1 else 0
    counts, spare = [largest] + [least] * (number_of - 1), total - largest - least * (number_of - 1)
    while spare > 0:
        movable = [i for i in range(1, number_of) if counts[i] < largest] or [i for i in range(1, number_of) if counts[i] < reach]
        mass, budget = sum([weights[i] for i in movable]), spare
        for i in movable:
            more = min(reach - counts[i], max(1, budget * weights[i] // mass), spare)
            counts[i] = counts[i] + more
            spare = spare - more
    return np.array(counts)


def noise(rng, shape, width, most, kind=jnp.bfloat16):
    return jnp.clip(width * jax.random.normal(rng, shape, jnp.float32), -most, most).astype(kind)


def setup_inputs(seed: int = 0) -> dict:
    key_list = jax.random.split(jax.random.key(seed), 6)
    offsets = draw_offsets(jax.random.fold_in(key_list[5], 71), 0)
    slant_weights = noise(key_list[1], (ANG, H), H ** -0.5, 1.0)
    live = draw_live(jax.random.fold_in(key_list[5], 71), 0)
    block_tile_keys = jax.random.split(jax.random.fold_in(key_list[3], 1), BLOCKS // BLK_DEV)
    block_tile_turns = jax.random.permutation(jax.random.fold_in(key_list[3], 3), BLOCKS // BLK_DEV)
    block_tile = jax.vmap(lambda own, number: deal_out(jax.random.fold_in(key_list[3], 2), own, number, BLK_DEV, N_SHOT, 1, CAP, 1))(block_tile_keys, block_tile_turns).reshape((BLOCKS, 1))
    image_slot = place_ends(jax.random.randint(key_list[4], (BLOCKS,), 0, IT), jax.random.fold_in(key_list[4], 1), 0, IT - 1).astype(jnp.int32)
    return {"offsets": offsets, "slant_weights": slant_weights, "live": live, "block_tile": block_tile, "image_slot": image_slot}


def reference(offsets, slant_weights, live, block_tile, image_slot):
    tile_rows = IMG_DEV * N_GRP
    weights = slant_weights.astype(jnp.float32)
    shards = (offsets.reshape(DEVICES, POS_DEV, H, Z), live.reshape(DEVICES, POS_DEV, ANG), block_tile.reshape(DEVICES, BLK_DEV), image_slot.reshape(DEVICES, BLK_DEV))

    def advance(state_in, pieces):
        stacked, square_sum, live_count = state_in
        shard_off, shard_live, shard_tile, shard_slot = pieces
        live_mask = shard_live.astype(jnp.float32)
        slanted = jnp.einsum('ah,phz->paz', weights, shard_off.astype(jnp.float32))
        angles = (slanted * live_mask[:, :, None]).astype(jnp.bfloat16)
        widened = angles.astype(jnp.float32)
        square_sum = square_sum + lax.optimization_barrier(jnp.sum(widened * widened, axis=(0, 2)))
        live_count = live_count + lax.optimization_barrier(jnp.sum(live_mask, axis=0))
        targets = (shard_tile.astype(jnp.int32) * tile_rows + shard_slot.astype(jnp.int32)).astype(jnp.int32)
        stacked = stacked.at[targets].add(widened.reshape(BLK_DEV, TRB, Z))
        return ((stacked, square_sum, live_count), None)
    initial = (jnp.zeros((IMAGE_BLOCKS, TRB, Z), jnp.float32), jnp.zeros((ANG,), jnp.float32), jnp.zeros((ANG,), jnp.float32))
    (stacked, square_sum, live_count), unused = lax.scan(advance, initial, shards)
    angle_gain = lax.rsqrt(square_sum / (Z * live_count) + 1e-06)
    trace_gain = jnp.tile(angle_gain, 2)
    return (stacked * trace_gain[None, :, None]).astype(jnp.bfloat16)
```

```python
import functools
import math

import jax
import jax.numpy as jnp
from jax import lax
from jax.experimental import pallas as pl
from jax.experimental.pallas import tpu as pltpu
from jax.sharding import PartitionSpec as P

IMG_DEV = 4
PAIR = 2
LANES = 128
UNROLL = 8
MESH = pl.DeviceIdType.MESH
VMEM_LIMIT = 62 * 1024 * 1024


def place(grp):
    shot, g = lax.axis_index("shot"), lax.axis_index("grp")
    return lax.div(shot, PAIR), lax.rem(shot, PAIR) * grp + g


def at(plane, spot, grp):
    return (plane * PAIR + lax.div(spot, grp), lax.rem(spot, grp))


def share(spot, width, depth):
    start = spot * width
    return lax.div(start, depth), pl.multiple_of(lax.rem(start, depth), LANES)


def relative(spot, grp, r):
    mid = grp // 2
    pair, rest = lax.div(spot, grp), lax.rem(spot, grp)
    m, c = lax.div(rest, 2), lax.rem(rest, 2)
    rp, rm, rc = r // grp, (r % grp) // 2, r % 2
    pair, m, c = lax.rem(pair + rp, PAIR), lax.rem(m + rm, mid), lax.rem(c + rc, 2)
    return (pair * mid + m) * 2 + c


def orders(grp):
    size = PAIR * grp
    far = list(range(grp + 2, size))
    side = list(range(grp, grp + 2))
    ahead = list(range(2, grp))
    turn = []
    for i in range(max(len(far), len(ahead))):
        for group in (far, side, ahead):
            turn += group[i : i + 1]
    return [1] + turn


def exchange_kernel(
    grp, off, aux, w_in, part, mom, w, raw, aux_in, codes, acc, seg, send, recv, asend, arecv, lsem
):
    size = PAIR * grp
    plane, spot = place(grp)
    blocks, depth, width = off.shape[0], off.shape[3], raw.shape[3]
    angles, images = w.shape[1], acc.shape[0]
    j, first = share(spot, width, depth)
    mine = pltpu.make_async_copy(off.at[:, j, :, pl.ds(first, width)], raw.at[0], lsem.at[0])
    mine.start()
    own_codes = pltpu.make_async_copy(aux, codes.at[0], lsem.at[1])
    own_codes.start()
    weigh = pltpu.make_async_copy(w_in, w, lsem.at[size + 1])
    weigh.start()
    barrier = pltpu.get_barrier_semaphore()
    for r in range(1, size):
        pl.semaphore_signal(
            barrier, inc=1, device_id=at(plane, relative(spot, grp, r), grp), device_id_type=MESH
        )
    pl.semaphore_wait(barrier, size - 1)
    data, notes = {}, {}
    for r in orders(grp):
        peer = relative(spot, grp, r)
        pj, pfirst = share(peer, width, depth)
        dev = at(plane, peer, grp)
        notes[r] = pltpu.make_async_remote_copy(
            src_ref=aux,
            dst_ref=aux_in.at[r],
            send_sem=asend.at[r - 1],
            recv_sem=arecv.at[r - 1],
            device_id=dev,
            device_id_type=MESH,
        )
        data[r] = pltpu.make_async_remote_copy(
            src_ref=off.at[:, pj, :, pl.ds(pfirst, width)],
            dst_ref=raw.at[r],
            send_sem=send.at[r - 1],
            recv_sem=recv.at[r - 1],
            device_id=dev,
            device_id_type=MESH,
        )
    for r in orders(grp):
        notes[r].start()
    for r in orders(grp):
        data[r].start()

    acc[...] = jnp.zeros_like(acc)
    seg[blocks] = jnp.zeros((angles, width), jnp.float32)
    row = lax.broadcasted_iota(jnp.int32, (angles, width), 0)
    weigh.wait()
    weights = w[...].astype(jnp.float32).T.astype(jnp.bfloat16)
    square = jnp.zeros((angles, width), jnp.float32)
    count = jnp.zeros((angles, width), jnp.float32)
    for r in [0] + orders(grp):
        if r:
            notes[r].wait()
            code = pltpu.make_async_copy(aux_in.at[r], codes.at[r], lsem.at[r + 1])
            code.start()
            code.wait()
            data[r].wait()
        else:
            own_codes.wait()
            mine.wait()

        def slant(i, carry, r=r):
            square, count = carry
            start = i * UNROLL
            x = jnp.concatenate([raw[r, start + t] for t in range(UNROLL)], axis=1)
            y = jnp.dot(weights, x, preferred_element_type=jnp.float32)
            for t in range(UNROLL):
                alive = row < codes[r, 1 + j, start + t]
                slanted = jnp.where(alive, y[:, t * width : (t + 1) * width], 0.0)
                slanted = slanted.astype(jnp.bfloat16).astype(jnp.float32)
                square += slanted * slanted
                count += jnp.where(alive, 1.0, 0.0)
                seg[start + t] = slanted + seg[codes[r, 0, start + t]]
            return square, count

        square, count = lax.fori_loop(0, blocks // UNROLL, slant, (square, count))

        def stack(i, _, r=r):
            start = i * UNROLL
            line, column = lax.div(start, LANES), lax.rem(start, LANES)
            for t in range(UNROLL):
                acc[start + t] += seg[codes[r, 3 + line, column + t]]
            return 0

        lax.fori_loop(0, images // UNROLL, stack, 0)

    def narrow(i, _):
        start = pl.multiple_of(i * UNROLL, UNROLL)
        part[pl.ds(start, UNROLL)] = acc[pl.ds(start, UNROLL)].astype(jnp.bfloat16)
        return 0

    lax.fori_loop(0, images // UNROLL, narrow, 0)
    lane = lax.broadcasted_iota(jnp.int32, (angles, LANES), 1)
    square = jnp.sum(square, axis=1, keepdims=True)
    count = jnp.sum(count, axis=1, keepdims=True)
    both = jnp.where(lane == 0, square, jnp.where(lane == 1, count, 0.0))
    both = jnp.concatenate([both, jnp.zeros((LANES - angles, LANES), jnp.float32)], axis=0)
    mom[...] = both.T[: mom.shape[0]]


def gather_kernel(
    grp, part, mom, out, held, total, fin, pin, qin, half_sum, zs, zr, ps, pr, qs, qr, fs, fr, lsem
):
    size = PAIR * grp
    planes = held.shape[1] + 1
    plane, spot = place(grp)
    pieces, rows, angles, width = held.shape[2:]
    depth = out.shape[2]
    chunk = pieces * rows
    lower = jnp.where(plane < planes // 2, 1, 0)
    barrier = pltpu.get_barrier_semaphore()
    for r in range(1, size):
        pl.semaphore_signal(
            barrier, inc=1, device_id=at(plane, lax.rem(spot + r, size), grp), device_id_type=MESH
        )
    for r in range(1, planes):
        pl.semaphore_signal(
            barrier, inc=1, device_id=at(lax.rem(plane + r, planes), spot, grp), device_id_type=MESH
        )
    pl.semaphore_wait(barrier, size + planes - 2)

    def along(up):
        spot_on_line = plane * up + (planes - 1 - plane) * (1 - up)
        following = lax.rem(plane + 2 * up - 1 + planes, planes)
        return 1 - up, spot_on_line, following

    def rows_of(up, s, h):
        target = (planes - 1 - s) * up + s * (1 - up)
        return target * chunk + h * rows

    def hop(up, s, h, source):
        way, _, following = along(up)
        return pltpu.make_async_remote_copy(
            src_ref=source,
            dst_ref=held.at[way, s, h],
            send_sem=zs.at[way, s, h],
            recv_sem=zr.at[way, s, h],
            device_id=at(following, spot, grp),
            device_id_type=MESH,
        )

    def begin(s):
        @pl.when(along(lower)[1] == 0)
        def _():
            for h in range(pieces):
                hop(lower, s, h, part.at[pl.ds(rows_of(lower, s, h), rows)]).start()

    def step(up, s, h):
        way, here, _ = along(up)
        end = planes - 1 - s

        @pl.when((here > 0) & (here <= end))
        def _():
            hop(up, s, h, held.at[way, s, h]).wait_recv()

        @pl.when((here > 0) & (here < end))
        def _():
            start = rows_of(up, s, h)

            def add(i, _):
                value = held[way, s, h, i].astype(jnp.float32) + part[start + i].astype(jnp.float32)
                held[way, s, h, i] = value.astype(jnp.bfloat16)
                return 0

            lax.fori_loop(0, rows, add, 0)
            hop(up, s, h, held.at[way, s, h]).start()

        @pl.when((here > 0) & (here == end))
        def _():
            def add(i, _):
                total[h * rows + i] += held[way, s, h, i].astype(jnp.float32)
                return 0

            lax.fori_loop(0, rows, add, 0)

    def finish(up, s, h):
        way, here, _ = along(up)

        @pl.when(here < planes - 1 - s)
        def _():
            hop(up, s, h, held.at[way, s, h]).wait_send()

    near = [
        pltpu.make_async_remote_copy(
            src_ref=mom,
            dst_ref=pin.at[r - 1],
            send_sem=ps.at[r - 1],
            recv_sem=pr.at[r - 1],
            device_id=at(plane, lax.rem(spot + r, size), grp),
            device_id_type=MESH,
        )
        for r in range(1, size)
    ]
    for copy in near:
        copy.start()
    begin(0)
    total[...] = part[pl.ds(plane * chunk, chunk)].astype(jnp.float32)
    moments = mom[...]
    for copy in near:
        copy.wait()
    for r in range(1, size):
        moments += pin[r - 1]
    half_sum[...] = moments
    wide = [
        pltpu.make_async_remote_copy(
            src_ref=half_sum,
            dst_ref=qin.at[r - 1],
            send_sem=qs.at[r - 1],
            recv_sem=qr.at[r - 1],
            device_id=at(lax.rem(plane + r, planes), spot, grp),
            device_id_type=MESH,
        )
        for r in range(1, planes)
    ]
    for copy in wide:
        copy.start()
    for s in range(1, planes - 1):
        begin(s)
    for s in range(planes - 1):
        for up in (lower, 1 - lower):
            for h in range(pieces):
                step(up, s, h)
    for copy in wide:
        copy.wait()
    moments = half_sum[...]
    for r in range(1, planes):
        moments += qin[r - 1]
    gain = lax.rsqrt(moments[0:1] / moments[1:2] + 1e-06)
    gain = jnp.broadcast_to(gain, (LANES, LANES)).T[:angles]

    def body(i, _):
        fin[i] = (total[i] * gain).astype(jnp.bfloat16)
        return 0

    lax.fori_loop(0, chunk, body, 0)

    each = chunk // size
    j, first = share(spot, width, depth)
    view = out.at[:, pl.ds(pl.multiple_of(j * angles, angles), angles), pl.ds(first, width)]
    last = pltpu.make_async_copy(fin.at[pl.ds(spot * each, each)], view, lsem.at[1])
    final = []
    for r in range(1, size):
        peer = lax.rem(spot + r, size)
        final.append(
            pltpu.make_async_remote_copy(
                src_ref=fin.at[pl.ds(peer * each, each)],
                dst_ref=view,
                send_sem=fs.at[r - 1],
                recv_sem=fr.at[r - 1],
                device_id=at(plane, peer, grp),
                device_id_type=MESH,
            )
        )
    for copy in final:
        copy.start()
    last.start()
    last.wait()
    for copy in final:
        copy.wait()
    for s in range(planes - 1):
        for up in (lower, 1 - lower):
            for h in range(pieces):
                finish(up, s, h)


def staged(offsets, slant_weights, live, block_tile, image_slot):
    shots, grp = lax.axis_size("shot"), lax.axis_size("grp")
    planes, size = shots // PAIR, PAIR * grp
    blocks = block_tile.shape[0]
    hs, depth = offsets.shape[1:]
    angles = slant_weights.shape[0]
    width = 2 * depth // size
    tile_rows = IMG_DEV * grp
    images = shots * tile_rows
    per_plane = images // planes
    any_space = pl.BlockSpec(memory_space=pl.ANY)
    vmem = pl.BlockSpec(memory_space=pltpu.VMEM)
    dma = pltpu.SemaphoreType.DMA

    cutoff = jnp.sum(live.reshape(blocks, 2, angles), axis=2)
    image = block_tile[:, 0] * tile_rows + image_slot
    index = jnp.arange(blocks, dtype=jnp.int32)
    same = (image[:, None] == image[None, :]) & (index[None, :] < index[:, None])
    before = jnp.max(jnp.where(same, index[None, :], -1), axis=1)
    found = image[None, :] == jnp.arange(images, dtype=jnp.int32)[:, None]
    final = jnp.max(jnp.where(found, index[None, :], -1), axis=1)
    final = jnp.where(final < 0, blocks, final).reshape(images // LANES, LANES)
    before = jnp.where(before < 0, blocks, before)
    aux = jnp.concatenate([before[None], cutoff.T], axis=0)
    aux = jnp.concatenate([jnp.pad(aux, ((0, 0), (0, LANES - blocks))), final], axis=0)
    aux = jnp.pad(aux, ((0, -aux.shape[0] % 8), (0, 0)))

    part, mom = pl.pallas_call(
        functools.partial(exchange_kernel, grp),
        out_shape=(
            jax.ShapeDtypeStruct((images, angles, width), jnp.bfloat16),
            jax.ShapeDtypeStruct((8, LANES), jnp.float32),
        ),
        in_specs=[any_space, vmem, any_space],
        out_specs=(vmem, vmem),
        scratch_shapes=[
            pltpu.VMEM((hs, angles), jnp.bfloat16),
            pltpu.VMEM((size, blocks, hs, width), jnp.bfloat16),
            pltpu.VMEM((size,) + aux.shape, jnp.int32),
            pltpu.SMEM((size,) + aux.shape, jnp.int32),
            pltpu.VMEM((images, angles, width), jnp.float32),
            pltpu.VMEM((blocks + 1, angles, width), jnp.float32),
            dma((size - 1,)),
            dma((size - 1,)),
            dma((size - 1,)),
            dma((size - 1,)),
            dma((size + 2,)),
        ],
        compiler_params=pltpu.CompilerParams(
            collective_id=0, has_side_effects=True, vmem_limit_bytes=62 * 1024 * 1024
        ),
        name="exchange",
    )(offsets.reshape(blocks, 2, hs, depth), aux, slant_weights.T)

    moments = (8, LANES)
    pieces = 4
    lines = (2, planes - 1, pieces)
    return pl.pallas_call(
        functools.partial(gather_kernel, grp),
        out_shape=jax.ShapeDtypeStruct((IMG_DEV, 2 * angles, depth), jnp.bfloat16),
        in_specs=[vmem, vmem],
        out_specs=any_space,
        scratch_shapes=[
            pltpu.VMEM(lines + (per_plane // pieces, angles, width), jnp.bfloat16),
            pltpu.VMEM((per_plane, angles, width), jnp.float32),
            pltpu.VMEM((per_plane, angles, width), jnp.bfloat16),
            pltpu.VMEM((size - 1,) + moments, jnp.float32),
            pltpu.VMEM((planes - 1,) + moments, jnp.float32),
            pltpu.VMEM(moments, jnp.float32),
            dma(lines),
            dma(lines),
            dma((size - 1,)),
            dma((size - 1,)),
            dma((planes - 1,)),
            dma((planes - 1,)),
            dma((size - 1,)),
            dma((size - 1,)),
            dma((2,)),
        ],
        compiler_params=pltpu.CompilerParams(
            collective_id=1, has_side_effects=True, vmem_limit_bytes=60 * 1024 * 1024
        ),
        name="gather",
    )(part, mom)


def round_up(value, unit):
    return -(-value // unit) * unit


def flip(value, bit):
    return value + bit - 2 * value * bit


def fused_kernel(
    shape, off, live, tile, slot, w_in, out,
    raw, wb, onehot, mine, theirs, cuts, squares, sl, own, part, rx1, rxv, held, ft, fin,
    mom, sums, pin, gains,
    in_sem, core_s, core_r, meta_s, meta_r, s1s, s1r, vs, vr, zs, zr, fs, fr, fl, ms, mr,
):
    planes, grp, kinds = shape
    shot, g = lax.axis_index("shot"), lax.axis_index("grp")
    z, y = lax.div(shot, PAIR), lax.rem(shot, PAIR)
    x, c = lax.div(g, 2), lax.rem(g, 2)
    blocks, hs, depth = raw.shape[1:]
    angles = live.shape[0]
    images = onehot.shape[0]
    img_dev = out.shape[0]
    wide = sl.shape[2]
    quarters = wide // LANES
    half = sl.shape[0]
    per = part.shape[3] * 2
    pairs = per // 2
    depths = depth // wide
    halves = angles // half
    units = half // per
    eight = 8

    def device(dz=None, fy=False, fx=False, fc=False):
        zz = z if dz is None else dz
        yy = 1 - y if fy else y
        xx = 1 - x if fx else x
        cc = 1 - c if fc else c
        return (zz * PAIR + yy, xx * 2 + cc)

    core_peer, x_peer, y_peer = device(fc=True), device(fx=True), device(fy=True)
    first_peer = (x_peer, y_peer)
    second_peer = (y_peer, x_peer)

    own_in = [
        pltpu.make_async_copy(
            off.at[:, c, :, pl.ds(d * wide, wide)],
            raw.at[0, :, :, pl.ds(d * wide, wide)],
            in_sem.at[d],
        )
        for d in range(depths)
    ]
    for copy in own_in:
        copy.start()
    barrier = pltpu.get_barrier_semaphore()
    near = [core_peer, x_peer, y_peer]
    near += [device(dz=lax.rem(z + r, planes)) for r in range(1, planes)]
    for peer in near:
        pl.semaphore_signal(barrier, inc=1, device_id=peer, device_id_type=MESH)

    count_rows = live[...].astype(jnp.float32)
    live_bf = count_rows.astype(jnp.bfloat16)
    ones = jnp.ones((angles, LANES), jnp.bfloat16)
    spot = lax.broadcasted_iota(jnp.int32, (blocks, 2 * blocks), 1)
    block = lax.broadcasted_iota(jnp.int32, (blocks, 2 * blocks), 0)

    def cutoff(j):
        pick = jnp.where(spot == 2 * block + j, 1.0, 0.0).astype(jnp.bfloat16)
        flags = lax.dot_general(
            pick, live_bf, (((1,), (1,)), ((), ())), preferred_element_type=jnp.float32
        )
        total = jnp.dot(flags.astype(jnp.bfloat16), ones, preferred_element_type=jnp.float32)
        return total.astype(jnp.int32)

    image = tile[...] * (img_dev * grp) + slot[...]
    mine[0:eight] = jnp.full((eight, LANES), -1, jnp.int32)
    mine[0:1, 0:blocks] = image
    mine[eight : eight + blocks] = cutoff(1 - c)
    cuts[0] = cutoff(c)

    pl.semaphore_wait(barrier, len(near))
    meta = pltpu.make_async_remote_copy(
        src_ref=mine, dst_ref=theirs, send_sem=meta_s.at[0], recv_sem=meta_r.at[0],
        device_id=core_peer, device_id_type=MESH,
    )
    core_in = [
        pltpu.make_async_remote_copy(
            src_ref=off.at[:, 1 - c, :, pl.ds(d * wide, wide)],
            dst_ref=raw.at[1, :, :, pl.ds(d * wide, wide)],
            send_sem=core_s.at[d], recv_sem=core_r.at[d],
            device_id=core_peer, device_id_type=MESH,
        )
        for d in range(depths)
    ]
    core_in[0].start()
    meta.start()
    for copy in core_in[1:]:
        copy.start()

    rows = angles * eight
    spread = lax.broadcasted_iota(jnp.int32, (rows, angles), 0)
    which = lax.broadcasted_iota(jnp.int32, (rows, angles), 1)
    pick = jnp.where(lax.div(spread, eight) == which, 1.0, 0.0).astype(jnp.bfloat16)
    tall = lax.dot_general(
        pick, w_in[...], (((1,), (1,)), ((), ())), preferred_element_type=jnp.float32
    ).astype(jnp.bfloat16)
    line = lax.broadcasted_iota(jnp.int32, (hs, eight * hs), 0)
    column = lax.broadcasted_iota(jnp.int32, (hs, eight * hs), 1)
    copies = jnp.where(lax.rem(column, hs) == line, 1.0, 0.0).astype(jnp.bfloat16)
    full = jnp.dot(tall, copies, preferred_element_type=jnp.float32)
    line = lax.broadcasted_iota(jnp.int32, full.shape, 0)
    column = lax.broadcasted_iota(jnp.int32, full.shape, 1)
    wb[...] = jnp.where(lax.rem(line, eight) == lax.div(column, hs), full, 0.0).astype(jnp.bfloat16)
    squares[...] = jnp.zeros_like(squares)

    def slant(d, h, r):
        def body(i, _):
            start = i * 2 * eight
            lhs = wb[h * half * eight : (h + 1) * half * eight]
            lanes = slice(d * wide, (d + 1) * wide)
            alive = cuts[r, pl.ds(start, 2 * eight)]
            a = lax.broadcasted_iota(jnp.int32, (half, 2 * eight, LANES), 0) + h * half
            alive = alive[None] > a
            ys = []
            for k in range(2):
                data = raw[r, pl.ds(start + k * eight, eight), :, lanes].reshape(eight * hs, wide)
                ys.append(
                    jnp.dot(lhs, data, preferred_element_type=jnp.float32).reshape(half, eight, wide)
                )
            total = squares[h * half : (h + 1) * half]
            for k in range(quarters):
                cut = slice(k * LANES, (k + 1) * LANES)
                v = jnp.concatenate([ys[0][:, :, cut], ys[1][:, :, cut]], axis=1)
                v = jnp.where(alive, v, 0.0)
                q = v * v
                total += q[:, :eight] + q[:, eight:]
                sl[:, pl.ds(r * blocks + start, 2 * eight), cut] = v.astype(jnp.bfloat16)
            squares[h * half : (h + 1) * half] = total
            return 0

        lax.fori_loop(0, blocks // (2 * eight), body, 0)

    def stack(cu):
        base = cu % units * per

        def body(m, _):
            ys = [
                jnp.dot(onehot[...], sl[base + 2 * m + k], preferred_element_type=jnp.float32)
                for k in range(2)
            ]
            for l in range(2):
                p = 2 * cu + l
                cut = slice(l * LANES, (l + 1) * LANES)
                for t in range(planes):
                    for ry in range(2):
                        for rx in range(2):
                            r = ((t * 2 + ry) * 2 + rx) * eight
                            v = jnp.concatenate([ys[k][r : r + eight, cut] for k in range(2)], axis=0)
                            one, two = (rx, ry) if l == 0 else (ry, rx)
                            if one == 0:
                                own[p, t, two, m] = v
                            else:
                                part[p, t, two, m] = v.astype(jnp.bfloat16)
            return 0

        lax.fori_loop(0, pairs, body, 0)

    def s1(p, t):
        return pltpu.make_async_remote_copy(
            src_ref=part.at[p, t], dst_ref=rx1.at[p, t],
            send_sem=s1s.at[p, t], recv_sem=s1r.at[p, t],
            device_id=first_peer[p % 2], device_id_type=MESH,
        )

    def across(p, t, source):
        return pltpu.make_async_remote_copy(
            src_ref=source, dst_ref=rxv.at[p, t],
            send_sem=vs.at[p, t], recv_sem=vr.at[p, t],
            device_id=second_peer[p % 2], device_id_type=MESH,
        )

    def late(p):
        return kinds[p // 2] == "vz"

    def hop(p, way, s, source):
        n = 1 if late(p) else 2
        following = lax.rem(z + (1 if way == 0 else planes - 1), planes)
        return pltpu.make_async_remote_copy(
            src_ref=source, dst_ref=held.at[p, way, s, pl.ds(0, n)],
            send_sem=zs.at[p, way, s], recv_sem=zr.at[p, way, s],
            device_id=device(dz=following), device_id_type=MESH,
        )

    def begin(p, t):
        n = 1 if late(p) else 2
        if t > 0:
            @pl.when(z == 0)
            def _():
                hop(p, 0, planes - 1 - t, rx1.at[p, t, pl.ds(0, n)]).start()
        if t < planes - 1:
            @pl.when(z == planes - 1)
            def _():
                hop(p, 1, t, rx1.at[p, t, pl.ds(0, n)]).start()

    def start_first(cu):
        for t in far_first(planes):
            for l in range(2):
                s1(2 * cu + l, t).start()

    def first(cu):
        for t in far_first(planes):
            for l in range(2):
                p = 2 * cu + l
                s1(p, t).wait_recv()
                for k in (1, 0):
                    total = own[p, t, k] + rx1[p, t, k].astype(jnp.float32)
                    own[p, t, k] = total
                    rx1[p, t, k] = total.astype(jnp.bfloat16)
                if late(p):
                    across(p, t, rx1.at[p, t, 1]).start()
                else:
                    begin(p, t)

    def second(cu):
        for t in far_first(planes):
            for l in range(2):
                p = 2 * cu + l
                across(p, t, rx1.at[p, t, 1]).wait_recv()
                total = own[p, t, 0] + rxv[p, t].astype(jnp.float32)
                own[p, t, 0] = total
                rx1[p, t, 0] = total.astype(jnp.bfloat16)
                begin(p, t)

    def tick(cu, tau):
        for way in range(2):
            here = z if way == 0 else planes - 1 - z
            s = tau - here
            target = planes - 1 - s if way == 0 else s
            for l in range(2):
                p = 2 * cu + l
                n = 1 if late(p) else 2

                @pl.when((here >= 1) & (s >= 0))
                def _(p=p, n=n, way=way, s=s, target=target):
                    hop(p, way, s, held.at[p, way, s, pl.ds(0, n)]).wait_recv()
                    for k in range(n):
                        value = held[p, way, s, k].astype(jnp.float32) + own[p, target, k]
                        if tau < planes - 1:
                            held[p, way, s, k] = value.astype(jnp.bfloat16)
                        else:
                            own[p, target, k] = value
                    if tau < planes - 1:
                        hop(p, way, s, held.at[p, way, s, pl.ds(0, n)]).start()

    def third(cu):
        for l in range(2):
            p = 2 * cu + l
            rx1[p, z, 1] = own[p, z, 1].astype(jnp.bfloat16)
            across(p, 0, rx1.at[p, z, 1]).start()

    def leave(p):
        cu, l = p // 2, p % 2
        line = slice(cu // units % halves * half + cu % units * per, None)
        line = slice(line.start, line.start + per)
        lanes = (cu // (units * halves)) * wide + l * LANES
        row = pl.multiple_of(c * angles + line.start, per)
        view = out.at[:, pl.ds(row, per), pl.ds(lanes, LANES)]
        send = pltpu.make_async_remote_copy(
            src_ref=fin.at[pl.ds(img_dev, img_dev), line, pl.ds(lanes, LANES)], dst_ref=view,
            send_sem=fs.at[p], recv_sem=fr.at[p],
            device_id=core_peer, device_id_type=MESH,
        )
        keep = pltpu.make_async_copy(
            fin.at[pl.ds(0, img_dev), line, pl.ds(lanes, LANES)], view, fl.at[p]
        )
        return send, keep, line, lanes

    def finish(cu):
        for l in range(2):
            p = 2 * cu + l
            total = own[p, z, 0]
            if not late(p):
                across(p, 0, rx1.at[p, z, 1]).wait_recv()
                total += rxv[p, 0].astype(jnp.float32)
            ft[l] = total.reshape(per * eight, LANES)
            send, keep, line, lanes = leave(p)
            for r in range(eight):
                v = ft[l, pl.ds(r, per, stride=eight)] * gains[line]
                fin[r, line, lanes : lanes + LANES] = v.astype(jnp.bfloat16)
            send.start()
            keep.start()

    def moment(stage, n=0):
        peer = (core_peer, x_peer, y_peer)[stage] if stage < 3 else device(dz=lax.rem(z + n, planes))
        slot = stage + max(n - 1, 0)
        return pltpu.make_async_remote_copy(
            src_ref=sums.at[stage], dst_ref=pin.at[slot],
            send_sem=ms.at[slot], recv_sem=mr.at[slot],
            device_id=peer, device_id_type=MESH,
        )

    def moments(stage):
        if stage == 0:
            total = jnp.sum(jnp.sum(squares[...], axis=1), axis=1, keepdims=True)
            count = jnp.sum(count_of(live), axis=1, keepdims=True)
            lane = lax.broadcasted_iota(jnp.int32, (angles, LANES), 1)
            both = jnp.where(lane == 0, total, jnp.where(lane == 1, count, 0.0))
            both = jnp.concatenate([both, jnp.zeros((LANES - angles, LANES), jnp.float32)], axis=0)
            sums[0] = both.T[:eight]
            moment(0).start()
        elif stage < 4:
            moment(stage - 1).wait_recv()
            sums[stage] = sums[stage - 1] + pin[stage - 1]
            if stage < 3:
                moment(stage).start()
            else:
                for n in range(1, planes):
                    moment(3, n).start()
        else:
            total = sums[3]
            for n in range(1, planes):
                moment(3, n).wait_recv()
                total += pin[3 + n - 1]
            gain = lax.rsqrt(total[0:1] / (depth * total[1:2]) + 1e-06)
            gains[...] = jnp.broadcast_to(gain, (LANES, LANES)).T[:angles]

    def compute(phase):
        d, h = phase // halves, phase % halves
        if h == 0:
            own_in[d].wait()
        slant(d, h, 0)
        if phase == 0:
            meta.wait_recv()
            cuts[1] = theirs[eight : eight + blocks]
            k_rows = jnp.full((eight, onehot_lanes - LANES), -1, jnp.int32)
            a_row = jnp.concatenate([jnp.broadcast_to(mine[0:1], (eight, LANES)), k_rows], axis=1)
            b_row = jnp.concatenate([jnp.broadcast_to(theirs[0:1], (eight, LANES)), k_rows], axis=1)
            b_row = pltpu.roll(b_row, blocks, 1)
            lane = lax.broadcasted_iota(jnp.int32, a_row.shape, 1)
            row = jnp.where(lane < blocks, a_row, b_row)
            mask = y * (img_dev * grp) + g * img_dev
            row = lax.bitwise_xor(row, jnp.full(row.shape, 0, jnp.int32) + mask)
            number = lax.broadcasted_iota(jnp.int32, (images, onehot_lanes), 0)
            hit = jnp.where(number == row[0:1], 1.0, 0.0).astype(jnp.bfloat16)
            onehot[...] = hit[:, : 2 * blocks]
        if h == 0:
            core_in[d].wait_recv()
        slant(d, h, 1)
        for k in range(units):
            cu = phase * units + k
            stack(cu)
            start_first(cu)

    onehot_lanes = round_up(2 * blocks, LANES)

    def count_of(ref):
        return ref[...].astype(jnp.float32)

    cus = depths * halves * units
    for _, action in sorted(schedule(planes, kinds, depths * halves, units), key=lambda e: e[0]):
        name, args = action[0], action[1:]
        {
            "compute": compute, "first": first, "second": second, "tick": tick,
            "third": third, "finish": finish, "moments": moments,
        }[name](*args)

    meta.wait_send()
    for copy in core_in:
        copy.wait_send()
    for cu in range(cus):
        for l in range(2):
            p = 2 * cu + l
            n = 1 if late(p) else 2
            for t in range(planes):
                s1(p, t).wait_send()
            for t in range(planes if late(p) else 1):
                across(p, t, rx1.at[p, t, 1]).wait_send()
            for way in range(2):
                here = z if way == 0 else planes - 1 - z
                for s in range(planes - 1):
                    @pl.when(here < planes - 1 - s)
                    def _(p=p, way=way, s=s, n=n):
                        hop(p, way, s, held.at[p, way, s, pl.ds(0, n)]).wait_send()
            send, keep, _, _ = leave(p)
            keep.wait()
            send.wait()
    for stage in range(3):
        moment(stage).wait_send()
    for n in range(1, planes):
        moment(3, n).wait_send()


def far_first(planes):
    order = []
    for i in range(planes):
        order.append(planes - 1 - i // 2 if i % 2 == 0 else i // 2)
    return order


def schedule(planes, kinds, phases, units):
    events = []
    step = 3.2
    for phase in range(phases):
        events.append((4.0 + step * phase, ("compute", phase)))
    ready = 4.0 + step * phases
    for stage in range(5):
        events.append((ready + 6.0 * stage, ("moments", stage)))
    gain = ready + 25.0
    now = 7.0
    for cu, kind in enumerate(kinds):
        now += 6.0
        at = now
        events.append((at, ("first", cu)))
        if kind == "vz":
            now += 2.5
            at += 6.0
            events.append((at, ("second", cu)))
        hop = 5.0 if kind == "zv" else 3.5
        for tau in range(1, planes):
            at += hop
            events.append((at, ("tick", cu, tau)))
        if kind == "zv":
            at += 0.1
            events.append((at, ("third", cu)))
            at += 4.0
        events.append((max(at + 0.2, gain), ("finish", cu)))
    return events


def fused(shapes, offsets, slant_weights, live, block_tile, image_slot):
    planes, grp, scratch, kinds = shapes
    blocks = block_tile.shape[0]
    hs, depth = offsets.shape[1:]
    angles = slant_weights.shape[0]
    any_space = pl.BlockSpec(memory_space=pl.ANY)
    vmem = pl.BlockSpec(memory_space=pltpu.VMEM)
    return pl.pallas_call(
        functools.partial(fused_kernel, (planes, grp, kinds)),
        out_shape=jax.ShapeDtypeStruct((IMG_DEV, 2 * angles, depth), jnp.bfloat16),
        in_specs=[any_space, vmem, vmem, vmem, vmem],
        out_specs=any_space,
        scratch_shapes=scratch,
        compiler_params=pltpu.CompilerParams(
            collective_id=2, has_side_effects=True, vmem_limit_bytes=VMEM_LIMIT
        ),
        name="calibrated_stack",
    )(
        offsets.reshape(blocks, 2, hs, depth),
        live.T,
        block_tile.reshape(1, blocks),
        image_slot.reshape(1, blocks),
        slant_weights.T,
    )


def buffers(planes, blocks, hs, depth, angles, images):
    wide = 2 * LANES
    per = 16
    half = 2 * per
    cus = (depth // wide) * (angles // per)
    pieces, pairs = 2 * cus, per // 2
    rows = 2 * 8
    tile = (pairs, rows, LANES)
    dma = pltpu.SemaphoreType.DMA
    bf, f32, i32 = jnp.bfloat16, jnp.float32, jnp.int32
    memory = [
        ((2, blocks, hs, depth), bf),
        ((angles * 8, 8 * hs), bf),
        ((images, 2 * blocks), bf),
        ((8 + blocks, LANES), i32),
        ((8 + blocks, LANES), i32),
        ((2, blocks, LANES), i32),
        ((angles, 8, LANES), f32),
        ((half, 2 * blocks, wide), bf),
        ((pieces, planes, 2) + tile, f32),
        ((pieces, planes, 2) + tile, bf),
        ((pieces, planes, 2) + tile, bf),
        ((pieces, planes) + tile, bf),
        ((pieces, 2, planes - 1, 2) + tile, bf),
        ((2, per * 8, LANES), f32),
        ((2 * IMG_DEV, angles, depth), bf),
        ((8, LANES), f32),
        ((4, 8, LANES), f32),
        ((3 + planes - 1, 8, LANES), f32),
        ((angles, LANES), f32),
    ]
    size = sum(math.prod(s) * jnp.dtype(d).itemsize for s, d in memory)
    scratch = [pltpu.VMEM(s, d) for s, d in memory]
    depths = depth // wide
    scratch += [
        dma((depths,)), dma((depths,)), dma((depths,)), dma((1,)), dma((1,)),
        dma((pieces, planes)), dma((pieces, planes)),
        dma((pieces, planes)), dma((pieces, planes)),
        dma((pieces, 2, planes - 1)), dma((pieces, 2, planes - 1)),
        dma((pieces,)), dma((pieces,)), dma((pieces,)),
        dma((3 + planes - 1,)), dma((3 + planes - 1,)),
    ]
    zfirst = (5 * cus + 4) // 8
    kinds = ("zv",) * zfirst + ("vz",) * (cus - zfirst)
    return size, scratch, kinds


def local(offsets, slant_weights, live, block_tile, image_slot):
    shots, grp = lax.axis_size("shot"), lax.axis_size("grp")
    planes = shots // PAIR
    blocks = block_tile.shape[0]
    hs, depth = offsets.shape[1:]
    angles = slant_weights.shape[0]
    images = shots * IMG_DEV * grp
    size, scratch, kinds = buffers(planes, blocks, hs, depth, angles, images)
    args = (offsets, slant_weights, live, block_tile, image_slot)
    if grp == 4 and size + (2 << 20) <= VMEM_LIMIT:
        return fused((planes, grp, scratch, kinds), *args)
    return staged(*args)


def solution(mesh):
    placed = (
        P(("shot", "grp"), None, None),
        P(),
        P(("shot", "grp"), None),
        P(("shot", "grp"), None),
        P(("shot", "grp")),
    )
    return jax.shard_map(
        local, mesh=mesh, in_specs=placed, out_specs=P(("shot", "grp"), None, None), check_vma=False
    )
```

```python
import functools
import math

import jax
import jax.numpy as jnp
from jax import lax
from jax.experimental import pallas as pl
from jax.experimental.pallas import tpu as pltpu
from jax.sharding import PartitionSpec as P

IMG_DEV = 4
PAIR = 2
LANES = 128
UNROLL = 8
MESH = pl.DeviceIdType.MESH
VMEM_LIMIT = 62 * 1024 * 1024
SLANT_UNROLL = 2
STACK_UNROLL = 4
SCHEDULE = {
    "compute": 3.2, "first": {"zv": 6.5, "vz": 10.5}, "begin": 0.2, "start": 12.7, "sub": 2.0,
    "second": 11.4, "hop": {"zv": 15.9, "vz": 11.4}, "third": 0.3, "finish": 21.0, "moments": 2.5,
}


def place(grp):
    shot, g = lax.axis_index("shot"), lax.axis_index("grp")
    return lax.div(shot, PAIR), lax.rem(shot, PAIR) * grp + g


def at(plane, spot, grp):
    return (plane * PAIR + lax.div(spot, grp), lax.rem(spot, grp))


def share(spot, width, depth):
    start = spot * width
    return lax.div(start, depth), pl.multiple_of(lax.rem(start, depth), LANES)


def relative(spot, grp, r):
    mid = grp // 2
    pair, rest = lax.div(spot, grp), lax.rem(spot, grp)
    m, c = lax.div(rest, 2), lax.rem(rest, 2)
    rp, rm, rc = r // grp, (r % grp) // 2, r % 2
    pair, m, c = lax.rem(pair + rp, PAIR), lax.rem(m + rm, mid), lax.rem(c + rc, 2)
    return (pair * mid + m) * 2 + c


def orders(grp):
    size = PAIR * grp
    far = list(range(grp + 2, size))
    side = list(range(grp, grp + 2))
    ahead = list(range(2, grp))
    turn = []
    for i in range(max(len(far), len(ahead))):
        for group in (far, side, ahead):
            turn += group[i : i + 1]
    return [1] + turn


def exchange_kernel(
    grp, off, aux, w_in, part, mom, w, raw, aux_in, codes, acc, seg, send, recv, asend, arecv, lsem
):
    size = PAIR * grp
    plane, spot = place(grp)
    blocks, depth, width = off.shape[0], off.shape[3], raw.shape[3]
    angles, images = w.shape[1], acc.shape[0]
    j, first = share(spot, width, depth)
    mine = pltpu.make_async_copy(off.at[:, j, :, pl.ds(first, width)], raw.at[0], lsem.at[0])
    mine.start()
    own_codes = pltpu.make_async_copy(aux, codes.at[0], lsem.at[1])
    own_codes.start()
    weigh = pltpu.make_async_copy(w_in, w, lsem.at[size + 1])
    weigh.start()
    barrier = pltpu.get_barrier_semaphore()
    for r in range(1, size):
        pl.semaphore_signal(
            barrier, inc=1, device_id=at(plane, relative(spot, grp, r), grp), device_id_type=MESH
        )
    pl.semaphore_wait(barrier, size - 1)
    data, notes = {}, {}
    for r in orders(grp):
        peer = relative(spot, grp, r)
        pj, pfirst = share(peer, width, depth)
        dev = at(plane, peer, grp)
        notes[r] = pltpu.make_async_remote_copy(
            src_ref=aux,
            dst_ref=aux_in.at[r],
            send_sem=asend.at[r - 1],
            recv_sem=arecv.at[r - 1],
            device_id=dev,
            device_id_type=MESH,
        )
        data[r] = pltpu.make_async_remote_copy(
            src_ref=off.at[:, pj, :, pl.ds(pfirst, width)],
            dst_ref=raw.at[r],
            send_sem=send.at[r - 1],
            recv_sem=recv.at[r - 1],
            device_id=dev,
            device_id_type=MESH,
        )
    for r in orders(grp):
        notes[r].start()
    for r in orders(grp):
        data[r].start()

    acc[...] = jnp.zeros_like(acc)
    seg[blocks] = jnp.zeros((angles, width), jnp.float32)
    row = lax.broadcasted_iota(jnp.int32, (angles, width), 0)
    weigh.wait()
    weights = w[...].astype(jnp.float32).T.astype(jnp.bfloat16)
    square = jnp.zeros((angles, width), jnp.float32)
    count = jnp.zeros((angles, width), jnp.float32)
    for r in [0] + orders(grp):
        if r:
            notes[r].wait()
            code = pltpu.make_async_copy(aux_in.at[r], codes.at[r], lsem.at[r + 1])
            code.start()
            code.wait()
            data[r].wait()
        else:
            own_codes.wait()
            mine.wait()

        def slant(i, carry, r=r):
            square, count = carry
            start = i * UNROLL
            x = jnp.concatenate([raw[r, start + t] for t in range(UNROLL)], axis=1)
            y = jnp.dot(weights, x, preferred_element_type=jnp.float32)
            for t in range(UNROLL):
                alive = row < codes[r, 1 + j, start + t]
                slanted = jnp.where(alive, y[:, t * width : (t + 1) * width], 0.0)
                slanted = slanted.astype(jnp.bfloat16).astype(jnp.float32)
                square += slanted * slanted
                count += jnp.where(alive, 1.0, 0.0)
                seg[start + t] = slanted + seg[codes[r, 0, start + t]]
            return square, count

        square, count = lax.fori_loop(0, blocks // UNROLL, slant, (square, count))

        def stack(i, _, r=r):
            start = i * UNROLL
            line, column = lax.div(start, LANES), lax.rem(start, LANES)
            for t in range(UNROLL):
                acc[start + t] += seg[codes[r, 3 + line, column + t]]
            return 0

        lax.fori_loop(0, images // UNROLL, stack, 0)

    def narrow(i, _):
        start = pl.multiple_of(i * UNROLL, UNROLL)
        part[pl.ds(start, UNROLL)] = acc[pl.ds(start, UNROLL)].astype(jnp.bfloat16)
        return 0

    lax.fori_loop(0, images // UNROLL, narrow, 0)
    lane = lax.broadcasted_iota(jnp.int32, (angles, LANES), 1)
    square = jnp.sum(square, axis=1, keepdims=True)
    count = jnp.sum(count, axis=1, keepdims=True)
    both = jnp.where(lane == 0, square, jnp.where(lane == 1, count, 0.0))
    both = jnp.concatenate([both, jnp.zeros((LANES - angles, LANES), jnp.float32)], axis=0)
    mom[...] = both.T[: mom.shape[0]]


def gather_kernel(
    grp, part, mom, out, held, total, fin, pin, qin, half_sum, zs, zr, ps, pr, qs, qr, fs, fr, lsem
):
    size = PAIR * grp
    planes = held.shape[1] + 1
    plane, spot = place(grp)
    pieces, rows, angles, width = held.shape[2:]
    depth = out.shape[2]
    chunk = pieces * rows
    lower = jnp.where(plane < planes // 2, 1, 0)
    barrier = pltpu.get_barrier_semaphore()
    for r in range(1, size):
        pl.semaphore_signal(
            barrier, inc=1, device_id=at(plane, lax.rem(spot + r, size), grp), device_id_type=MESH
        )
    for r in range(1, planes):
        pl.semaphore_signal(
            barrier, inc=1, device_id=at(lax.rem(plane + r, planes), spot, grp), device_id_type=MESH
        )
    pl.semaphore_wait(barrier, size + planes - 2)

    def along(up):
        spot_on_line = plane * up + (planes - 1 - plane) * (1 - up)
        following = lax.rem(plane + 2 * up - 1 + planes, planes)
        return 1 - up, spot_on_line, following

    def rows_of(up, s, h):
        target = (planes - 1 - s) * up + s * (1 - up)
        return target * chunk + h * rows

    def hop(up, s, h, source):
        way, _, following = along(up)
        return pltpu.make_async_remote_copy(
            src_ref=source,
            dst_ref=held.at[way, s, h],
            send_sem=zs.at[way, s, h],
            recv_sem=zr.at[way, s, h],
            device_id=at(following, spot, grp),
            device_id_type=MESH,
        )

    def begin(s):
        @pl.when(along(lower)[1] == 0)
        def _():
            for h in range(pieces):
                hop(lower, s, h, part.at[pl.ds(rows_of(lower, s, h), rows)]).start()

    def step(up, s, h):
        way, here, _ = along(up)
        end = planes - 1 - s

        @pl.when((here > 0) & (here <= end))
        def _():
            hop(up, s, h, held.at[way, s, h]).wait_recv()

        @pl.when((here > 0) & (here < end))
        def _():
            start = rows_of(up, s, h)

            def add(i, _):
                value = held[way, s, h, i].astype(jnp.float32) + part[start + i].astype(jnp.float32)
                held[way, s, h, i] = value.astype(jnp.bfloat16)
                return 0

            lax.fori_loop(0, rows, add, 0)
            hop(up, s, h, held.at[way, s, h]).start()

        @pl.when((here > 0) & (here == end))
        def _():
            def add(i, _):
                total[h * rows + i] += held[way, s, h, i].astype(jnp.float32)
                return 0

            lax.fori_loop(0, rows, add, 0)

    def finish(up, s, h):
        way, here, _ = along(up)

        @pl.when(here < planes - 1 - s)
        def _():
            hop(up, s, h, held.at[way, s, h]).wait_send()

    near = [
        pltpu.make_async_remote_copy(
            src_ref=mom,
            dst_ref=pin.at[r - 1],
            send_sem=ps.at[r - 1],
            recv_sem=pr.at[r - 1],
            device_id=at(plane, lax.rem(spot + r, size), grp),
            device_id_type=MESH,
        )
        for r in range(1, size)
    ]
    for copy in near:
        copy.start()
    begin(0)
    total[...] = part[pl.ds(plane * chunk, chunk)].astype(jnp.float32)
    moments = mom[...]
    for copy in near:
        copy.wait()
    for r in range(1, size):
        moments += pin[r - 1]
    half_sum[...] = moments
    wide = [
        pltpu.make_async_remote_copy(
            src_ref=half_sum,
            dst_ref=qin.at[r - 1],
            send_sem=qs.at[r - 1],
            recv_sem=qr.at[r - 1],
            device_id=at(lax.rem(plane + r, planes), spot, grp),
            device_id_type=MESH,
        )
        for r in range(1, planes)
    ]
    for copy in wide:
        copy.start()
    for s in range(1, planes - 1):
        begin(s)
    for s in range(planes - 1):
        for up in (lower, 1 - lower):
            for h in range(pieces):
                step(up, s, h)
    for copy in wide:
        copy.wait()
    moments = half_sum[...]
    for r in range(1, planes):
        moments += qin[r - 1]
    gain = lax.rsqrt(moments[0:1] / moments[1:2] + 1e-06)
    gain = jnp.broadcast_to(gain, (LANES, LANES)).T[:angles]

    def body(i, _):
        fin[i] = (total[i] * gain).astype(jnp.bfloat16)
        return 0

    lax.fori_loop(0, chunk, body, 0)

    each = chunk // size
    j, first = share(spot, width, depth)
    view = out.at[:, pl.ds(pl.multiple_of(j * angles, angles), angles), pl.ds(first, width)]
    last = pltpu.make_async_copy(fin.at[pl.ds(spot * each, each)], view, lsem.at[1])
    final = []
    for r in range(1, size):
        peer = lax.rem(spot + r, size)
        final.append(
            pltpu.make_async_remote_copy(
                src_ref=fin.at[pl.ds(peer * each, each)],
                dst_ref=view,
                send_sem=fs.at[r - 1],
                recv_sem=fr.at[r - 1],
                device_id=at(plane, peer, grp),
                device_id_type=MESH,
            )
        )
    for copy in final:
        copy.start()
    last.start()
    last.wait()
    for copy in final:
        copy.wait()
    for s in range(planes - 1):
        for up in (lower, 1 - lower):
            for h in range(pieces):
                finish(up, s, h)


def staged(offsets, slant_weights, live, block_tile, image_slot):
    shots, grp = lax.axis_size("shot"), lax.axis_size("grp")
    planes, size = shots // PAIR, PAIR * grp
    blocks = block_tile.shape[0]
    hs, depth = offsets.shape[1:]
    angles = slant_weights.shape[0]
    width = 2 * depth // size
    tile_rows = IMG_DEV * grp
    images = shots * tile_rows
    per_plane = images // planes
    any_space = pl.BlockSpec(memory_space=pl.ANY)
    vmem = pl.BlockSpec(memory_space=pltpu.VMEM)
    dma = pltpu.SemaphoreType.DMA

    cutoff = jnp.sum(live.reshape(blocks, 2, angles), axis=2)
    image = block_tile[:, 0] * tile_rows + image_slot
    index = jnp.arange(blocks, dtype=jnp.int32)
    same = (image[:, None] == image[None, :]) & (index[None, :] < index[:, None])
    before = jnp.max(jnp.where(same, index[None, :], -1), axis=1)
    found = image[None, :] == jnp.arange(images, dtype=jnp.int32)[:, None]
    final = jnp.max(jnp.where(found, index[None, :], -1), axis=1)
    final = jnp.where(final < 0, blocks, final).reshape(images // LANES, LANES)
    before = jnp.where(before < 0, blocks, before)
    aux = jnp.concatenate([before[None], cutoff.T], axis=0)
    aux = jnp.concatenate([jnp.pad(aux, ((0, 0), (0, LANES - blocks))), final], axis=0)
    aux = jnp.pad(aux, ((0, -aux.shape[0] % 8), (0, 0)))

    part, mom = pl.pallas_call(
        functools.partial(exchange_kernel, grp),
        out_shape=(
            jax.ShapeDtypeStruct((images, angles, width), jnp.bfloat16),
            jax.ShapeDtypeStruct((8, LANES), jnp.float32),
        ),
        in_specs=[any_space, vmem, any_space],
        out_specs=(vmem, vmem),
        scratch_shapes=[
            pltpu.VMEM((hs, angles), jnp.bfloat16),
            pltpu.VMEM((size, blocks, hs, width), jnp.bfloat16),
            pltpu.VMEM((size,) + aux.shape, jnp.int32),
            pltpu.SMEM((size,) + aux.shape, jnp.int32),
            pltpu.VMEM((images, angles, width), jnp.float32),
            pltpu.VMEM((blocks + 1, angles, width), jnp.float32),
            dma((size - 1,)),
            dma((size - 1,)),
            dma((size - 1,)),
            dma((size - 1,)),
            dma((size + 2,)),
        ],
        compiler_params=pltpu.CompilerParams(
            collective_id=0, has_side_effects=True, vmem_limit_bytes=62 * 1024 * 1024
        ),
        name="exchange",
    )(offsets.reshape(blocks, 2, hs, depth), aux, slant_weights.T)

    moments = (8, LANES)
    pieces = 4
    lines = (2, planes - 1, pieces)
    return pl.pallas_call(
        functools.partial(gather_kernel, grp),
        out_shape=jax.ShapeDtypeStruct((IMG_DEV, 2 * angles, depth), jnp.bfloat16),
        in_specs=[vmem, vmem],
        out_specs=any_space,
        scratch_shapes=[
            pltpu.VMEM(lines + (per_plane // pieces, angles, width), jnp.bfloat16),
            pltpu.VMEM((per_plane, angles, width), jnp.float32),
            pltpu.VMEM((per_plane, angles, width), jnp.bfloat16),
            pltpu.VMEM((size - 1,) + moments, jnp.float32),
            pltpu.VMEM((planes - 1,) + moments, jnp.float32),
            pltpu.VMEM(moments, jnp.float32),
            dma(lines),
            dma(lines),
            dma((size - 1,)),
            dma((size - 1,)),
            dma((planes - 1,)),
            dma((planes - 1,)),
            dma((size - 1,)),
            dma((size - 1,)),
            dma((2,)),
        ],
        compiler_params=pltpu.CompilerParams(
            collective_id=1, has_side_effects=True, vmem_limit_bytes=60 * 1024 * 1024
        ),
        name="gather",
    )(part, mom)


def round_up(value, unit):
    return -(-value // unit) * unit


def fused_kernel(
    shape, off, live_in, tile_in, slot_in, w_in, out,
    live, tile, slot, weights, raw, wb, onehot, mine, theirs, cuts, squares, sl,
    own, part, rx1, rxv, held, ft, fin, sums, pin, gains,
    load_sem, in_sem, core_s, core_r, meta_s, meta_r, s1s, s1r, vs, vr, zs, zr, fs, fr, fl, ms, mr,
):
    planes, grp, kinds = shape
    shot, g = lax.axis_index("shot"), lax.axis_index("grp")
    z, y = lax.div(shot, PAIR), lax.rem(shot, PAIR)
    x, c = lax.div(g, 2), lax.rem(g, 2)
    blocks, hs, depth = raw.shape[1:]
    angles = live.shape[0]
    images = onehot.shape[0]
    img_dev = out.shape[0]
    per, wide = sl.shape[1], sl.shape[3]
    pairs = per // 2
    depths, groups = depth // wide, angles // per
    cus = depths * groups
    early = 2 * kinds.count("zv")
    late_count = 2 * cus - early

    def device(step=0, fy=False, fx=False, fc=False):
        yy = 1 - y if fy else y
        xx = 1 - x if fx else x
        cc = 1 - c if fc else c
        return ((z + step) * PAIR + yy, xx * 2 + cc)

    core_peer, x_peer, y_peer = device(fc=True), device(fx=True), device(fy=True)
    first_peer = (x_peer, y_peer)
    second_peer = (y_peer, x_peer)

    def remote(src, dst, send_sem, recv_sem, peer):
        return pltpu.make_async_remote_copy(
            src_ref=src, dst_ref=dst, send_sem=send_sem, recv_sem=recv_sem,
            device_id=peer, device_id_type=MESH,
        )

    barrier = pltpu.get_barrier_semaphore()

    def greet(peer):
        pl.semaphore_signal(barrier, inc=1, device_id=peer, device_id_type=MESH)

    for peer in (core_peer, x_peer, y_peer):
        greet(peer)

    @pl.when(z > 0)
    def _():
        greet(device(step=-1))

    @pl.when(z < planes - 1)
    def _():
        greet(device(step=1))

    loads = [
        pltpu.make_async_copy(src, dst, load_sem.at[n])
        for n, (src, dst) in enumerate(
            ((w_in, weights), (live_in, live), (tile_in, tile), (slot_in, slot))
        )
    ]
    for copy in loads:
        copy.start()
    own_in = [
        pltpu.make_async_copy(
            off.at[:, c, :, pl.ds(d * wide, wide)],
            raw.at[0, :, :, pl.ds(d * wide, wide)],
            in_sem.at[d],
        )
        for d in range(depths)
    ]
    for copy in own_in:
        copy.start()
    core_in = [
        remote(
            off.at[:, 1 - c, :, pl.ds(d * wide, wide)],
            raw.at[1, :, :, pl.ds(d * wide, wide)],
            core_s.at[d], core_r.at[d], core_peer,
        )
        for d in range(depths)
    ]
    meta = remote(mine, theirs, meta_s.at[0], meta_r.at[0], core_peer)

    eight = 8
    for copy in loads:
        copy.wait()
    ones = jnp.ones((angles, LANES), jnp.bfloat16)
    spot = lax.broadcasted_iota(jnp.int32, (blocks, 2 * blocks), 1)
    block = lax.broadcasted_iota(jnp.int32, (blocks, 2 * blocks), 0)

    def cutoff(j):
        pick = jnp.where(spot == 2 * block + j, 1.0, 0.0).astype(jnp.bfloat16)
        flags = lax.dot_general(
            pick, live[...].astype(jnp.float32).astype(jnp.bfloat16),
            (((1,), (1,)), ((), ())), preferred_element_type=jnp.float32,
        )
        total = jnp.dot(flags.astype(jnp.bfloat16), ones, preferred_element_type=jnp.float32)
        return total.astype(jnp.int32)

    mine[0:eight] = jnp.full((eight, LANES), -1, jnp.int32)
    mine[0:1, 0:blocks] = tile[...] * (img_dev * grp) + slot[...]
    mine[eight : eight + blocks] = cutoff(1 - c)
    cuts[0] = cutoff(c)

    ends = jnp.where(z == 0, 1, 0) + jnp.where(z == planes - 1, 1, 0)
    pl.semaphore_wait(barrier, 5 - ends)
    core_in[0].start()
    meta.start()
    for copy in core_in[1:]:
        copy.start()

    rows = angles * eight
    spread = lax.broadcasted_iota(jnp.int32, (rows, angles), 0)
    which = lax.broadcasted_iota(jnp.int32, (rows, angles), 1)
    pick = jnp.where(lax.div(spread, eight) == which, 1.0, 0.0).astype(jnp.bfloat16)
    tall = lax.dot_general(
        pick, weights[...], (((1,), (1,)), ((), ())), preferred_element_type=jnp.float32
    ).astype(jnp.bfloat16)
    line = lax.broadcasted_iota(jnp.int32, (hs, eight * hs), 0)
    column = lax.broadcasted_iota(jnp.int32, (hs, eight * hs), 1)
    copies = jnp.where(lax.rem(column, hs) == line, 1.0, 0.0).astype(jnp.bfloat16)
    full = jnp.dot(tall, copies, preferred_element_type=jnp.float32)
    line = lax.broadcasted_iota(jnp.int32, full.shape, 0)
    column = lax.broadcasted_iota(jnp.int32, full.shape, 1)
    wb[...] = jnp.where(lax.rem(line, eight) == lax.div(column, hs), full, 0.0).astype(jnp.bfloat16)
    squares[...] = jnp.zeros_like(squares)

    def slant(cu, r):
        d, a0 = cu // groups, cu % groups * per
        if r == 0 and cu % groups == 0:
            own_in[d].wait()
        if r == 1 and cu == 0:
            meta.wait_recv()
            cuts[1] = theirs[eight : eight + blocks]
            select_rows()
        if r == 1 and cu % groups == 0:
            core_in[d].wait_recv()

        def body(i, _):
            lhs = wb[a0 * eight : (a0 + per) * eight]
            lanes = slice(d * wide, (d + 1) * wide)
            a = lax.broadcasted_iota(jnp.int32, (per, 2 * eight, LANES), 0) + a0
            total = squares[a0 : a0 + per]
            for n in range(SLANT_UNROLL):
                start = (i * SLANT_UNROLL + n) * 2 * eight
                alive = cuts[r, pl.ds(start, 2 * eight)][None] > a
                ys = []
                for k in range(2):
                    data = raw[r, pl.ds(start + k * eight, eight), :, lanes]
                    data = data.reshape(eight * hs, wide)
                    y = jnp.dot(lhs, data, preferred_element_type=jnp.float32)
                    ys.append(y.reshape(per, eight, wide))
                for k in range(wide // LANES):
                    cut = slice(k * LANES, (k + 1) * LANES)
                    v = jnp.concatenate([ys[0][:, :, cut], ys[1][:, :, cut]], axis=1)
                    v = jnp.where(alive, v, 0.0)
                    q = v * v
                    total += q[:, :eight] + q[:, eight:]
                    sl[cu % 2, :, pl.ds(r * blocks + start, 2 * eight), cut] = v.astype(jnp.bfloat16)
            squares[a0 : a0 + per] = total
            return 0

        lax.fori_loop(0, blocks // (2 * eight * SLANT_UNROLL), body, 0)

    def select_rows():
        lanes = round_up(2 * blocks, LANES)
        rest = jnp.full((eight, lanes - LANES), -1, jnp.int32)
        a_row = jnp.concatenate([jnp.broadcast_to(mine[0:1], (eight, LANES)), rest], axis=1)
        b_row = jnp.concatenate([jnp.broadcast_to(theirs[0:1], (eight, LANES)), rest], axis=1)
        b_row = pltpu.roll(b_row, blocks, 1)
        lane = lax.broadcasted_iota(jnp.int32, a_row.shape, 1)
        row = jnp.where(lane < blocks, a_row, b_row)
        mask = y * (img_dev * grp) + g * img_dev
        row = lax.bitwise_xor(row, jnp.full(row.shape, 0, jnp.int32) + mask)
        number = lax.broadcasted_iota(jnp.int32, (images, lanes), 0)
        hit = jnp.where(number == row[0:1], 1.0, 0.0).astype(jnp.bfloat16)
        onehot[...] = hit[:, : 2 * blocks]

    def stack(cu):
        def body(i, _):
            for n in range(STACK_UNROLL):
                m = i * STACK_UNROLL + n
                ys = [
                    jnp.dot(onehot[...], sl[cu % 2, 2 * m + k], preferred_element_type=jnp.float32)
                    for k in range(2)
                ]
                for l in range(2):
                    p = 2 * cu + l
                    cut = slice(l * LANES, (l + 1) * LANES)
                    for t in range(planes):
                        for ry in range(2):
                            for rx in range(2):
                                r = ((t * 2 + ry) * 2 + rx) * eight
                                v = [ys[k][r : r + eight, cut] for k in range(2)]
                                v = jnp.concatenate(v, axis=0)
                                one, two = (rx, ry) if l == 0 else (ry, rx)
                                if one == 0:
                                    own[p, t, two, m] = v
                                else:
                                    part[p, t, two, m] = v.astype(jnp.bfloat16)
            return 0

        lax.fori_loop(0, pairs // STACK_UNROLL, body, 0)

    def late(cu):
        return kinds[cu] == "vz"

    def s1(cu, l, t):
        p = 2 * cu + l
        return remote(part.at[p, t], rx1.at[p, t], s1s.at[0], s1r.at[cu, t], first_peer[l])

    def across_slot(cu, t):
        return early // 2 + (cu - early // 2) * planes + t if late(cu) else cu

    def across(cu, l, t, source):
        p, slot = 2 * cu + l, across_slot(cu, t)
        kind = 1 if late(cu) else 0
        return remote(source, rxv.at[p, t], vs.at[kind], vr.at[slot], second_peer[l])

    def arrived(region, sem):
        remote(region, region, ms.at[0], sem, core_peer).wait_recv()

    def hop(cu, way, s, source):
        p, n = pl.ds(2 * cu, 2), pl.ds(0, 1 if late(cu) else 2)
        kind = 1 if late(cu) else 0
        return remote(
            source, held.at[p, way, s, n], zs.at[kind, way, s], zr.at[cu, way, s],
            device(step=1 - 2 * way),
        )

    def begin(cu, t):
        source = rx1.at[pl.ds(2 * cu, 2), t, pl.ds(0, 1 if late(cu) else 2)]
        if t > 0:
            @pl.when(z == 0)
            def _():
                hop(cu, 0, planes - 1 - t, source).start()
        if t < planes - 1:
            @pl.when(z == planes - 1)
            def _():
                hop(cu, 1, t, source).start()

    def start(cu):
        for t in far_first(planes):
            for l in range(2):
                s1(cu, l, t).start()

    def first(cu, t):
        arrived(rx1.at[pl.ds(2 * cu, 2), t], s1r.at[cu, t])
        for l in range(2):
            p = 2 * cu + l
            for k in (1, 0):
                total = own[p, t, k] + rx1[p, t, k].astype(jnp.float32)
                own[p, t, k] = total
                rx1[p, t, k] = total.astype(jnp.bfloat16)
            if late(cu):
                across(cu, l, t, rx1.at[p, t, 1]).start()
        if not late(cu):
            begin(cu, t)

    def second(cu, t):
        arrived(rxv.at[pl.ds(2 * cu, 2), t], vr.at[across_slot(cu, t)])
        for l in range(2):
            p = 2 * cu + l
            total = own[p, t, 0] + rxv[p, t].astype(jnp.float32)
            own[p, t, 0] = total
            rx1[p, t, 0] = total.astype(jnp.bfloat16)
        begin(cu, t)

    def tick(cu, tau, way):
        here = z if way == 0 else planes - 1 - z
        s = tau - here
        target = planes - 1 - s if way == 0 else s
        n = 1 if late(cu) else 2

        @pl.when((here >= 1) & (s >= 0))
        def _():
            message = held.at[pl.ds(2 * cu, 2), way, s, pl.ds(0, n)]
            hop(cu, way, s, message).wait_recv()
            for l in range(2):
                p = 2 * cu + l
                for k in range(n):
                    value = held[p, way, s, k].astype(jnp.float32) + own[p, target, k]
                    if tau < planes - 1:
                        held[p, way, s, k] = value.astype(jnp.bfloat16)
                    else:
                        own[p, target, k] = value
            if tau < planes - 1:
                hop(cu, way, s, message).start()

    def third(cu):
        for l in range(2):
            p = 2 * cu + l
            rx1[p, z, 1] = own[p, z, 1].astype(jnp.bfloat16)
            across(cu, l, 0, rx1.at[p, z, 1]).start()

    def leave(line, lanes):
        row = pl.multiple_of(c * angles + line.start, per)
        view = out.at[:, pl.ds(row, line.size), pl.ds(lanes.start, lanes.size)]
        send = remote(fin.at[pl.ds(img_dev, img_dev), line, lanes], view, fs.at[0], fr.at[0], core_peer)
        keep = pltpu.make_async_copy(fin.at[pl.ds(0, img_dev), line, lanes], view, fl.at[0])
        return send, keep

    def finish(cu):
        if not late(cu):
            arrived(rxv.at[pl.ds(2 * cu, 2), 0], vr.at[across_slot(cu, 0)])
        a0, lane0 = cu % groups * per, cu // groups * wide
        for l in range(2):
            p = 2 * cu + l
            total = own[p, z, 0]
            if not late(cu):
                total += rxv[p, 0].astype(jnp.float32)
            ft[l] = total.reshape(per * eight, LANES)
            lanes = slice(lane0 + l * LANES, lane0 + (l + 1) * LANES)
            for r in range(eight):
                v = ft[l, pl.ds(r, per, stride=eight)] * gains[a0 : a0 + per]
                fin[r, a0 : a0 + per, lanes] = v.astype(jnp.bfloat16)
        for copy in leave(pl.ds(a0, per), pl.ds(lane0, wide)):
            copy.start()

    def moment(stage):
        peer = (core_peer, x_peer, y_peer)[stage]
        return remote(sums.at[stage], pin.at[stage], ms.at[stage], mr.at[stage], peer)

    def passing(way):
        n = 3 + way
        return remote(sums.at[n + 1], pin.at[n], ms.at[n], mr.at[n], device(step=1 - 2 * way))

    def moments(stage):
        if stage == 0:
            total = jnp.sum(jnp.sum(squares[...], axis=1), axis=1, keepdims=True)
            count = jnp.sum(live[...].astype(jnp.float32), axis=1, keepdims=True)
            lane = lax.broadcasted_iota(jnp.int32, (angles, LANES), 1)
            both = jnp.where(lane == 0, total, jnp.where(lane == 1, count, 0.0))
            both = jnp.concatenate([both, jnp.zeros((LANES - angles, LANES), jnp.float32)], axis=0)
            sums[0] = both.T[:eight]
            moment(0).start()
            return
        if stage <= 3:
            moment(stage - 1).wait_recv()
            sums[stage] = sums[stage - 1] + pin[stage - 1]
            if stage < 3:
                moment(stage).start()
                return
            sums[6] = sums[3]
        tau = stage - 3
        if tau < planes:
            for way in range(2):
                here = z if way == 0 else planes - 1 - z

                @pl.when(here == tau)
                def _(way=way):
                    if tau > 0:
                        passing(way).wait_recv()
                        sums[6] = sums[6] + pin[3 + way]
                        sums[4 + way] = sums[3] + pin[3 + way]
                    else:
                        sums[4 + way] = sums[3]
                    if tau < planes - 1:
                        passing(way).start()
        else:
            total = sums[6]
            gain = lax.rsqrt(total[0:1] / (depth * total[1:2]) + 1e-06)
            gains[...] = jnp.broadcast_to(gain, (LANES, LANES)).T[:angles]

    run = {
        "slant": slant, "stack": stack, "start": start, "first": first, "second": second,
        "tick": tick, "third": third, "finish": finish, "moments": moments,
    }
    for _, action in sorted(schedule(planes, kinds), key=lambda e: e[0]):
        run[action[0]](*action[1:])

    meta.wait_send()
    for copy in core_in:
        copy.wait_send()
    remote(part, rx1, s1s.at[0], s1r.at[0, 0], core_peer).wait_send()
    if early:
        region = rxv.at[pl.ds(0, early), 0]
        remote(region, region, vs.at[0], vr.at[0], core_peer).wait_send()
    if late_count:
        region = rxv.at[pl.ds(early, late_count)]
        remote(region, region, vs.at[1], vr.at[0], core_peer).wait_send()
    for way in range(2):
        here = z if way == 0 else planes - 1 - z

        @pl.when(here < planes - 1)
        def _(way=way):
            passing(way).wait_send()

        for s in range(planes - 1):
            @pl.when(here < planes - 1 - s)
            def _(way=way, s=s):
                for kind, region in enumerate(
                    (
                        held.at[pl.ds(0, early), way, s],
                        held.at[pl.ds(early, late_count), way, s, pl.ds(0, 1)],
                    )
                ):
                    if (early, late_count)[kind]:
                        remote(
                            region, region, zs.at[kind, way, s], zr.at[0, way, s], core_peer
                        ).wait_send()
    for stage in range(3):
        moment(stage).wait_send()
    send, keep = leave(pl.ds(0, angles), pl.ds(0, depth))
    keep.wait()
    send.wait()


def far_first(planes):
    return [planes - 1 - i // 2 if i % 2 == 0 else i // 2 for i in range(planes)]


def schedule(planes, kinds):
    compute, spacing, lag, sub = SCHEDULE["compute"], SCHEDULE["first"], SCHEDULE["start"], SCHEDULE["sub"]
    cus = len(kinds)
    events = [(-2.0, ("slant", 0, 0)), (-1.0, ("slant", 1, 0))]
    for cu in range(cus):
        at = compute * cu
        if cu > 1:
            events.append((at, ("slant", cu, 0)))
        events.append((at + 0.1 * compute, ("slant", cu, 1)))
        events.append((at + 0.2 * compute, ("stack", cu)))
    done = compute * cus
    for stage in range(3 + planes + 1):
        events.append((done + SCHEDULE["moments"] * stage, ("moments", stage)))
    gain = done + SCHEDULE["moments"] * (3 + planes) + 0.1
    now = SCHEDULE["begin"]
    for cu, kind in enumerate(kinds):
        at = now
        events.append((max(compute * cu + 0.3 * compute, at - lag), ("start", cu)))
        at = max(at, compute * cu + 0.3 * compute + 0.1)
        for i, t in enumerate(far_first(planes)):
            events.append((at + i * sub, ("first", cu, t)))
        now += spacing[kind]
        at += (planes - 1) * sub
        if kind == "vz":
            at += SCHEDULE["second"] - (planes - 1) * sub
            for i, t in enumerate(far_first(planes)):
                events.append((at + i * sub, ("second", cu, t)))
            at += (planes - 1) * sub
        for tau in range(1, planes):
            at += SCHEDULE["hop"][kind]
            for way in range(2):
                events.append((at, ("tick", cu, tau, way)))
        if kind == "zv":
            at += SCHEDULE["third"]
            events.append((at, ("third", cu)))
            at += SCHEDULE["finish"]
        events.append((max(at + 0.01, gain), ("finish", cu)))
    return events


def fused(shapes, offsets, slant_weights, live, block_tile, image_slot):
    planes, grp, scratch, kinds = shapes
    blocks = block_tile.shape[0]
    hs, depth = offsets.shape[1:]
    angles = slant_weights.shape[0]
    any_space = pl.BlockSpec(memory_space=pl.ANY)
    return pl.pallas_call(
        functools.partial(fused_kernel, (planes, grp, kinds)),
        out_shape=jax.ShapeDtypeStruct((IMG_DEV, 2 * angles, depth), jnp.bfloat16),
        in_specs=[any_space] * 5,
        out_specs=any_space,
        scratch_shapes=scratch,
        compiler_params=pltpu.CompilerParams(
            collective_id=2, has_side_effects=True, vmem_limit_bytes=VMEM_LIMIT
        ),
        name="calibrated_stack",
    )(
        offsets.reshape(blocks, 2, hs, depth),
        live.T,
        block_tile.reshape(1, blocks),
        image_slot.reshape(1, blocks),
        slant_weights.T,
    )


def buffers(planes, blocks, hs, depth, angles, images):
    wide, per = 2 * LANES, 16
    cus = (depth // wide) * (angles // per)
    pieces = 2 * cus
    tile = (per // 2, 16, LANES)
    dma = pltpu.SemaphoreType.DMA
    bf, f32, i32 = jnp.bfloat16, jnp.float32, jnp.int32
    early = (5 * cus + 4) // 8
    kinds = ("zv",) * early + ("vz",) * (cus - early)
    memory = [
        ((angles, 2 * blocks), i32),
        ((1, blocks), i32),
        ((1, blocks), i32),
        ((hs, angles), bf),
        ((2, blocks, hs, depth), bf),
        ((angles * 8, 8 * hs), bf),
        ((images, 2 * blocks), bf),
        ((8 + blocks, LANES), i32),
        ((8 + blocks, LANES), i32),
        ((2, blocks, LANES), i32),
        ((angles, 8, LANES), f32),
        ((2, per, 2 * blocks, wide), bf),
        ((pieces, planes, 2) + tile, f32),
        ((pieces, planes, 2) + tile, bf),
        ((pieces, planes, 2) + tile, bf),
        ((pieces, planes) + tile, bf),
        ((pieces, 2, planes - 1, 2) + tile, bf),
        ((2, per * 8, LANES), f32),
        ((2 * IMG_DEV, angles, depth), bf),
        ((7, 8, LANES), f32),
        ((5, 8, LANES), f32),
        ((angles, LANES), f32),
    ]
    size = sum(math.prod(s) * jnp.dtype(d).itemsize for s, d in memory)
    scratch = [pltpu.VMEM(s, d) for s, d in memory]
    depths = depth // wide
    scratch += [
        dma((4,)), dma((depths,)), dma((depths,)), dma((depths,)), dma((1,)), dma((1,)),
        dma((1,)), dma((cus, planes)),
        dma((2,)), dma((early + (cus - early) * planes,)),
        dma((2, 2, planes - 1)), dma((cus, 2, planes - 1)),
        dma((1,)), dma((1,)), dma((1,)), dma((5,)), dma((5,)),
    ]
    return size, scratch, kinds


def local(offsets, slant_weights, live, block_tile, image_slot):
    shots, grp = lax.axis_size("shot"), lax.axis_size("grp")
    planes = shots // PAIR
    blocks = block_tile.shape[0]
    hs, depth = offsets.shape[1:]
    angles = slant_weights.shape[0]
    images = shots * IMG_DEV * grp
    size, scratch, kinds = buffers(planes, blocks, hs, depth, angles, images)
    args = (offsets, slant_weights, live, block_tile, image_slot)
    if grp == 4 and size + (2 << 20) <= VMEM_LIMIT:
        return fused((planes, grp, scratch, kinds), *args)
    return staged(*args)


def solution(mesh):
    placed = (
        P(("shot", "grp"), None, None),
        P(),
        P(("shot", "grp"), None),
        P(("shot", "grp"), None),
        P(("shot", "grp")),
    )
    return jax.shard_map(
        local, mesh=mesh, in_specs=placed, out_specs=P(("shot", "grp"), None, None), check_vma=False
    )
```

```python
import functools
import math

import jax
import jax.numpy as jnp
from jax import lax
from jax.experimental import pallas as pl
from jax.experimental.pallas import tpu as pltpu
from jax.sharding import PartitionSpec as P

IMG_DEV = 4
PAIR = 2
LANES = 128
UNROLL = 8
MESH = pl.DeviceIdType.MESH
VMEM_LIMIT = 62 * 1024 * 1024
SLANT_UNROLL = 2
STACK_UNROLL = 4
SCHEDULE = {
    "compute": 3.19, "first": {"zv": 7.98, "vz": 14.69}, "begin": 3.59, "start": 15.93, "sub": 2.8,
    "second": 19.16, "hop": {"zv": 14.36, "vz": 19.05}, "third": 32.32, "finish": 0.39,
    "moments": 16.35,
}


def place(grp):
    shot, g = lax.axis_index("shot"), lax.axis_index("grp")
    return lax.div(shot, PAIR), lax.rem(shot, PAIR) * grp + g


def at(plane, spot, grp):
    return (plane * PAIR + lax.div(spot, grp), lax.rem(spot, grp))


def share(spot, width, depth):
    start = spot * width
    return lax.div(start, depth), pl.multiple_of(lax.rem(start, depth), LANES)


def relative(spot, grp, r):
    mid = grp // 2
    pair, rest = lax.div(spot, grp), lax.rem(spot, grp)
    m, c = lax.div(rest, 2), lax.rem(rest, 2)
    rp, rm, rc = r // grp, (r % grp) // 2, r % 2
    pair, m, c = lax.rem(pair + rp, PAIR), lax.rem(m + rm, mid), lax.rem(c + rc, 2)
    return (pair * mid + m) * 2 + c


def orders(grp):
    size = PAIR * grp
    far = list(range(grp + 2, size))
    side = list(range(grp, grp + 2))
    ahead = list(range(2, grp))
    turn = []
    for i in range(max(len(far), len(ahead))):
        for group in (far, side, ahead):
            turn += group[i : i + 1]
    return [1] + turn


def exchange_kernel(
    grp, off, aux, w_in, part, mom, w, raw, aux_in, codes, acc, seg, send, recv, asend, arecv, lsem
):
    size = PAIR * grp
    plane, spot = place(grp)
    blocks, depth, width = off.shape[0], off.shape[3], raw.shape[3]
    angles, images = w.shape[1], acc.shape[0]
    j, first = share(spot, width, depth)
    mine = pltpu.make_async_copy(off.at[:, j, :, pl.ds(first, width)], raw.at[0], lsem.at[0])
    mine.start()
    own_codes = pltpu.make_async_copy(aux, codes.at[0], lsem.at[1])
    own_codes.start()
    weigh = pltpu.make_async_copy(w_in, w, lsem.at[size + 1])
    weigh.start()
    barrier = pltpu.get_barrier_semaphore()
    for r in range(1, size):
        pl.semaphore_signal(
            barrier, inc=1, device_id=at(plane, relative(spot, grp, r), grp), device_id_type=MESH
        )
    pl.semaphore_wait(barrier, size - 1)
    data, notes = {}, {}
    for r in orders(grp):
        peer = relative(spot, grp, r)
        pj, pfirst = share(peer, width, depth)
        dev = at(plane, peer, grp)
        notes[r] = pltpu.make_async_remote_copy(
            src_ref=aux,
            dst_ref=aux_in.at[r],
            send_sem=asend.at[r - 1],
            recv_sem=arecv.at[r - 1],
            device_id=dev,
            device_id_type=MESH,
        )
        data[r] = pltpu.make_async_remote_copy(
            src_ref=off.at[:, pj, :, pl.ds(pfirst, width)],
            dst_ref=raw.at[r],
            send_sem=send.at[r - 1],
            recv_sem=recv.at[r - 1],
            device_id=dev,
            device_id_type=MESH,
        )
    for r in orders(grp):
        notes[r].start()
    for r in orders(grp):
        data[r].start()

    acc[...] = jnp.zeros_like(acc)
    seg[blocks] = jnp.zeros((angles, width), jnp.float32)
    row = lax.broadcasted_iota(jnp.int32, (angles, width), 0)
    weigh.wait()
    weights = w[...].astype(jnp.float32).T.astype(jnp.bfloat16)
    square = jnp.zeros((angles, width), jnp.float32)
    count = jnp.zeros((angles, width), jnp.float32)
    for r in [0] + orders(grp):
        if r:
            notes[r].wait()
            code = pltpu.make_async_copy(aux_in.at[r], codes.at[r], lsem.at[r + 1])
            code.start()
            code.wait()
            data[r].wait()
        else:
            own_codes.wait()
            mine.wait()

        def slant(i, carry, r=r):
            square, count = carry
            start = i * UNROLL
            x = jnp.concatenate([raw[r, start + t] for t in range(UNROLL)], axis=1)
            y = jnp.dot(weights, x, preferred_element_type=jnp.float32)
            for t in range(UNROLL):
                alive = row < codes[r, 1 + j, start + t]
                slanted = jnp.where(alive, y[:, t * width : (t + 1) * width], 0.0)
                slanted = slanted.astype(jnp.bfloat16).astype(jnp.float32)
                square += slanted * slanted
                count += jnp.where(alive, 1.0, 0.0)
                seg[start + t] = slanted + seg[codes[r, 0, start + t]]
            return square, count

        square, count = lax.fori_loop(0, blocks // UNROLL, slant, (square, count))

        def stack(i, _, r=r):
            start = i * UNROLL
            line, column = lax.div(start, LANES), lax.rem(start, LANES)
            for t in range(UNROLL):
                acc[start + t] += seg[codes[r, 3 + line, column + t]]
            return 0

        lax.fori_loop(0, images // UNROLL, stack, 0)

    def narrow(i, _):
        start = pl.multiple_of(i * UNROLL, UNROLL)
        part[pl.ds(start, UNROLL)] = acc[pl.ds(start, UNROLL)].astype(jnp.bfloat16)
        return 0

    lax.fori_loop(0, images // UNROLL, narrow, 0)
    lane = lax.broadcasted_iota(jnp.int32, (angles, LANES), 1)
    square = jnp.sum(square, axis=1, keepdims=True)
    count = jnp.sum(count, axis=1, keepdims=True)
    both = jnp.where(lane == 0, square, jnp.where(lane == 1, count, 0.0))
    both = jnp.concatenate([both, jnp.zeros((LANES - angles, LANES), jnp.float32)], axis=0)
    mom[...] = both.T[: mom.shape[0]]


def gather_kernel(
    grp, part, mom, out, held, total, fin, pin, qin, half_sum, zs, zr, ps, pr, qs, qr, fs, fr, lsem
):
    size = PAIR * grp
    planes = held.shape[1] + 1
    plane, spot = place(grp)
    pieces, rows, angles, width = held.shape[2:]
    depth = out.shape[2]
    chunk = pieces * rows
    lower = jnp.where(plane < planes // 2, 1, 0)
    barrier = pltpu.get_barrier_semaphore()
    for r in range(1, size):
        pl.semaphore_signal(
            barrier, inc=1, device_id=at(plane, lax.rem(spot + r, size), grp), device_id_type=MESH
        )
    for r in range(1, planes):
        pl.semaphore_signal(
            barrier, inc=1, device_id=at(lax.rem(plane + r, planes), spot, grp), device_id_type=MESH
        )
    pl.semaphore_wait(barrier, size + planes - 2)

    def along(up):
        spot_on_line = plane * up + (planes - 1 - plane) * (1 - up)
        following = lax.rem(plane + 2 * up - 1 + planes, planes)
        return 1 - up, spot_on_line, following

    def rows_of(up, s, h):
        target = (planes - 1 - s) * up + s * (1 - up)
        return target * chunk + h * rows

    def hop(up, s, h, source):
        way, _, following = along(up)
        return pltpu.make_async_remote_copy(
            src_ref=source,
            dst_ref=held.at[way, s, h],
            send_sem=zs.at[way, s, h],
            recv_sem=zr.at[way, s, h],
            device_id=at(following, spot, grp),
            device_id_type=MESH,
        )

    def begin(s):
        @pl.when(along(lower)[1] == 0)
        def _():
            for h in range(pieces):
                hop(lower, s, h, part.at[pl.ds(rows_of(lower, s, h), rows)]).start()

    def step(up, s, h):
        way, here, _ = along(up)
        end = planes - 1 - s

        @pl.when((here > 0) & (here <= end))
        def _():
            hop(up, s, h, held.at[way, s, h]).wait_recv()

        @pl.when((here > 0) & (here < end))
        def _():
            start = rows_of(up, s, h)

            def add(i, _):
                value = held[way, s, h, i].astype(jnp.float32) + part[start + i].astype(jnp.float32)
                held[way, s, h, i] = value.astype(jnp.bfloat16)
                return 0

            lax.fori_loop(0, rows, add, 0)
            hop(up, s, h, held.at[way, s, h]).start()

        @pl.when((here > 0) & (here == end))
        def _():
            def add(i, _):
                total[h * rows + i] += held[way, s, h, i].astype(jnp.float32)
                return 0

            lax.fori_loop(0, rows, add, 0)

    def finish(up, s, h):
        way, here, _ = along(up)

        @pl.when(here < planes - 1 - s)
        def _():
            hop(up, s, h, held.at[way, s, h]).wait_send()

    near = [
        pltpu.make_async_remote_copy(
            src_ref=mom,
            dst_ref=pin.at[r - 1],
            send_sem=ps.at[r - 1],
            recv_sem=pr.at[r - 1],
            device_id=at(plane, lax.rem(spot + r, size), grp),
            device_id_type=MESH,
        )
        for r in range(1, size)
    ]
    for copy in near:
        copy.start()
    begin(0)
    total[...] = part[pl.ds(plane * chunk, chunk)].astype(jnp.float32)
    moments = mom[...]
    for copy in near:
        copy.wait()
    for r in range(1, size):
        moments += pin[r - 1]
    half_sum[...] = moments
    wide = [
        pltpu.make_async_remote_copy(
            src_ref=half_sum,
            dst_ref=qin.at[r - 1],
            send_sem=qs.at[r - 1],
            recv_sem=qr.at[r - 1],
            device_id=at(lax.rem(plane + r, planes), spot, grp),
            device_id_type=MESH,
        )
        for r in range(1, planes)
    ]
    for copy in wide:
        copy.start()
    for s in range(1, planes - 1):
        begin(s)
    for s in range(planes - 1):
        for up in (lower, 1 - lower):
            for h in range(pieces):
                step(up, s, h)
    for copy in wide:
        copy.wait()
    moments = half_sum[...]
    for r in range(1, planes):
        moments += qin[r - 1]
    gain = lax.rsqrt(moments[0:1] / moments[1:2] + 1e-06)
    gain = jnp.broadcast_to(gain, (LANES, LANES)).T[:angles]

    def body(i, _):
        fin[i] = (total[i] * gain).astype(jnp.bfloat16)
        return 0

    lax.fori_loop(0, chunk, body, 0)

    each = chunk // size
    j, first = share(spot, width, depth)
    view = out.at[:, pl.ds(pl.multiple_of(j * angles, angles), angles), pl.ds(first, width)]
    last = pltpu.make_async_copy(fin.at[pl.ds(spot * each, each)], view, lsem.at[1])
    final = []
    for r in range(1, size):
        peer = lax.rem(spot + r, size)
        final.append(
            pltpu.make_async_remote_copy(
                src_ref=fin.at[pl.ds(peer * each, each)],
                dst_ref=view,
                send_sem=fs.at[r - 1],
                recv_sem=fr.at[r - 1],
                device_id=at(plane, peer, grp),
                device_id_type=MESH,
            )
        )
    for copy in final:
        copy.start()
    last.start()
    last.wait()
    for copy in final:
        copy.wait()
    for s in range(planes - 1):
        for up in (lower, 1 - lower):
            for h in range(pieces):
                finish(up, s, h)


def staged(offsets, slant_weights, live, block_tile, image_slot):
    shots, grp = lax.axis_size("shot"), lax.axis_size("grp")
    planes, size = shots // PAIR, PAIR * grp
    blocks = block_tile.shape[0]
    hs, depth = offsets.shape[1:]
    angles = slant_weights.shape[0]
    width = 2 * depth // size
    tile_rows = IMG_DEV * grp
    images = shots * tile_rows
    per_plane = images // planes
    any_space = pl.BlockSpec(memory_space=pl.ANY)
    vmem = pl.BlockSpec(memory_space=pltpu.VMEM)
    dma = pltpu.SemaphoreType.DMA

    cutoff = jnp.sum(live.reshape(blocks, 2, angles), axis=2)
    image = block_tile[:, 0] * tile_rows + image_slot
    index = jnp.arange(blocks, dtype=jnp.int32)
    same = (image[:, None] == image[None, :]) & (index[None, :] < index[:, None])
    before = jnp.max(jnp.where(same, index[None, :], -1), axis=1)
    found = image[None, :] == jnp.arange(images, dtype=jnp.int32)[:, None]
    final = jnp.max(jnp.where(found, index[None, :], -1), axis=1)
    final = jnp.where(final < 0, blocks, final).reshape(images // LANES, LANES)
    before = jnp.where(before < 0, blocks, before)
    aux = jnp.concatenate([before[None], cutoff.T], axis=0)
    aux = jnp.concatenate([jnp.pad(aux, ((0, 0), (0, LANES - blocks))), final], axis=0)
    aux = jnp.pad(aux, ((0, -aux.shape[0] % 8), (0, 0)))

    part, mom = pl.pallas_call(
        functools.partial(exchange_kernel, grp),
        out_shape=(
            jax.ShapeDtypeStruct((images, angles, width), jnp.bfloat16),
            jax.ShapeDtypeStruct((8, LANES), jnp.float32),
        ),
        in_specs=[any_space, vmem, any_space],
        out_specs=(vmem, vmem),
        scratch_shapes=[
            pltpu.VMEM((hs, angles), jnp.bfloat16),
            pltpu.VMEM((size, blocks, hs, width), jnp.bfloat16),
            pltpu.VMEM((size,) + aux.shape, jnp.int32),
            pltpu.SMEM((size,) + aux.shape, jnp.int32),
            pltpu.VMEM((images, angles, width), jnp.float32),
            pltpu.VMEM((blocks + 1, angles, width), jnp.float32),
            dma((size - 1,)),
            dma((size - 1,)),
            dma((size - 1,)),
            dma((size - 1,)),
            dma((size + 2,)),
        ],
        compiler_params=pltpu.CompilerParams(
            collective_id=0, has_side_effects=True, vmem_limit_bytes=62 * 1024 * 1024
        ),
        name="exchange",
    )(offsets.reshape(blocks, 2, hs, depth), aux, slant_weights.T)

    moments = (8, LANES)
    pieces = 4
    lines = (2, planes - 1, pieces)
    return pl.pallas_call(
        functools.partial(gather_kernel, grp),
        out_shape=jax.ShapeDtypeStruct((IMG_DEV, 2 * angles, depth), jnp.bfloat16),
        in_specs=[vmem, vmem],
        out_specs=any_space,
        scratch_shapes=[
            pltpu.VMEM(lines + (per_plane // pieces, angles, width), jnp.bfloat16),
            pltpu.VMEM((per_plane, angles, width), jnp.float32),
            pltpu.VMEM((per_plane, angles, width), jnp.bfloat16),
            pltpu.VMEM((size - 1,) + moments, jnp.float32),
            pltpu.VMEM((planes - 1,) + moments, jnp.float32),
            pltpu.VMEM(moments, jnp.float32),
            dma(lines),
            dma(lines),
            dma((size - 1,)),
            dma((size - 1,)),
            dma((planes - 1,)),
            dma((planes - 1,)),
            dma((size - 1,)),
            dma((size - 1,)),
            dma((2,)),
        ],
        compiler_params=pltpu.CompilerParams(
            collective_id=1, has_side_effects=True, vmem_limit_bytes=60 * 1024 * 1024
        ),
        name="gather",
    )(part, mom)


def round_up(value, unit):
    return -(-value // unit) * unit


def fused_kernel(
    shape, off, live_in, tile_in, slot_in, w_in, out,
    live, tile, slot, weights, raw, wb, onehot, mine, theirs, cuts, squares, sl,
    own, part, rx1, rxv, held, ft, fin, sums, pin, gains,
    load_sem, in_sem, core_s, core_r, meta_s, meta_r, s1s, s1r, vs, vr, zs, zr, fs, fr, fl, ms, mr,
):
    planes, grp, kinds = shape
    shot, g = lax.axis_index("shot"), lax.axis_index("grp")
    z, y = lax.div(shot, PAIR), lax.rem(shot, PAIR)
    x, c = lax.div(g, 2), lax.rem(g, 2)
    blocks, hs, depth = raw.shape[1:]
    angles = live.shape[0]
    images = onehot.shape[0]
    img_dev = out.shape[0]
    per, wide = sl.shape[1], sl.shape[3]
    pairs = per // 2
    depths, groups = depth // wide, angles // per
    cus = depths * groups
    early = 2 * kinds.count("zv")
    late_count = 2 * cus - early

    def device(step=0, fy=False, fx=False, fc=False):
        yy = 1 - y if fy else y
        xx = 1 - x if fx else x
        cc = 1 - c if fc else c
        return ((z + step) * PAIR + yy, xx * 2 + cc)

    core_peer, x_peer, y_peer = device(fc=True), device(fx=True), device(fy=True)
    first_peer = (x_peer, y_peer)
    second_peer = (y_peer, x_peer)

    def remote(src, dst, send_sem, recv_sem, peer):
        return pltpu.make_async_remote_copy(
            src_ref=src, dst_ref=dst, send_sem=send_sem, recv_sem=recv_sem,
            device_id=peer, device_id_type=MESH,
        )

    barrier = pltpu.get_barrier_semaphore()

    def greet(peer):
        pl.semaphore_signal(barrier, inc=1, device_id=peer, device_id_type=MESH)

    for peer in (core_peer, x_peer, y_peer):
        greet(peer)

    @pl.when(z > 0)
    def _():
        greet(device(step=-1))

    @pl.when(z < planes - 1)
    def _():
        greet(device(step=1))

    loads = [
        pltpu.make_async_copy(src, dst, load_sem.at[n])
        for n, (src, dst) in enumerate(
            ((w_in, weights), (live_in, live), (tile_in, tile), (slot_in, slot))
        )
    ]
    for copy in loads:
        copy.start()
    own_in = [
        pltpu.make_async_copy(
            off.at[:, c, :, pl.ds(d * wide, wide)],
            raw.at[0, :, :, pl.ds(d * wide, wide)],
            in_sem.at[d],
        )
        for d in range(depths)
    ]
    for copy in own_in:
        copy.start()
    core_in = [
        remote(
            off.at[:, 1 - c, :, pl.ds(d * wide, wide)],
            raw.at[1, :, :, pl.ds(d * wide, wide)],
            core_s.at[d], core_r.at[d], core_peer,
        )
        for d in range(depths)
    ]
    meta = remote(mine, theirs, meta_s.at[0], meta_r.at[0], core_peer)

    eight = 8
    for copy in loads:
        copy.wait()
    ones = jnp.ones((angles, LANES), jnp.bfloat16)
    spot = lax.broadcasted_iota(jnp.int32, (blocks, 2 * blocks), 1)
    block = lax.broadcasted_iota(jnp.int32, (blocks, 2 * blocks), 0)

    def cutoff(j):
        pick = jnp.where(spot == 2 * block + j, 1.0, 0.0).astype(jnp.bfloat16)
        flags = lax.dot_general(
            pick, live[...].astype(jnp.float32).astype(jnp.bfloat16),
            (((1,), (1,)), ((), ())), preferred_element_type=jnp.float32,
        )
        total = jnp.dot(flags.astype(jnp.bfloat16), ones, preferred_element_type=jnp.float32)
        return total.astype(jnp.int32)

    mine[0:eight] = jnp.full((eight, LANES), -1, jnp.int32)
    mine[0:1, 0:blocks] = tile[...] * (img_dev * grp) + slot[...]
    mine[eight : eight + blocks] = cutoff(1 - c)
    cuts[0] = cutoff(c)

    ends = jnp.where(z == 0, 1, 0) + jnp.where(z == planes - 1, 1, 0)
    pl.semaphore_wait(barrier, 5 - ends)
    core_in[0].start()
    meta.start()
    for copy in core_in[1:]:
        copy.start()

    rows = angles * eight
    spread = lax.broadcasted_iota(jnp.int32, (rows, angles), 0)
    which = lax.broadcasted_iota(jnp.int32, (rows, angles), 1)
    pick = jnp.where(lax.div(spread, eight) == which, 1.0, 0.0).astype(jnp.bfloat16)
    tall = lax.dot_general(
        pick, weights[...], (((1,), (1,)), ((), ())), preferred_element_type=jnp.float32
    ).astype(jnp.bfloat16)
    line = lax.broadcasted_iota(jnp.int32, (hs, eight * hs), 0)
    column = lax.broadcasted_iota(jnp.int32, (hs, eight * hs), 1)
    copies = jnp.where(lax.rem(column, hs) == line, 1.0, 0.0).astype(jnp.bfloat16)
    full = jnp.dot(tall, copies, preferred_element_type=jnp.float32)
    line = lax.broadcasted_iota(jnp.int32, full.shape, 0)
    column = lax.broadcasted_iota(jnp.int32, full.shape, 1)
    wb[...] = jnp.where(lax.rem(line, eight) == lax.div(column, hs), full, 0.0).astype(jnp.bfloat16)
    squares[...] = jnp.zeros_like(squares)

    def slant(cu, r):
        d, a0 = cu // groups, cu % groups * per
        if r == 0 and cu % groups == 0:
            own_in[d].wait()
        if r == 1 and cu == 0:
            meta.wait_recv()
            cuts[1] = theirs[eight : eight + blocks]
            select_rows()
        if r == 1 and cu % groups == 0:
            core_in[d].wait_recv()

        def body(i, _):
            lhs = wb[a0 * eight : (a0 + per) * eight]
            lanes = slice(d * wide, (d + 1) * wide)
            a = lax.broadcasted_iota(jnp.int32, (per, 2 * eight, LANES), 0) + a0
            total = squares[a0 : a0 + per]
            for n in range(SLANT_UNROLL):
                start = (i * SLANT_UNROLL + n) * 2 * eight
                alive = cuts[r, pl.ds(start, 2 * eight)][None] > a
                ys = []
                for k in range(2):
                    data = raw[r, pl.ds(start + k * eight, eight), :, lanes]
                    data = data.reshape(eight * hs, wide)
                    y = jnp.dot(lhs, data, preferred_element_type=jnp.float32)
                    ys.append(y.reshape(per, eight, wide))
                for k in range(wide // LANES):
                    cut = slice(k * LANES, (k + 1) * LANES)
                    v = jnp.concatenate([ys[0][:, :, cut], ys[1][:, :, cut]], axis=1)
                    v = jnp.where(alive, v, 0.0)
                    q = v * v
                    total += q[:, :eight] + q[:, eight:]
                    sl[cu % 2, :, pl.ds(r * blocks + start, 2 * eight), cut] = v.astype(jnp.bfloat16)
            squares[a0 : a0 + per] = total
            return 0

        lax.fori_loop(0, blocks // (2 * eight * SLANT_UNROLL), body, 0)

    def select_rows():
        lanes = round_up(2 * blocks, LANES)
        rest = jnp.full((eight, lanes - LANES), -1, jnp.int32)
        a_row = jnp.concatenate([jnp.broadcast_to(mine[0:1], (eight, LANES)), rest], axis=1)
        b_row = jnp.concatenate([jnp.broadcast_to(theirs[0:1], (eight, LANES)), rest], axis=1)
        b_row = pltpu.roll(b_row, blocks, 1)
        lane = lax.broadcasted_iota(jnp.int32, a_row.shape, 1)
        row = jnp.where(lane < blocks, a_row, b_row)
        mask = y * (img_dev * grp) + g * img_dev
        row = lax.bitwise_xor(row, jnp.full(row.shape, 0, jnp.int32) + mask)
        number = lax.broadcasted_iota(jnp.int32, (images, lanes), 0)
        hit = jnp.where(number == row[0:1], 1.0, 0.0).astype(jnp.bfloat16)
        onehot[...] = hit[:, : 2 * blocks]

    def stack(cu):
        def body(i, _):
            for n in range(STACK_UNROLL):
                m = i * STACK_UNROLL + n
                ys = [
                    jnp.dot(onehot[...], sl[cu % 2, 2 * m + k], preferred_element_type=jnp.float32)
                    for k in range(2)
                ]
                for l in range(2):
                    p = 2 * cu + l
                    cut = slice(l * LANES, (l + 1) * LANES)
                    for t in range(planes):
                        for ry in range(2):
                            for rx in range(2):
                                r = ((t * 2 + ry) * 2 + rx) * eight
                                v = [ys[k][r : r + eight, cut] for k in range(2)]
                                v = jnp.concatenate(v, axis=0)
                                one, two = (rx, ry) if l == 0 else (ry, rx)
                                if one == 0:
                                    own[p, t, two, m] = v
                                else:
                                    part[p, t, two, m] = v.astype(jnp.bfloat16)
            return 0

        lax.fori_loop(0, pairs // STACK_UNROLL, body, 0)

    def late(cu):
        return kinds[cu] == "vz"

    def s1(cu, l, t):
        p = 2 * cu + l
        return remote(part.at[p, t], rx1.at[p, t], s1s.at[0], s1r.at[cu, t], first_peer[l])

    def across_slot(cu, t):
        return early // 2 + (cu - early // 2) * planes + t if late(cu) else cu

    def across(cu, l, t, source):
        p, slot = 2 * cu + l, across_slot(cu, t)
        kind = 1 if late(cu) else 0
        return remote(source, rxv.at[p, t], vs.at[kind], vr.at[slot], second_peer[l])

    def arrived(region, sem):
        remote(region, region, ms.at[0], sem, core_peer).wait_recv()

    def hop(cu, way, s, source):
        p, n = pl.ds(2 * cu, 2), pl.ds(0, 1 if late(cu) else 2)
        kind = 1 if late(cu) else 0
        return remote(
            source, held.at[p, way, s, n], zs.at[kind, way, s], zr.at[cu, way, s],
            device(step=1 - 2 * way),
        )

    def begin(cu, t):
        source = rx1.at[pl.ds(2 * cu, 2), t, pl.ds(0, 1 if late(cu) else 2)]
        if t > 0:
            @pl.when(z == 0)
            def _():
                hop(cu, 0, planes - 1 - t, source).start()
        if t < planes - 1:
            @pl.when(z == planes - 1)
            def _():
                hop(cu, 1, t, source).start()

    def start(cu):
        for t in far_first(planes):
            for l in range(2):
                s1(cu, l, t).start()

    def first(cu, t):
        arrived(rx1.at[pl.ds(2 * cu, 2), t], s1r.at[cu, t])
        for l in range(2):
            p = 2 * cu + l
            for k in (1, 0):
                total = own[p, t, k] + rx1[p, t, k].astype(jnp.float32)
                own[p, t, k] = total
                rx1[p, t, k] = total.astype(jnp.bfloat16)
            if late(cu):
                across(cu, l, t, rx1.at[p, t, 1]).start()
        if not late(cu):
            begin(cu, t)

    def second(cu, t):
        arrived(rxv.at[pl.ds(2 * cu, 2), t], vr.at[across_slot(cu, t)])
        for l in range(2):
            p = 2 * cu + l
            total = own[p, t, 0] + rxv[p, t].astype(jnp.float32)
            own[p, t, 0] = total
            rx1[p, t, 0] = total.astype(jnp.bfloat16)
        begin(cu, t)

    def tick(cu, tau, way):
        here = z if way == 0 else planes - 1 - z
        s = tau - here
        target = planes - 1 - s if way == 0 else s
        n = 1 if late(cu) else 2

        @pl.when((here >= 1) & (s >= 0))
        def _():
            message = held.at[pl.ds(2 * cu, 2), way, s, pl.ds(0, n)]
            hop(cu, way, s, message).wait_recv()
            for l in range(2):
                p = 2 * cu + l
                for k in range(n):
                    value = held[p, way, s, k].astype(jnp.float32) + own[p, target, k]
                    if tau < planes - 1:
                        held[p, way, s, k] = value.astype(jnp.bfloat16)
                    else:
                        own[p, target, k] = value
            if tau < planes - 1:
                hop(cu, way, s, message).start()

    def third(cu):
        for l in range(2):
            p = 2 * cu + l
            rx1[p, z, 1] = own[p, z, 1].astype(jnp.bfloat16)
            across(cu, l, 0, rx1.at[p, z, 1]).start()

    def leave(line, lanes):
        row = pl.multiple_of(c * angles + line.start, per)
        view = out.at[:, pl.ds(row, line.size), pl.ds(lanes.start, lanes.size)]
        send = remote(fin.at[pl.ds(img_dev, img_dev), line, lanes], view, fs.at[0], fr.at[0], core_peer)
        keep = pltpu.make_async_copy(fin.at[pl.ds(0, img_dev), line, lanes], view, fl.at[0])
        return send, keep

    def finish(cu):
        if not late(cu):
            arrived(rxv.at[pl.ds(2 * cu, 2), 0], vr.at[across_slot(cu, 0)])
        a0, lane0 = cu % groups * per, cu // groups * wide
        for l in range(2):
            p = 2 * cu + l
            total = own[p, z, 0]
            if not late(cu):
                total += rxv[p, 0].astype(jnp.float32)
            ft[l] = total.reshape(per * eight, LANES)
            lanes = slice(lane0 + l * LANES, lane0 + (l + 1) * LANES)
            for r in range(eight):
                v = ft[l, pl.ds(r, per, stride=eight)] * gains[a0 : a0 + per]
                fin[r, a0 : a0 + per, lanes] = v.astype(jnp.bfloat16)
        for copy in leave(pl.ds(a0, per), pl.ds(lane0, wide)):
            copy.start()

    def moment(stage):
        peer = (core_peer, x_peer, y_peer)[stage]
        return remote(sums.at[stage], pin.at[stage], ms.at[stage], mr.at[stage], peer)

    def passing(way):
        n = 3 + way
        return remote(sums.at[n + 1], pin.at[n], ms.at[n], mr.at[n], device(step=1 - 2 * way))

    def moments(stage):
        if stage == 0:
            total = jnp.sum(jnp.sum(squares[...], axis=1), axis=1, keepdims=True)
            count = jnp.sum(live[...].astype(jnp.float32), axis=1, keepdims=True)
            lane = lax.broadcasted_iota(jnp.int32, (angles, LANES), 1)
            both = jnp.where(lane == 0, total, jnp.where(lane == 1, count, 0.0))
            both = jnp.concatenate([both, jnp.zeros((LANES - angles, LANES), jnp.float32)], axis=0)
            sums[0] = both.T[:eight]
            moment(0).start()
            return
        if stage <= 3:
            moment(stage - 1).wait_recv()
            sums[stage] = sums[stage - 1] + pin[stage - 1]
            if stage < 3:
                moment(stage).start()
                return
            sums[6] = sums[3]
        tau = stage - 3
        if tau < planes:
            for way in range(2):
                here = z if way == 0 else planes - 1 - z

                @pl.when(here == tau)
                def _(way=way):
                    if tau > 0:
                        passing(way).wait_recv()
                        sums[6] = sums[6] + pin[3 + way]
                        sums[4 + way] = sums[3] + pin[3 + way]
                    else:
                        sums[4 + way] = sums[3]
                    if tau < planes - 1:
                        passing(way).start()
        else:
            total = sums[6]
            gain = lax.rsqrt(total[0:1] / (depth * total[1:2]) + 1e-06)
            gains[...] = jnp.broadcast_to(gain, (LANES, LANES)).T[:angles]

    run = {
        "slant": slant, "stack": stack, "start": start, "first": first, "second": second,
        "tick": tick, "third": third, "finish": finish, "moments": moments,
    }
    for _, action in sorted(schedule(planes, kinds), key=lambda e: e[0]):
        run[action[0]](*action[1:])

    meta.wait_send()
    for copy in core_in:
        copy.wait_send()
    remote(part, rx1, s1s.at[0], s1r.at[0, 0], core_peer).wait_send()
    if early:
        region = rxv.at[pl.ds(0, early), 0]
        remote(region, region, vs.at[0], vr.at[0], core_peer).wait_send()
    if late_count:
        region = rxv.at[pl.ds(early, late_count)]
        remote(region, region, vs.at[1], vr.at[0], core_peer).wait_send()
    for way in range(2):
        here = z if way == 0 else planes - 1 - z

        @pl.when(here < planes - 1)
        def _(way=way):
            passing(way).wait_send()

        for s in range(planes - 1):
            @pl.when(here < planes - 1 - s)
            def _(way=way, s=s):
                for kind, region in enumerate(
                    (
                        held.at[pl.ds(0, early), way, s],
                        held.at[pl.ds(early, late_count), way, s, pl.ds(0, 1)],
                    )
                ):
                    if (early, late_count)[kind]:
                        remote(
                            region, region, zs.at[kind, way, s], zr.at[0, way, s], core_peer
                        ).wait_send()
    for stage in range(3):
        moment(stage).wait_send()
    send, keep = leave(pl.ds(0, angles), pl.ds(0, depth))
    keep.wait()
    send.wait()


def far_first(planes):
    return [planes - 1 - i // 2 if i % 2 == 0 else i // 2 for i in range(planes)]


def schedule(planes, kinds):
    compute, spacing, lag, sub = SCHEDULE["compute"], SCHEDULE["first"], SCHEDULE["start"], SCHEDULE["sub"]
    cus = len(kinds)
    events = [(-2.0, ("slant", 0, 0)), (-1.0, ("slant", 1, 0))]
    for cu in range(cus):
        at = compute * cu
        if cu > 1:
            events.append((at, ("slant", cu, 0)))
        events.append((at + 0.1 * compute, ("slant", cu, 1)))
        events.append((at + 0.2 * compute, ("stack", cu)))
    done = compute * cus
    for stage in range(3 + planes + 1):
        events.append((done + SCHEDULE["moments"] * stage, ("moments", stage)))
    gain = done + SCHEDULE["moments"] * (3 + planes) + 0.1
    now = SCHEDULE["begin"]
    for cu, kind in enumerate(kinds):
        at = now
        events.append((max(compute * cu + 0.3 * compute, at - lag), ("start", cu)))
        at = max(at, compute * cu + 0.3 * compute + 0.1)
        for i, t in enumerate(far_first(planes)):
            events.append((at + i * sub, ("first", cu, t)))
        now += spacing[kind]
        at += (planes - 1) * sub
        if kind == "vz":
            at += SCHEDULE["second"] - (planes - 1) * sub
            for i, t in enumerate(far_first(planes)):
                events.append((at + i * sub, ("second", cu, t)))
            at += (planes - 1) * sub
        for tau in range(1, planes):
            at += SCHEDULE["hop"][kind]
            for way in range(2):
                events.append((at, ("tick", cu, tau, way)))
        if kind == "zv":
            at += SCHEDULE["third"]
            events.append((at, ("third", cu)))
            at += SCHEDULE["finish"]
        events.append((max(at + 0.01, gain), ("finish", cu)))
    return events


def fused(shapes, offsets, slant_weights, live, block_tile, image_slot):
    planes, grp, scratch, kinds = shapes
    blocks = block_tile.shape[0]
    hs, depth = offsets.shape[1:]
    angles = slant_weights.shape[0]
    any_space = pl.BlockSpec(memory_space=pl.ANY)
    return pl.pallas_call(
        functools.partial(fused_kernel, (planes, grp, kinds)),
        out_shape=jax.ShapeDtypeStruct((IMG_DEV, 2 * angles, depth), jnp.bfloat16),
        in_specs=[any_space] * 5,
        out_specs=any_space,
        scratch_shapes=scratch,
        compiler_params=pltpu.CompilerParams(
            collective_id=2, has_side_effects=True, vmem_limit_bytes=VMEM_LIMIT
        ),
        name="calibrated_stack",
    )(
        offsets.reshape(blocks, 2, hs, depth),
        live.T,
        block_tile.reshape(1, blocks),
        image_slot.reshape(1, blocks),
        slant_weights.T,
    )


def buffers(planes, blocks, hs, depth, angles, images):
    wide, per = 2 * LANES, 16
    cus = (depth // wide) * (angles // per)
    pieces = 2 * cus
    tile = (per // 2, 16, LANES)
    dma = pltpu.SemaphoreType.DMA
    bf, f32, i32 = jnp.bfloat16, jnp.float32, jnp.int32
    early = (5 * cus + 4) // 8
    kinds = ("zv",) * early + ("vz",) * (cus - early)
    memory = [
        ((angles, 2 * blocks), i32),
        ((1, blocks), i32),
        ((1, blocks), i32),
        ((hs, angles), bf),
        ((2, blocks, hs, depth), bf),
        ((angles * 8, 8 * hs), bf),
        ((images, 2 * blocks), bf),
        ((8 + blocks, LANES), i32),
        ((8 + blocks, LANES), i32),
        ((2, blocks, LANES), i32),
        ((angles, 8, LANES), f32),
        ((2, per, 2 * blocks, wide), bf),
        ((pieces, planes, 2) + tile, f32),
        ((pieces, planes, 2) + tile, bf),
        ((pieces, planes, 2) + tile, bf),
        ((pieces, planes) + tile, bf),
        ((pieces, 2, planes - 1, 2) + tile, bf),
        ((2, per * 8, LANES), f32),
        ((2 * IMG_DEV, angles, depth), bf),
        ((7, 8, LANES), f32),
        ((5, 8, LANES), f32),
        ((angles, LANES), f32),
    ]
    size = sum(math.prod(s) * jnp.dtype(d).itemsize for s, d in memory)
    scratch = [pltpu.VMEM(s, d) for s, d in memory]
    depths = depth // wide
    scratch += [
        dma((4,)), dma((depths,)), dma((depths,)), dma((depths,)), dma((1,)), dma((1,)),
        dma((1,)), dma((cus, planes)),
        dma((2,)), dma((early + (cus - early) * planes,)),
        dma((2, 2, planes - 1)), dma((cus, 2, planes - 1)),
        dma((1,)), dma((1,)), dma((1,)), dma((5,)), dma((5,)),
    ]
    return size, scratch, kinds


def local(offsets, slant_weights, live, block_tile, image_slot):
    shots, grp = lax.axis_size("shot"), lax.axis_size("grp")
    planes = shots // PAIR
    blocks = block_tile.shape[0]
    hs, depth = offsets.shape[1:]
    angles = slant_weights.shape[0]
    images = shots * IMG_DEV * grp
    size, scratch, kinds = buffers(planes, blocks, hs, depth, angles, images)
    args = (offsets, slant_weights, live, block_tile, image_slot)
    if grp == 4 and size + (2 << 20) <= VMEM_LIMIT:
        return fused((planes, grp, scratch, kinds), *args)
    return staged(*args)


def solution(mesh):
    placed = (
        P(("shot", "grp"), None, None),
        P(),
        P(("shot", "grp"), None),
        P(("shot", "grp"), None),
        P(("shot", "grp")),
    )
    return jax.shard_map(
        local, mesh=mesh, in_specs=placed, out_specs=P(("shot", "grp"), None, None), check_vma=False
    )
```

```python
import functools
import math

import jax
import jax.numpy as jnp
from jax import lax
from jax.experimental import pallas as pl
from jax.experimental.pallas import tpu as pltpu
from jax.sharding import PartitionSpec as P

IMG_DEV = 4
PAIR = 2
LANES = 128
UNROLL = 8
MESH = pl.DeviceIdType.MESH
VMEM_LIMIT = 62 * 1024 * 1024
SLANT_UNROLL = 2
STACK_UNROLL = 4
SCHEDULE = {
    "compute": 3.19, "first": {"zv": 7.98, "vz": 14.69}, "begin": 3.59, "start": 15.93, "sub": 2.8,
    "second": 19.16, "hop": {"zv": 14.36, "vz": 19.05}, "third": 32.32, "finish": 0.39,
    "moments": 16.35,
}


def place(grp):
    shot, g = lax.axis_index("shot"), lax.axis_index("grp")
    return lax.div(shot, PAIR), lax.rem(shot, PAIR) * grp + g


def at(plane, spot, grp):
    return (plane * PAIR + lax.div(spot, grp), lax.rem(spot, grp))


def share(spot, width, depth):
    start = spot * width
    return lax.div(start, depth), pl.multiple_of(lax.rem(start, depth), LANES)


def relative(spot, grp, r):
    mid = grp // 2
    pair, rest = lax.div(spot, grp), lax.rem(spot, grp)
    m, c = lax.div(rest, 2), lax.rem(rest, 2)
    rp, rm, rc = r // grp, (r % grp) // 2, r % 2
    pair, m, c = lax.rem(pair + rp, PAIR), lax.rem(m + rm, mid), lax.rem(c + rc, 2)
    return (pair * mid + m) * 2 + c


def orders(grp):
    size = PAIR * grp
    far = list(range(grp + 2, size))
    side = list(range(grp, grp + 2))
    ahead = list(range(2, grp))
    turn = []
    for i in range(max(len(far), len(ahead))):
        for group in (far, side, ahead):
            turn += group[i : i + 1]
    return [1] + turn


def exchange_kernel(
    grp, off, aux, w_in, part, mom, w, raw, aux_in, codes, acc, seg, send, recv, asend, arecv, lsem
):
    size = PAIR * grp
    plane, spot = place(grp)
    blocks, depth, width = off.shape[0], off.shape[3], raw.shape[3]
    angles, images = w.shape[1], acc.shape[0]
    j, first = share(spot, width, depth)
    mine = pltpu.make_async_copy(off.at[:, j, :, pl.ds(first, width)], raw.at[0], lsem.at[0])
    mine.start()
    own_codes = pltpu.make_async_copy(aux, codes.at[0], lsem.at[1])
    own_codes.start()
    weigh = pltpu.make_async_copy(w_in, w, lsem.at[size + 1])
    weigh.start()
    barrier = pltpu.get_barrier_semaphore()
    for r in range(1, size):
        pl.semaphore_signal(
            barrier, inc=1, device_id=at(plane, relative(spot, grp, r), grp), device_id_type=MESH
        )
    pl.semaphore_wait(barrier, size - 1)
    data, notes = {}, {}
    for r in orders(grp):
        peer = relative(spot, grp, r)
        pj, pfirst = share(peer, width, depth)
        dev = at(plane, peer, grp)
        notes[r] = pltpu.make_async_remote_copy(
            src_ref=aux,
            dst_ref=aux_in.at[r],
            send_sem=asend.at[r - 1],
            recv_sem=arecv.at[r - 1],
            device_id=dev,
            device_id_type=MESH,
        )
        data[r] = pltpu.make_async_remote_copy(
            src_ref=off.at[:, pj, :, pl.ds(pfirst, width)],
            dst_ref=raw.at[r],
            send_sem=send.at[r - 1],
            recv_sem=recv.at[r - 1],
            device_id=dev,
            device_id_type=MESH,
        )
    for r in orders(grp):
        notes[r].start()
    for r in orders(grp):
        data[r].start()

    acc[...] = jnp.zeros_like(acc)
    seg[blocks] = jnp.zeros((angles, width), jnp.float32)
    row = lax.broadcasted_iota(jnp.int32, (angles, width), 0)
    weigh.wait()
    weights = w[...].astype(jnp.float32).T.astype(jnp.bfloat16)
    square = jnp.zeros((angles, width), jnp.float32)
    count = jnp.zeros((angles, width), jnp.float32)
    for r in [0] + orders(grp):
        if r:
            notes[r].wait()
            code = pltpu.make_async_copy(aux_in.at[r], codes.at[r], lsem.at[r + 1])
            code.start()
            code.wait()
            data[r].wait()
        else:
            own_codes.wait()
            mine.wait()

        def slant(i, carry, r=r):
            square, count = carry
            start = i * UNROLL
            x = jnp.concatenate([raw[r, start + t] for t in range(UNROLL)], axis=1)
            y = jnp.dot(weights, x, preferred_element_type=jnp.float32)
            for t in range(UNROLL):
                alive = row < codes[r, 1 + j, start + t]
                slanted = jnp.where(alive, y[:, t * width : (t + 1) * width], 0.0)
                slanted = slanted.astype(jnp.bfloat16).astype(jnp.float32)
                square += slanted * slanted
                count += jnp.where(alive, 1.0, 0.0)
                seg[start + t] = slanted + seg[codes[r, 0, start + t]]
            return square, count

        square, count = lax.fori_loop(0, blocks // UNROLL, slant, (square, count))

        def stack(i, _, r=r):
            start = i * UNROLL
            line, column = lax.div(start, LANES), lax.rem(start, LANES)
            for t in range(UNROLL):
                acc[start + t] += seg[codes[r, 3 + line, column + t]]
            return 0

        lax.fori_loop(0, images // UNROLL, stack, 0)

    def narrow(i, _):
        start = pl.multiple_of(i * UNROLL, UNROLL)
        part[pl.ds(start, UNROLL)] = acc[pl.ds(start, UNROLL)].astype(jnp.bfloat16)
        return 0

    lax.fori_loop(0, images // UNROLL, narrow, 0)
    lane = lax.broadcasted_iota(jnp.int32, (angles, LANES), 1)
    square = jnp.sum(square, axis=1, keepdims=True)
    count = jnp.sum(count, axis=1, keepdims=True)
    both = jnp.where(lane == 0, square, jnp.where(lane == 1, count, 0.0))
    both = jnp.concatenate([both, jnp.zeros((LANES - angles, LANES), jnp.float32)], axis=0)
    mom[...] = both.T[: mom.shape[0]]


def gather_kernel(
    grp, part, mom, out, held, total, fin, pin, qin, half_sum, zs, zr, ps, pr, qs, qr, fs, fr, lsem
):
    size = PAIR * grp
    planes = held.shape[1] + 1
    plane, spot = place(grp)
    pieces, rows, angles, width = held.shape[2:]
    depth = out.shape[2]
    chunk = pieces * rows
    lower = jnp.where(plane < planes // 2, 1, 0)
    barrier = pltpu.get_barrier_semaphore()
    for r in range(1, size):
        pl.semaphore_signal(
            barrier, inc=1, device_id=at(plane, lax.rem(spot + r, size), grp), device_id_type=MESH
        )
    for r in range(1, planes):
        pl.semaphore_signal(
            barrier, inc=1, device_id=at(lax.rem(plane + r, planes), spot, grp), device_id_type=MESH
        )
    pl.semaphore_wait(barrier, size + planes - 2)

    def along(up):
        spot_on_line = plane * up + (planes - 1 - plane) * (1 - up)
        following = lax.rem(plane + 2 * up - 1 + planes, planes)
        return 1 - up, spot_on_line, following

    def rows_of(up, s, h):
        target = (planes - 1 - s) * up + s * (1 - up)
        return target * chunk + h * rows

    def hop(up, s, h, source):
        way, _, following = along(up)
        return pltpu.make_async_remote_copy(
            src_ref=source,
            dst_ref=held.at[way, s, h],
            send_sem=zs.at[way, s, h],
            recv_sem=zr.at[way, s, h],
            device_id=at(following, spot, grp),
            device_id_type=MESH,
        )

    def begin(s):
        @pl.when(along(lower)[1] == 0)
        def _():
            for h in range(pieces):
                hop(lower, s, h, part.at[pl.ds(rows_of(lower, s, h), rows)]).start()

    def step(up, s, h):
        way, here, _ = along(up)
        end = planes - 1 - s

        @pl.when((here > 0) & (here <= end))
        def _():
            hop(up, s, h, held.at[way, s, h]).wait_recv()

        @pl.when((here > 0) & (here < end))
        def _():
            start = rows_of(up, s, h)

            def add(i, _):
                value = held[way, s, h, i].astype(jnp.float32) + part[start + i].astype(jnp.float32)
                held[way, s, h, i] = value.astype(jnp.bfloat16)
                return 0

            lax.fori_loop(0, rows, add, 0)
            hop(up, s, h, held.at[way, s, h]).start()

        @pl.when((here > 0) & (here == end))
        def _():
            def add(i, _):
                total[h * rows + i] += held[way, s, h, i].astype(jnp.float32)
                return 0

            lax.fori_loop(0, rows, add, 0)

    def finish(up, s, h):
        way, here, _ = along(up)

        @pl.when(here < planes - 1 - s)
        def _():
            hop(up, s, h, held.at[way, s, h]).wait_send()

    near = [
        pltpu.make_async_remote_copy(
            src_ref=mom,
            dst_ref=pin.at[r - 1],
            send_sem=ps.at[r - 1],
            recv_sem=pr.at[r - 1],
            device_id=at(plane, lax.rem(spot + r, size), grp),
            device_id_type=MESH,
        )
        for r in range(1, size)
    ]
    for copy in near:
        copy.start()
    begin(0)
    total[...] = part[pl.ds(plane * chunk, chunk)].astype(jnp.float32)
    moments = mom[...]
    for copy in near:
        copy.wait()
    for r in range(1, size):
        moments += pin[r - 1]
    half_sum[...] = moments
    wide = [
        pltpu.make_async_remote_copy(
            src_ref=half_sum,
            dst_ref=qin.at[r - 1],
            send_sem=qs.at[r - 1],
            recv_sem=qr.at[r - 1],
            device_id=at(lax.rem(plane + r, planes), spot, grp),
            device_id_type=MESH,
        )
        for r in range(1, planes)
    ]
    for copy in wide:
        copy.start()
    for s in range(1, planes - 1):
        begin(s)
    for s in range(planes - 1):
        for up in (lower, 1 - lower):
            for h in range(pieces):
                step(up, s, h)
    for copy in wide:
        copy.wait()
    moments = half_sum[...]
    for r in range(1, planes):
        moments += qin[r - 1]
    gain = lax.rsqrt(moments[0:1] / moments[1:2] + 1e-06)
    gain = jnp.broadcast_to(gain, (LANES, LANES)).T[:angles]

    def body(i, _):
        fin[i] = (total[i] * gain).astype(jnp.bfloat16)
        return 0

    lax.fori_loop(0, chunk, body, 0)

    each = chunk // size
    j, first = share(spot, width, depth)
    view = out.at[:, pl.ds(pl.multiple_of(j * angles, angles), angles), pl.ds(first, width)]
    last = pltpu.make_async_copy(fin.at[pl.ds(spot * each, each)], view, lsem.at[1])
    final = []
    for r in range(1, size):
        peer = lax.rem(spot + r, size)
        final.append(
            pltpu.make_async_remote_copy(
                src_ref=fin.at[pl.ds(peer * each, each)],
                dst_ref=view,
                send_sem=fs.at[r - 1],
                recv_sem=fr.at[r - 1],
                device_id=at(plane, peer, grp),
                device_id_type=MESH,
            )
        )
    for copy in final:
        copy.start()
    last.start()
    last.wait()
    for copy in final:
        copy.wait()
    for s in range(planes - 1):
        for up in (lower, 1 - lower):
            for h in range(pieces):
                finish(up, s, h)


def staged(offsets, slant_weights, live, block_tile, image_slot):
    shots, grp = lax.axis_size("shot"), lax.axis_size("grp")
    planes, size = shots // PAIR, PAIR * grp
    blocks = block_tile.shape[0]
    hs, depth = offsets.shape[1:]
    angles = slant_weights.shape[0]
    width = 2 * depth // size
    tile_rows = IMG_DEV * grp
    images = shots * tile_rows
    per_plane = images // planes
    any_space = pl.BlockSpec(memory_space=pl.ANY)
    vmem = pl.BlockSpec(memory_space=pltpu.VMEM)
    dma = pltpu.SemaphoreType.DMA

    cutoff = jnp.sum(live.reshape(blocks, 2, angles), axis=2)
    image = block_tile[:, 0] * tile_rows + image_slot
    index = jnp.arange(blocks, dtype=jnp.int32)
    same = (image[:, None] == image[None, :]) & (index[None, :] < index[:, None])
    before = jnp.max(jnp.where(same, index[None, :], -1), axis=1)
    found = image[None, :] == jnp.arange(images, dtype=jnp.int32)[:, None]
    final = jnp.max(jnp.where(found, index[None, :], -1), axis=1)
    final = jnp.where(final < 0, blocks, final).reshape(images // LANES, LANES)
    before = jnp.where(before < 0, blocks, before)
    aux = jnp.concatenate([before[None], cutoff.T], axis=0)
    aux = jnp.concatenate([jnp.pad(aux, ((0, 0), (0, LANES - blocks))), final], axis=0)
    aux = jnp.pad(aux, ((0, -aux.shape[0] % 8), (0, 0)))

    part, mom = pl.pallas_call(
        functools.partial(exchange_kernel, grp),
        out_shape=(
            jax.ShapeDtypeStruct((images, angles, width), jnp.bfloat16),
            jax.ShapeDtypeStruct((8, LANES), jnp.float32),
        ),
        in_specs=[any_space, vmem, any_space],
        out_specs=(vmem, vmem),
        scratch_shapes=[
            pltpu.VMEM((hs, angles), jnp.bfloat16),
            pltpu.VMEM((size, blocks, hs, width), jnp.bfloat16),
            pltpu.VMEM((size,) + aux.shape, jnp.int32),
            pltpu.SMEM((size,) + aux.shape, jnp.int32),
            pltpu.VMEM((images, angles, width), jnp.float32),
            pltpu.VMEM((blocks + 1, angles, width), jnp.float32),
            dma((size - 1,)),
            dma((size - 1,)),
            dma((size - 1,)),
            dma((size - 1,)),
            dma((size + 2,)),
        ],
        compiler_params=pltpu.CompilerParams(
            collective_id=0, has_side_effects=True, vmem_limit_bytes=62 * 1024 * 1024
        ),
        name="exchange",
    )(offsets.reshape(blocks, 2, hs, depth), aux, slant_weights.T)

    moments = (8, LANES)
    pieces = 4
    lines = (2, planes - 1, pieces)
    return pl.pallas_call(
        functools.partial(gather_kernel, grp),
        out_shape=jax.ShapeDtypeStruct((IMG_DEV, 2 * angles, depth), jnp.bfloat16),
        in_specs=[vmem, vmem],
        out_specs=any_space,
        scratch_shapes=[
            pltpu.VMEM(lines + (per_plane // pieces, angles, width), jnp.bfloat16),
            pltpu.VMEM((per_plane, angles, width), jnp.float32),
            pltpu.VMEM((per_plane, angles, width), jnp.bfloat16),
            pltpu.VMEM((size - 1,) + moments, jnp.float32),
            pltpu.VMEM((planes - 1,) + moments, jnp.float32),
            pltpu.VMEM(moments, jnp.float32),
            dma(lines),
            dma(lines),
            dma((size - 1,)),
            dma((size - 1,)),
            dma((planes - 1,)),
            dma((planes - 1,)),
            dma((size - 1,)),
            dma((size - 1,)),
            dma((2,)),
        ],
        compiler_params=pltpu.CompilerParams(
            collective_id=1, has_side_effects=True, vmem_limit_bytes=60 * 1024 * 1024
        ),
        name="gather",
    )(part, mom)


def round_up(value, unit):
    return -(-value // unit) * unit


def fused_kernel(
    shape, off, live_in, tile_in, slot_in, w_in, out,
    live, tile, slot, weights, raw, wb, onehot, mine, theirs, cuts, squares, sl,
    own, part, rx1, rxv, held, ft, fin, sums, pin, gains,
    load_sem, in_sem, core_s, core_r, meta_s, meta_r, s1s, s1r, vs, vr, zs, zr, fs, fr, ms, mr,
):
    planes, grp, kinds = shape
    shot, g = lax.axis_index("shot"), lax.axis_index("grp")
    z, y = lax.div(shot, PAIR), lax.rem(shot, PAIR)
    x, c = lax.div(g, 2), lax.rem(g, 2)
    blocks, hs, depth = raw.shape[1:]
    angles = live.shape[0]
    images = onehot.shape[0]
    img_dev = out.shape[0]
    per, wide = sl.shape[1], sl.shape[3]
    pairs = per // 2
    depths, groups = depth // wide, angles // per
    cus = depths * groups
    early = 2 * kinds.count("zv")
    late_count = 2 * cus - early

    def device(step=0, fy=False, fx=False, fc=False):
        yy = 1 - y if fy else y
        xx = 1 - x if fx else x
        cc = 1 - c if fc else c
        return ((z + step) * PAIR + yy, xx * 2 + cc)

    core_peer, x_peer, y_peer = device(fc=True), device(fx=True), device(fy=True)
    first_peer = (x_peer, y_peer)
    second_peer = (y_peer, x_peer)

    def remote(src, dst, send_sem, recv_sem, peer):
        return pltpu.make_async_remote_copy(
            src_ref=src, dst_ref=dst, send_sem=send_sem, recv_sem=recv_sem,
            device_id=peer, device_id_type=MESH,
        )

    barrier = pltpu.get_barrier_semaphore()

    def greet(peer):
        pl.semaphore_signal(barrier, inc=1, device_id=peer, device_id_type=MESH)

    for peer in (core_peer, x_peer, y_peer):
        greet(peer)

    @pl.when(z > 0)
    def _():
        greet(device(step=-1))

    @pl.when(z < planes - 1)
    def _():
        greet(device(step=1))

    loads = [
        pltpu.make_async_copy(src, dst, load_sem.at[n])
        for n, (src, dst) in enumerate(
            ((w_in, weights), (live_in, live), (tile_in, tile), (slot_in, slot))
        )
    ]
    for copy in loads:
        copy.start()
    own_in = [
        pltpu.make_async_copy(
            off.at[:, c, :, pl.ds(d * wide, wide)],
            raw.at[0, :, :, pl.ds(d * wide, wide)],
            in_sem.at[d],
        )
        for d in range(depths)
    ]
    for copy in own_in:
        copy.start()
    spans = [(0, LANES), (LANES, wide - LANES)] + [(d * wide, wide) for d in range(1, depths)]
    core_in = [
        remote(
            off.at[:, 1 - c, :, pl.ds(lane, size)],
            raw.at[1, :, :, pl.ds(lane, size)],
            core_s.at[n], core_r.at[n], core_peer,
        )
        for n, (lane, size) in enumerate(spans)
    ]
    meta = remote(mine, theirs, meta_s.at[0], meta_r.at[0], core_peer)

    eight = 8
    for copy in loads:
        copy.wait()
    ones = jnp.ones((angles, LANES), jnp.bfloat16)
    spot = lax.broadcasted_iota(jnp.int32, (blocks, 2 * blocks), 1)
    block = lax.broadcasted_iota(jnp.int32, (blocks, 2 * blocks), 0)

    def cutoff(j):
        pick = jnp.where(spot == 2 * block + j, 1.0, 0.0).astype(jnp.bfloat16)
        flags = lax.dot_general(
            pick, live[...].astype(jnp.float32).astype(jnp.bfloat16),
            (((1,), (1,)), ((), ())), preferred_element_type=jnp.float32,
        )
        total = jnp.dot(flags.astype(jnp.bfloat16), ones, preferred_element_type=jnp.float32)
        return total.astype(jnp.int32)

    mine[0:eight] = jnp.full((eight, LANES), -1, jnp.int32)
    mine[0:1, 0:blocks] = tile[...] * (img_dev * grp) + slot[...]
    mine[eight : eight + blocks] = cutoff(1 - c)
    cuts[0] = cutoff(c)

    ends = jnp.where(z == 0, 1, 0) + jnp.where(z == planes - 1, 1, 0)
    pl.semaphore_wait(barrier, 5 - ends)
    core_in[0].start()
    meta.start()
    for copy in core_in[1:]:
        copy.start()

    rows = angles * eight
    spread = lax.broadcasted_iota(jnp.int32, (rows, angles), 0)
    which = lax.broadcasted_iota(jnp.int32, (rows, angles), 1)
    pick = jnp.where(lax.div(spread, eight) == which, 1.0, 0.0).astype(jnp.bfloat16)
    tall = lax.dot_general(
        pick, weights[...], (((1,), (1,)), ((), ())), preferred_element_type=jnp.float32
    ).astype(jnp.bfloat16)
    line = lax.broadcasted_iota(jnp.int32, (hs, eight * hs), 0)
    column = lax.broadcasted_iota(jnp.int32, (hs, eight * hs), 1)
    copies = jnp.where(lax.rem(column, hs) == line, 1.0, 0.0).astype(jnp.bfloat16)
    full = jnp.dot(tall, copies, preferred_element_type=jnp.float32)
    line = lax.broadcasted_iota(jnp.int32, full.shape, 0)
    column = lax.broadcasted_iota(jnp.int32, full.shape, 1)
    wb[...] = jnp.where(lax.rem(line, eight) == lax.div(column, hs), full, 0.0).astype(jnp.bfloat16)
    squares[...] = jnp.zeros_like(squares)

    def slant(cu, r, tiles=(0, 1)):
        d, a0 = cu // groups, cu % groups * per
        lane0, size = tiles[0] * LANES, len(tiles) * LANES
        if r == 0 and cu % groups == 0:
            own_in[d].wait()
        if r == 1 and cu == 0 and lane0 == 0:
            meta.wait_recv()
            cuts[1] = theirs[eight : eight + blocks]
            select_rows()
        if r == 1 and cu % groups == 0:
            core_in[spans.index((d * wide + lane0, size))].wait_recv()

        def body(i, _):
            lhs = wb[a0 * eight : (a0 + per) * eight]
            lanes = slice(d * wide + lane0, d * wide + lane0 + size)
            a = lax.broadcasted_iota(jnp.int32, (per, 2 * eight, LANES), 0) + a0
            total = squares[a0 : a0 + per]
            for n in range(SLANT_UNROLL):
                start = (i * SLANT_UNROLL + n) * 2 * eight
                alive = cuts[r, pl.ds(start, 2 * eight)][None] > a
                ys = []
                for k in range(2):
                    data = raw[r, pl.ds(start + k * eight, eight), :, lanes]
                    data = data.reshape(eight * hs, size)
                    y = jnp.dot(lhs, data, preferred_element_type=jnp.float32)
                    ys.append(y.reshape(per, eight, size))
                for k in range(len(tiles)):
                    cut = slice(k * LANES, (k + 1) * LANES)
                    to = slice(lane0 + k * LANES, lane0 + (k + 1) * LANES)
                    v = jnp.concatenate([ys[0][:, :, cut], ys[1][:, :, cut]], axis=1)
                    v = jnp.where(alive, v, 0.0)
                    q = v * v
                    total += q[:, :eight] + q[:, eight:]
                    sl[cu % 2, :, pl.ds(r * blocks + start, 2 * eight), to] = v.astype(jnp.bfloat16)
            squares[a0 : a0 + per] = total
            return 0

        lax.fori_loop(0, blocks // (2 * eight * SLANT_UNROLL), body, 0)

    def select_rows():
        lanes = round_up(2 * blocks, LANES)
        rest = jnp.full((eight, lanes - LANES), -1, jnp.int32)
        a_row = jnp.concatenate([jnp.broadcast_to(mine[0:1], (eight, LANES)), rest], axis=1)
        b_row = jnp.concatenate([jnp.broadcast_to(theirs[0:1], (eight, LANES)), rest], axis=1)
        b_row = pltpu.roll(b_row, blocks, 1)
        lane = lax.broadcasted_iota(jnp.int32, a_row.shape, 1)
        row = jnp.where(lane < blocks, a_row, b_row)
        mask = y * (img_dev * grp) + g * img_dev
        row = lax.bitwise_xor(row, jnp.full(row.shape, 0, jnp.int32) + mask)
        number = lax.broadcasted_iota(jnp.int32, (images, lanes), 0)
        hit = jnp.where(number == row[0:1], 1.0, 0.0).astype(jnp.bfloat16)
        onehot[...] = hit[:, : 2 * blocks]

    def stack(cu, tiles=(0, 1)):
        near = slice(tiles[0] * LANES, (tiles[-1] + 1) * LANES)

        def body(i, _):
            for o in range(STACK_UNROLL):
                m = i * STACK_UNROLL + o
                ys = [
                    jnp.dot(onehot[...], sl[cu % 2, 2 * m + k, :, near], preferred_element_type=jnp.float32)
                    for k in range(2)
                ]
                for n, l in enumerate(tiles):
                    p = 2 * cu + l
                    cut = slice(n * LANES, (n + 1) * LANES)
                    for t in range(planes):
                        for ry in range(2):
                            for rx in range(2):
                                r = ((t * 2 + ry) * 2 + rx) * eight
                                v = [ys[k][r : r + eight, cut] for k in range(2)]
                                v = jnp.concatenate(v, axis=0)
                                one, two = (rx, ry) if l == 0 else (ry, rx)
                                if one == 0:
                                    own[p, t, two, m] = v
                                else:
                                    part[p, t, two, m] = v.astype(jnp.bfloat16)
            return 0

        lax.fori_loop(0, pairs // STACK_UNROLL, body, 0)

    def late(cu):
        return kinds[cu] == "vz"

    def s1(cu, l, t):
        p = 2 * cu + l
        return remote(part.at[p, t], rx1.at[p, t], s1s.at[0], s1r.at[cu, t], first_peer[l])

    def across_slot(cu, t):
        return early // 2 + (cu - early // 2) * planes + t if late(cu) else cu

    def across(cu, l, t, source):
        p, slot = 2 * cu + l, across_slot(cu, t)
        kind = 1 if late(cu) else 0
        return remote(source, rxv.at[p, t], vs.at[kind], vr.at[slot], second_peer[l])

    def arrived(region, sem):
        remote(region, region, ms.at[0], sem, core_peer).wait_recv()

    def messages(cu):
        return [(0,), (1,)] if late(cu) else [(0, 1)]

    def hop(cu, tiles, way, s, source):
        p, n = pl.ds(2 * cu + tiles[0], len(tiles)), pl.ds(0, 1 if late(cu) else 2)
        kind = 1 if late(cu) else 0
        slot = early // 2 + 2 * (cu - early // 2) + tiles[0] if late(cu) else cu
        return remote(
            source, held.at[p, way, s, n], zs.at[kind, way, s], zr.at[slot, way, s],
            device(step=1 - 2 * way),
        )

    def begin(cu, t):
        for tiles in messages(cu):
            p = pl.ds(2 * cu + tiles[0], len(tiles))
            source = rx1.at[p, t, pl.ds(0, 1 if late(cu) else 2)]
            if t > 0:
                @pl.when(z == 0)
                def _(tiles=tiles, source=source):
                    hop(cu, tiles, 0, planes - 1 - t, source).start()
            if t < planes - 1:
                @pl.when(z == planes - 1)
                def _(tiles=tiles, source=source):
                    hop(cu, tiles, 1, t, source).start()

    def start(cu, tiles=(0, 1)):
        for t in far_first(planes):
            for l in tiles:
                s1(cu, l, t).start()

    def first(cu, t):
        arrived(rx1.at[pl.ds(2 * cu, 2), t], s1r.at[cu, t])
        for l in range(2):
            p = 2 * cu + l
            for k in (1, 0):
                total = own[p, t, k] + rx1[p, t, k].astype(jnp.float32)
                own[p, t, k] = total
                rx1[p, t, k] = total.astype(jnp.bfloat16)
            if late(cu):
                across(cu, l, t, rx1.at[p, t, 1]).start()
        if not late(cu):
            begin(cu, t)

    def second(cu, t):
        arrived(rxv.at[pl.ds(2 * cu, 2), t], vr.at[across_slot(cu, t)])
        for l in range(2):
            p = 2 * cu + l
            total = own[p, t, 0] + rxv[p, t].astype(jnp.float32)
            own[p, t, 0] = total
            rx1[p, t, 0] = total.astype(jnp.bfloat16)
        begin(cu, t)

    def tick(cu, tau, way):
        here = z if way == 0 else planes - 1 - z
        s = tau - here
        target = planes - 1 - s if way == 0 else s
        n = 1 if late(cu) else 2

        @pl.when((here >= 1) & (s >= 0))
        def _():
            for tiles in messages(cu):
                p = pl.ds(2 * cu + tiles[0], len(tiles))
                message = held.at[p, way, s, pl.ds(0, n)]
                hop(cu, tiles, way, s, message).wait_recv()
                for l in tiles:
                    p = 2 * cu + l
                    for k in range(n):
                        value = held[p, way, s, k].astype(jnp.float32) + own[p, target, k]
                        if tau < planes - 1:
                            held[p, way, s, k] = value.astype(jnp.bfloat16)
                        else:
                            own[p, target, k] = value
                if tau < planes - 1:
                    hop(cu, tiles, way, s, message).start()

    def third(cu):
        for l in range(2):
            p = 2 * cu + l
            rx1[p, z, 1] = own[p, z, 1].astype(jnp.bfloat16)
            across(cu, l, 0, rx1.at[p, z, 1]).start()

    def leave(line, lanes):
        row = pl.multiple_of(c * angles + line.start, per)
        view = out.at[:, pl.ds(row, line.size), pl.ds(lanes.start, lanes.size)]
        return remote(fin.at[:, line, lanes], view, fs.at[0], fr.at[0], core_peer)

    def finish(cu):
        if not late(cu):
            arrived(rxv.at[pl.ds(2 * cu, 2), 0], vr.at[across_slot(cu, 0)])
        a0, lane0 = cu % groups * per, cu // groups * wide
        for l in range(2):
            p = 2 * cu + l
            total = own[p, z, 0]
            if not late(cu):
                total += rxv[p, 0].astype(jnp.float32)
            ft[l] = total.reshape(per * eight, LANES)
            lanes = slice(lane0 + l * LANES, lane0 + (l + 1) * LANES)
            for r in range(eight):
                v = ft[l, pl.ds(r, per, stride=eight)] * gains[a0 : a0 + per]
                if r < img_dev:
                    row = pl.multiple_of(c * angles + a0, per)
                    out[r, pl.ds(row, per), lanes] = v.astype(jnp.bfloat16)
                else:
                    fin[r - img_dev, a0 : a0 + per, lanes] = v.astype(jnp.bfloat16)
        leave(pl.ds(a0, per), pl.ds(lane0, wide)).start()

    def moment(stage):
        peer = (core_peer, x_peer, y_peer)[stage]
        return remote(sums.at[stage], pin.at[stage], ms.at[stage], mr.at[stage], peer)

    def passing(way):
        n = 3 + way
        return remote(sums.at[n + 1], pin.at[n], ms.at[n], mr.at[n], device(step=1 - 2 * way))

    def moments(stage):
        if stage == 0:
            total = jnp.sum(jnp.sum(squares[...], axis=1), axis=1, keepdims=True)
            count = jnp.sum(live[...].astype(jnp.float32), axis=1, keepdims=True)
            lane = lax.broadcasted_iota(jnp.int32, (angles, LANES), 1)
            both = jnp.where(lane == 0, total, jnp.where(lane == 1, count, 0.0))
            both = jnp.concatenate([both, jnp.zeros((LANES - angles, LANES), jnp.float32)], axis=0)
            sums[0] = both.T[:eight]
            moment(0).start()
            return
        if stage <= 3:
            moment(stage - 1).wait_recv()
            sums[stage] = sums[stage - 1] + pin[stage - 1]
            if stage < 3:
                moment(stage).start()
                return
            sums[6] = sums[3]
        tau = stage - 3
        if tau < planes:
            for way in range(2):
                here = z if way == 0 else planes - 1 - z

                @pl.when(here == tau)
                def _(way=way):
                    if tau > 0:
                        passing(way).wait_recv()
                        sums[6] = sums[6] + pin[3 + way]
                        sums[4 + way] = sums[3] + pin[3 + way]
                    else:
                        sums[4 + way] = sums[3]
                    if tau < planes - 1:
                        passing(way).start()
        else:
            total = sums[6]
            gain = lax.rsqrt(total[0:1] / (depth * total[1:2]) + 1e-06)
            gains[...] = jnp.broadcast_to(gain, (LANES, LANES)).T[:angles]

    run = {
        "slant": slant, "stack": stack, "start": start, "first": first, "second": second,
        "tick": tick, "third": third, "finish": finish, "moments": moments,
    }
    for _, action in sorted(schedule(planes, kinds), key=lambda e: e[0]):
        run[action[0]](*action[1:])

    meta.wait_send()
    for copy in core_in:
        copy.wait_send()
    remote(part, rx1, s1s.at[0], s1r.at[0, 0], core_peer).wait_send()
    if early:
        region = rxv.at[pl.ds(0, early), 0]
        remote(region, region, vs.at[0], vr.at[0], core_peer).wait_send()
    if late_count:
        region = rxv.at[pl.ds(early, late_count)]
        remote(region, region, vs.at[1], vr.at[0], core_peer).wait_send()
    for way in range(2):
        here = z if way == 0 else planes - 1 - z

        @pl.when(here < planes - 1)
        def _(way=way):
            passing(way).wait_send()

        for s in range(planes - 1):
            @pl.when(here < planes - 1 - s)
            def _(way=way, s=s):
                for kind, region in enumerate(
                    (
                        held.at[pl.ds(0, early), way, s],
                        held.at[pl.ds(early, late_count), way, s, pl.ds(0, 1)],
                    )
                ):
                    if (early, late_count)[kind]:
                        remote(
                            region, region, zs.at[kind, way, s], zr.at[0, way, s], core_peer
                        ).wait_send()
    for stage in range(3):
        moment(stage).wait_send()
    leave(pl.ds(0, angles), pl.ds(0, depth)).wait()


def far_first(planes):
    return [planes - 1 - i // 2 if i % 2 == 0 else i // 2 for i in range(planes)]


def schedule(planes, kinds):
    compute, spacing, lag, sub = SCHEDULE["compute"], SCHEDULE["first"], SCHEDULE["start"], SCHEDULE["sub"]
    cus = len(kinds)
    events = [(-2.0, ("slant", 0, 0))]
    for l in range(2):
        for n, name in enumerate((("slant", 0, 1), ("stack", 0), ("start", 0))):
            events.append((-1.0 + 0.1 * n + 0.4 * l, name + ((l,),)))
    events.append((-0.3, ("slant", 1, 0)))
    for cu in range(1, cus):
        at = compute * cu
        if cu > 1:
            events.append((at, ("slant", cu, 0)))
        events.append((at + 0.1 * compute, ("slant", cu, 1)))
        events.append((at + 0.2 * compute, ("stack", cu)))
    done = compute * cus
    for stage in range(3 + planes + 1):
        events.append((done + SCHEDULE["moments"] * stage, ("moments", stage)))
    gain = done + SCHEDULE["moments"] * (3 + planes) + 0.1
    now = SCHEDULE["begin"]
    for cu, kind in enumerate(kinds):
        at = now
        if cu > 0:
            events.append((max(compute * cu + 0.3 * compute, at - lag), ("start", cu)))
        at = max(at, compute * cu + 0.3 * compute + 0.1)
        for i, t in enumerate(far_first(planes)):
            events.append((at + i * sub, ("first", cu, t)))
        now += spacing[kind]
        at += (planes - 1) * sub
        if kind == "vz":
            at += SCHEDULE["second"] - (planes - 1) * sub
            for i, t in enumerate(far_first(planes)):
                events.append((at + i * sub, ("second", cu, t)))
            at += (planes - 1) * sub
        for tau in range(1, planes):
            at += SCHEDULE["hop"][kind]
            for way in range(2):
                events.append((at, ("tick", cu, tau, way)))
        if kind == "zv":
            at += SCHEDULE["third"]
            events.append((at, ("third", cu)))
            at += SCHEDULE["finish"]
        events.append((max(at + 0.01, gain), ("finish", cu)))
    return events


def fused(shapes, offsets, slant_weights, live, block_tile, image_slot):
    planes, grp, scratch, kinds = shapes
    blocks = block_tile.shape[0]
    hs, depth = offsets.shape[1:]
    angles = slant_weights.shape[0]
    any_space = pl.BlockSpec(memory_space=pl.ANY)
    return pl.pallas_call(
        functools.partial(fused_kernel, (planes, grp, kinds)),
        out_shape=pltpu.VMEM((IMG_DEV, 2 * angles, depth), jnp.bfloat16),
        in_specs=[any_space] * 5,
        out_specs=pl.BlockSpec(memory_space=pltpu.VMEM),
        scratch_shapes=scratch,
        compiler_params=pltpu.CompilerParams(
            collective_id=2, has_side_effects=True, vmem_limit_bytes=VMEM_LIMIT
        ),
        name="calibrated_stack",
    )(
        offsets.reshape(blocks, 2, hs, depth),
        live.T,
        block_tile.reshape(1, blocks),
        image_slot.reshape(1, blocks),
        slant_weights.T,
    )


def buffers(planes, blocks, hs, depth, angles, images):
    wide, per = 2 * LANES, 16
    cus = (depth // wide) * (angles // per)
    pieces = 2 * cus
    tile = (per // 2, 16, LANES)
    dma = pltpu.SemaphoreType.DMA
    bf, f32, i32 = jnp.bfloat16, jnp.float32, jnp.int32
    early = (5 * cus + 4) // 8
    kinds = ("zv",) * early + ("vz",) * (cus - early)
    memory = [
        ((angles, 2 * blocks), i32),
        ((1, blocks), i32),
        ((1, blocks), i32),
        ((hs, angles), bf),
        ((2, blocks, hs, depth), bf),
        ((angles * 8, 8 * hs), bf),
        ((images, 2 * blocks), bf),
        ((8 + blocks, LANES), i32),
        ((8 + blocks, LANES), i32),
        ((2, blocks, LANES), i32),
        ((angles, 8, LANES), f32),
        ((2, per, 2 * blocks, wide), bf),
        ((pieces, planes, 2) + tile, f32),
        ((pieces, planes, 2) + tile, bf),
        ((pieces, planes, 2) + tile, bf),
        ((pieces, planes) + tile, bf),
        ((pieces, 2, planes - 1, 2) + tile, bf),
        ((2, per * 8, LANES), f32),
        ((IMG_DEV, angles, depth), bf),
        ((7, 8, LANES), f32),
        ((5, 8, LANES), f32),
        ((angles, LANES), f32),
    ]
    size = sum(math.prod(s) * jnp.dtype(d).itemsize for s, d in memory)
    scratch = [pltpu.VMEM(s, d) for s, d in memory]
    depths = depth // wide
    scratch += [
        dma((4,)), dma((depths,)), dma((depths + 1,)), dma((depths + 1,)), dma((1,)), dma((1,)),
        dma((1,)), dma((cus, planes)),
        dma((2,)), dma((early + (cus - early) * planes,)),
        dma((2, 2, planes - 1)), dma((early + 2 * (cus - early), 2, planes - 1)),
        dma((1,)), dma((1,)), dma((5,)), dma((5,)),
    ]
    return size, scratch, kinds


def local(offsets, slant_weights, live, block_tile, image_slot):
    shots, grp = lax.axis_size("shot"), lax.axis_size("grp")
    planes = shots // PAIR
    blocks = block_tile.shape[0]
    hs, depth = offsets.shape[1:]
    angles = slant_weights.shape[0]
    images = shots * IMG_DEV * grp
    size, scratch, kinds = buffers(planes, blocks, hs, depth, angles, images)
    args = (offsets, slant_weights, live, block_tile, image_slot)
    if grp == 4 and size + (2 << 20) <= VMEM_LIMIT:
        return fused((planes, grp, scratch, kinds), *args)
    return staged(*args)


def solution(mesh):
    placed = (
        P(("shot", "grp"), None, None),
        P(),
        P(("shot", "grp"), None),
        P(("shot", "grp"), None),
        P(("shot", "grp")),
    )
    return jax.shard_map(
        local, mesh=mesh, in_specs=placed, out_specs=P(("shot", "grp"), None, None), check_vma=False
    )
```

```python
import functools
import math

import jax
import jax.numpy as jnp
from jax import lax
from jax.experimental import pallas as pl
from jax.experimental.pallas import tpu as pltpu
from jax.sharding import PartitionSpec as P

IMG_DEV = 4
PAIR = 2
LANES = 128
UNROLL = 8
MESH = pl.DeviceIdType.MESH
VMEM_LIMIT = 62 * 1024 * 1024
SLANT_UNROLL = 2
STACK_UNROLL = 4
SCHEDULE = {
    "compute": 3.19, "first": {"zv": 7.98, "vz": 14.69}, "begin": 3.59, "start": 15.93, "sub": 2.8,
    "second": 19.16, "hop": {"zv": 14.36, "vz": 19.05}, "third": 32.32, "finish": 0.39,
    "moments": 16.35,
}


def place(grp):
    shot, g = lax.axis_index("shot"), lax.axis_index("grp")
    return lax.div(shot, PAIR), lax.rem(shot, PAIR) * grp + g


def at(plane, spot, grp):
    return (plane * PAIR + lax.div(spot, grp), lax.rem(spot, grp))


def share(spot, width, depth):
    start = spot * width
    return lax.div(start, depth), pl.multiple_of(lax.rem(start, depth), LANES)


def relative(spot, grp, r):
    mid = grp // 2
    pair, rest = lax.div(spot, grp), lax.rem(spot, grp)
    m, c = lax.div(rest, 2), lax.rem(rest, 2)
    rp, rm, rc = r // grp, (r % grp) // 2, r % 2
    pair, m, c = lax.rem(pair + rp, PAIR), lax.rem(m + rm, mid), lax.rem(c + rc, 2)
    return (pair * mid + m) * 2 + c


def orders(grp):
    size = PAIR * grp
    far = list(range(grp + 2, size))
    side = list(range(grp, grp + 2))
    ahead = list(range(2, grp))
    turn = []
    for i in range(max(len(far), len(ahead))):
        for group in (far, side, ahead):
            turn += group[i : i + 1]
    return [1] + turn


def exchange_kernel(
    grp, off, aux, w_in, part, mom, w, raw, aux_in, codes, acc, seg, send, recv, asend, arecv, lsem
):
    size = PAIR * grp
    plane, spot = place(grp)
    blocks, depth, width = off.shape[0], off.shape[3], raw.shape[3]
    angles, images = w.shape[1], acc.shape[0]
    j, first = share(spot, width, depth)
    mine = pltpu.make_async_copy(off.at[:, j, :, pl.ds(first, width)], raw.at[0], lsem.at[0])
    mine.start()
    own_codes = pltpu.make_async_copy(aux, codes.at[0], lsem.at[1])
    own_codes.start()
    weigh = pltpu.make_async_copy(w_in, w, lsem.at[size + 1])
    weigh.start()
    barrier = pltpu.get_barrier_semaphore()
    for r in range(1, size):
        pl.semaphore_signal(
            barrier, inc=1, device_id=at(plane, relative(spot, grp, r), grp), device_id_type=MESH
        )
    pl.semaphore_wait(barrier, size - 1)
    data, notes = {}, {}
    for r in orders(grp):
        peer = relative(spot, grp, r)
        pj, pfirst = share(peer, width, depth)
        dev = at(plane, peer, grp)
        notes[r] = pltpu.make_async_remote_copy(
            src_ref=aux,
            dst_ref=aux_in.at[r],
            send_sem=asend.at[r - 1],
            recv_sem=arecv.at[r - 1],
            device_id=dev,
            device_id_type=MESH,
        )
        data[r] = pltpu.make_async_remote_copy(
            src_ref=off.at[:, pj, :, pl.ds(pfirst, width)],
            dst_ref=raw.at[r],
            send_sem=send.at[r - 1],
            recv_sem=recv.at[r - 1],
            device_id=dev,
            device_id_type=MESH,
        )
    for r in orders(grp):
        notes[r].start()
    for r in orders(grp):
        data[r].start()

    acc[...] = jnp.zeros_like(acc)
    seg[blocks] = jnp.zeros((angles, width), jnp.float32)
    row = lax.broadcasted_iota(jnp.int32, (angles, width), 0)
    weigh.wait()
    weights = w[...].astype(jnp.float32).T.astype(jnp.bfloat16)
    square = jnp.zeros((angles, width), jnp.float32)
    count = jnp.zeros((angles, width), jnp.float32)
    for r in [0] + orders(grp):
        if r:
            notes[r].wait()
            code = pltpu.make_async_copy(aux_in.at[r], codes.at[r], lsem.at[r + 1])
            code.start()
            code.wait()
            data[r].wait()
        else:
            own_codes.wait()
            mine.wait()

        def slant(i, carry, r=r):
            square, count = carry
            start = i * UNROLL
            x = jnp.concatenate([raw[r, start + t] for t in range(UNROLL)], axis=1)
            y = jnp.dot(weights, x, preferred_element_type=jnp.float32)
            for t in range(UNROLL):
                alive = row < codes[r, 1 + j, start + t]
                slanted = jnp.where(alive, y[:, t * width : (t + 1) * width], 0.0)
                slanted = slanted.astype(jnp.bfloat16).astype(jnp.float32)
                square += slanted * slanted
                count += jnp.where(alive, 1.0, 0.0)
                seg[start + t] = slanted + seg[codes[r, 0, start + t]]
            return square, count

        square, count = lax.fori_loop(0, blocks // UNROLL, slant, (square, count))

        def stack(i, _, r=r):
            start = i * UNROLL
            line, column = lax.div(start, LANES), lax.rem(start, LANES)
            for t in range(UNROLL):
                acc[start + t] += seg[codes[r, 3 + line, column + t]]
            return 0

        lax.fori_loop(0, images // UNROLL, stack, 0)

    def narrow(i, _):
        start = pl.multiple_of(i * UNROLL, UNROLL)
        part[pl.ds(start, UNROLL)] = acc[pl.ds(start, UNROLL)].astype(jnp.bfloat16)
        return 0

    lax.fori_loop(0, images // UNROLL, narrow, 0)
    lane = lax.broadcasted_iota(jnp.int32, (angles, LANES), 1)
    square = jnp.sum(square, axis=1, keepdims=True)
    count = jnp.sum(count, axis=1, keepdims=True)
    both = jnp.where(lane == 0, square, jnp.where(lane == 1, count, 0.0))
    both = jnp.concatenate([both, jnp.zeros((LANES - angles, LANES), jnp.float32)], axis=0)
    mom[...] = both.T[: mom.shape[0]]


def gather_kernel(
    grp, part, mom, out, held, total, fin, pin, qin, half_sum, zs, zr, ps, pr, qs, qr, fs, fr, lsem
):
    size = PAIR * grp
    planes = held.shape[1] + 1
    plane, spot = place(grp)
    pieces, rows, angles, width = held.shape[2:]
    depth = out.shape[2]
    chunk = pieces * rows
    lower = jnp.where(plane < planes // 2, 1, 0)
    barrier = pltpu.get_barrier_semaphore()
    for r in range(1, size):
        pl.semaphore_signal(
            barrier, inc=1, device_id=at(plane, lax.rem(spot + r, size), grp), device_id_type=MESH
        )
    for r in range(1, planes):
        pl.semaphore_signal(
            barrier, inc=1, device_id=at(lax.rem(plane + r, planes), spot, grp), device_id_type=MESH
        )
    pl.semaphore_wait(barrier, size + planes - 2)

    def along(up):
        spot_on_line = plane * up + (planes - 1 - plane) * (1 - up)
        following = lax.rem(plane + 2 * up - 1 + planes, planes)
        return 1 - up, spot_on_line, following

    def rows_of(up, s, h):
        target = (planes - 1 - s) * up + s * (1 - up)
        return target * chunk + h * rows

    def hop(up, s, h, source):
        way, _, following = along(up)
        return pltpu.make_async_remote_copy(
            src_ref=source,
            dst_ref=held.at[way, s, h],
            send_sem=zs.at[way, s, h],
            recv_sem=zr.at[way, s, h],
            device_id=at(following, spot, grp),
            device_id_type=MESH,
        )

    def begin(s):
        @pl.when(along(lower)[1] == 0)
        def _():
            for h in range(pieces):
                hop(lower, s, h, part.at[pl.ds(rows_of(lower, s, h), rows)]).start()

    def step(up, s, h):
        way, here, _ = along(up)
        end = planes - 1 - s

        @pl.when((here > 0) & (here <= end))
        def _():
            hop(up, s, h, held.at[way, s, h]).wait_recv()

        @pl.when((here > 0) & (here < end))
        def _():
            start = rows_of(up, s, h)

            def add(i, _):
                value = held[way, s, h, i].astype(jnp.float32) + part[start + i].astype(jnp.float32)
                held[way, s, h, i] = value.astype(jnp.bfloat16)
                return 0

            lax.fori_loop(0, rows, add, 0)
            hop(up, s, h, held.at[way, s, h]).start()

        @pl.when((here > 0) & (here == end))
        def _():
            def add(i, _):
                total[h * rows + i] += held[way, s, h, i].astype(jnp.float32)
                return 0

            lax.fori_loop(0, rows, add, 0)

    def finish(up, s, h):
        way, here, _ = along(up)

        @pl.when(here < planes - 1 - s)
        def _():
            hop(up, s, h, held.at[way, s, h]).wait_send()

    near = [
        pltpu.make_async_remote_copy(
            src_ref=mom,
            dst_ref=pin.at[r - 1],
            send_sem=ps.at[r - 1],
            recv_sem=pr.at[r - 1],
            device_id=at(plane, lax.rem(spot + r, size), grp),
            device_id_type=MESH,
        )
        for r in range(1, size)
    ]
    for copy in near:
        copy.start()
    begin(0)
    total[...] = part[pl.ds(plane * chunk, chunk)].astype(jnp.float32)
    moments = mom[...]
    for copy in near:
        copy.wait()
    for r in range(1, size):
        moments += pin[r - 1]
    half_sum[...] = moments
    wide = [
        pltpu.make_async_remote_copy(
            src_ref=half_sum,
            dst_ref=qin.at[r - 1],
            send_sem=qs.at[r - 1],
            recv_sem=qr.at[r - 1],
            device_id=at(lax.rem(plane + r, planes), spot, grp),
            device_id_type=MESH,
        )
        for r in range(1, planes)
    ]
    for copy in wide:
        copy.start()
    for s in range(1, planes - 1):
        begin(s)
    for s in range(planes - 1):
        for up in (lower, 1 - lower):
            for h in range(pieces):
                step(up, s, h)
    for copy in wide:
        copy.wait()
    moments = half_sum[...]
    for r in range(1, planes):
        moments += qin[r - 1]
    gain = lax.rsqrt(moments[0:1] / moments[1:2] + 1e-06)
    gain = jnp.broadcast_to(gain, (LANES, LANES)).T[:angles]

    def body(i, _):
        fin[i] = (total[i] * gain).astype(jnp.bfloat16)
        return 0

    lax.fori_loop(0, chunk, body, 0)

    each = chunk // size
    j, first = share(spot, width, depth)
    view = out.at[:, pl.ds(pl.multiple_of(j * angles, angles), angles), pl.ds(first, width)]
    last = pltpu.make_async_copy(fin.at[pl.ds(spot * each, each)], view, lsem.at[1])
    final = []
    for r in range(1, size):
        peer = lax.rem(spot + r, size)
        final.append(
            pltpu.make_async_remote_copy(
                src_ref=fin.at[pl.ds(peer * each, each)],
                dst_ref=view,
                send_sem=fs.at[r - 1],
                recv_sem=fr.at[r - 1],
                device_id=at(plane, peer, grp),
                device_id_type=MESH,
            )
        )
    for copy in final:
        copy.start()
    last.start()
    last.wait()
    for copy in final:
        copy.wait()
    for s in range(planes - 1):
        for up in (lower, 1 - lower):
            for h in range(pieces):
                finish(up, s, h)


def staged(offsets, slant_weights, live, block_tile, image_slot):
    shots, grp = lax.axis_size("shot"), lax.axis_size("grp")
    planes, size = shots // PAIR, PAIR * grp
    blocks = block_tile.shape[0]
    hs, depth = offsets.shape[1:]
    angles = slant_weights.shape[0]
    width = 2 * depth // size
    tile_rows = IMG_DEV * grp
    images = shots * tile_rows
    per_plane = images // planes
    any_space = pl.BlockSpec(memory_space=pl.ANY)
    vmem = pl.BlockSpec(memory_space=pltpu.VMEM)
    dma = pltpu.SemaphoreType.DMA

    cutoff = jnp.sum(live.reshape(blocks, 2, angles), axis=2)
    image = block_tile[:, 0] * tile_rows + image_slot
    index = jnp.arange(blocks, dtype=jnp.int32)
    same = (image[:, None] == image[None, :]) & (index[None, :] < index[:, None])
    before = jnp.max(jnp.where(same, index[None, :], -1), axis=1)
    found = image[None, :] == jnp.arange(images, dtype=jnp.int32)[:, None]
    final = jnp.max(jnp.where(found, index[None, :], -1), axis=1)
    final = jnp.where(final < 0, blocks, final).reshape(images // LANES, LANES)
    before = jnp.where(before < 0, blocks, before)
    aux = jnp.concatenate([before[None], cutoff.T], axis=0)
    aux = jnp.concatenate([jnp.pad(aux, ((0, 0), (0, LANES - blocks))), final], axis=0)
    aux = jnp.pad(aux, ((0, -aux.shape[0] % 8), (0, 0)))

    part, mom = pl.pallas_call(
        functools.partial(exchange_kernel, grp),
        out_shape=(
            jax.ShapeDtypeStruct((images, angles, width), jnp.bfloat16),
            jax.ShapeDtypeStruct((8, LANES), jnp.float32),
        ),
        in_specs=[any_space, vmem, any_space],
        out_specs=(vmem, vmem),
        scratch_shapes=[
            pltpu.VMEM((hs, angles), jnp.bfloat16),
            pltpu.VMEM((size, blocks, hs, width), jnp.bfloat16),
            pltpu.VMEM((size,) + aux.shape, jnp.int32),
            pltpu.SMEM((size,) + aux.shape, jnp.int32),
            pltpu.VMEM((images, angles, width), jnp.float32),
            pltpu.VMEM((blocks + 1, angles, width), jnp.float32),
            dma((size - 1,)),
            dma((size - 1,)),
            dma((size - 1,)),
            dma((size - 1,)),
            dma((size + 2,)),
        ],
        compiler_params=pltpu.CompilerParams(
            collective_id=0, has_side_effects=True, vmem_limit_bytes=62 * 1024 * 1024
        ),
        name="exchange",
    )(offsets.reshape(blocks, 2, hs, depth), aux, slant_weights.T)

    moments = (8, LANES)
    pieces = 4
    lines = (2, planes - 1, pieces)
    return pl.pallas_call(
        functools.partial(gather_kernel, grp),
        out_shape=jax.ShapeDtypeStruct((IMG_DEV, 2 * angles, depth), jnp.bfloat16),
        in_specs=[vmem, vmem],
        out_specs=any_space,
        scratch_shapes=[
            pltpu.VMEM(lines + (per_plane // pieces, angles, width), jnp.bfloat16),
            pltpu.VMEM((per_plane, angles, width), jnp.float32),
            pltpu.VMEM((per_plane, angles, width), jnp.bfloat16),
            pltpu.VMEM((size - 1,) + moments, jnp.float32),
            pltpu.VMEM((planes - 1,) + moments, jnp.float32),
            pltpu.VMEM(moments, jnp.float32),
            dma(lines),
            dma(lines),
            dma((size - 1,)),
            dma((size - 1,)),
            dma((planes - 1,)),
            dma((planes - 1,)),
            dma((size - 1,)),
            dma((size - 1,)),
            dma((2,)),
        ],
        compiler_params=pltpu.CompilerParams(
            collective_id=1, has_side_effects=True, vmem_limit_bytes=60 * 1024 * 1024
        ),
        name="gather",
    )(part, mom)


def round_up(value, unit):
    return -(-value // unit) * unit


def fused_kernel(
    shape, off, live_in, tile_in, slot_in, w_in, out,
    live, tile, slot, weights, raw, wb, onehot, mine, theirs, cuts, squares, sl,
    own, part, rx1, rxv, held, ft, fin, sums, pin, gains,
    load_sem, in_sem, core_s, core_r, meta_s, meta_r, s1s, s1r, vs, vr, zs, zr, fs, fr, ms, mr,
):
    planes, grp, kinds = shape
    shot, g = lax.axis_index("shot"), lax.axis_index("grp")
    z, y = lax.div(shot, PAIR), lax.rem(shot, PAIR)
    x, c = lax.div(g, 2), lax.rem(g, 2)
    blocks, hs, depth = raw.shape[1:]
    angles = live.shape[0]
    images = onehot.shape[0]
    img_dev = out.shape[0]
    per, wide = sl.shape[1], sl.shape[3]
    pairs = per // 2
    depths, groups = depth // wide, angles // per
    cus = depths * groups
    early = 2 * kinds.count("zv")
    late_count = 2 * cus - early

    def device(step=0, fy=False, fx=False, fc=False):
        yy = 1 - y if fy else y
        xx = 1 - x if fx else x
        cc = 1 - c if fc else c
        return ((z + step) * PAIR + yy, xx * 2 + cc)

    core_peer, x_peer, y_peer = device(fc=True), device(fx=True), device(fy=True)
    first_peer = (x_peer, y_peer)
    second_peer = (y_peer, x_peer)

    def remote(src, dst, send_sem, recv_sem, peer):
        return pltpu.make_async_remote_copy(
            src_ref=src, dst_ref=dst, send_sem=send_sem, recv_sem=recv_sem,
            device_id=peer, device_id_type=MESH,
        )

    barrier = pltpu.get_barrier_semaphore()

    def greet(peer):
        pl.semaphore_signal(barrier, inc=1, device_id=peer, device_id_type=MESH)

    for peer in (core_peer, x_peer, y_peer):
        greet(peer)

    @pl.when(z > 0)
    def _():
        greet(device(step=-1))

    @pl.when(z < planes - 1)
    def _():
        greet(device(step=1))

    loads = [
        pltpu.make_async_copy(src, dst, load_sem.at[n])
        for n, (src, dst) in enumerate(
            ((w_in, weights), (live_in, live), (tile_in, tile), (slot_in, slot))
        )
    ]
    for copy in loads:
        copy.start()
    own_in = [
        pltpu.make_async_copy(
            off.at[:, c, :, pl.ds(d * wide, wide)],
            raw.at[0, :, :, pl.ds(d * wide, wide)],
            in_sem.at[d],
        )
        for d in range(depths)
    ]
    for copy in own_in:
        copy.start()
    spans = [(0, LANES), (LANES, wide - LANES)] + [(d * wide, wide) for d in range(1, depths)]
    core_in = [
        remote(
            off.at[:, 1 - c, :, pl.ds(lane, size)],
            raw.at[1, :, :, pl.ds(lane, size)],
            core_s.at[n], core_r.at[n], core_peer,
        )
        for n, (lane, size) in enumerate(spans)
    ]
    meta = remote(mine, theirs, meta_s.at[0], meta_r.at[0], core_peer)

    eight = 8
    for copy in loads:
        copy.wait()
    ones = jnp.ones((angles, LANES), jnp.bfloat16)
    spot = lax.broadcasted_iota(jnp.int32, (blocks, 2 * blocks), 1)
    block = lax.broadcasted_iota(jnp.int32, (blocks, 2 * blocks), 0)

    def cutoff(j):
        pick = jnp.where(spot == 2 * block + j, 1.0, 0.0).astype(jnp.bfloat16)
        flags = lax.dot_general(
            pick, live[...].astype(jnp.float32).astype(jnp.bfloat16),
            (((1,), (1,)), ((), ())), preferred_element_type=jnp.float32,
        )
        total = jnp.dot(flags.astype(jnp.bfloat16), ones, preferred_element_type=jnp.float32)
        return total.astype(jnp.int32)

    mine[0:eight] = jnp.full((eight, LANES), -1, jnp.int32)
    mine[0:1, 0:blocks] = tile[...] * (img_dev * grp) + slot[...]
    mine[eight : eight + blocks] = cutoff(1 - c)
    cuts[0] = cutoff(c)

    ends = jnp.where(z == 0, 1, 0) + jnp.where(z == planes - 1, 1, 0)
    pl.semaphore_wait(barrier, 5 - ends)
    core_in[0].start()
    meta.start()
    for copy in core_in[1:]:
        copy.start()

    rows = angles * eight
    spread = lax.broadcasted_iota(jnp.int32, (rows, angles), 0)
    which = lax.broadcasted_iota(jnp.int32, (rows, angles), 1)
    pick = jnp.where(lax.div(spread, eight) == which, 1.0, 0.0).astype(jnp.bfloat16)
    tall = lax.dot_general(
        pick, weights[...], (((1,), (1,)), ((), ())), preferred_element_type=jnp.float32
    ).astype(jnp.bfloat16)
    line = lax.broadcasted_iota(jnp.int32, (hs, eight * hs), 0)
    column = lax.broadcasted_iota(jnp.int32, (hs, eight * hs), 1)
    copies = jnp.where(lax.rem(column, hs) == line, 1.0, 0.0).astype(jnp.bfloat16)
    full = jnp.dot(tall, copies, preferred_element_type=jnp.float32)
    line = lax.broadcasted_iota(jnp.int32, full.shape, 0)
    column = lax.broadcasted_iota(jnp.int32, full.shape, 1)
    wb[...] = jnp.where(lax.rem(line, eight) == lax.div(column, hs), full, 0.0).astype(jnp.bfloat16)
    squares[...] = jnp.zeros_like(squares)

    def slant(cu, r, tiles=(0, 1)):
        d, a0 = cu // groups, cu % groups * per
        lane0, size = tiles[0] * LANES, len(tiles) * LANES
        if r == 0 and cu % groups == 0:
            own_in[d].wait()
        if r == 1 and cu == 0 and lane0 == 0:
            meta.wait_recv()
            cuts[1] = theirs[eight : eight + blocks]
            select_rows()
        if r == 1 and cu % groups == 0:
            core_in[spans.index((d * wide + lane0, size))].wait_recv()

        def body(i, _):
            lhs = wb[a0 * eight : (a0 + per) * eight]
            lanes = slice(d * wide + lane0, d * wide + lane0 + size)
            a = lax.broadcasted_iota(jnp.int32, (per, 2 * eight, LANES), 0) + a0
            total = squares[a0 : a0 + per]
            for n in range(SLANT_UNROLL):
                start = (i * SLANT_UNROLL + n) * 2 * eight
                alive = cuts[r, pl.ds(start, 2 * eight)][None] > a
                ys = []
                for k in range(2):
                    data = raw[r, pl.ds(start + k * eight, eight), :, lanes]
                    data = data.reshape(eight * hs, size)
                    y = jnp.dot(lhs, data, preferred_element_type=jnp.float32)
                    ys.append(y.reshape(per, eight, size))
                for k in range(len(tiles)):
                    cut = slice(k * LANES, (k + 1) * LANES)
                    to = slice(lane0 + k * LANES, lane0 + (k + 1) * LANES)
                    v = jnp.concatenate([ys[0][:, :, cut], ys[1][:, :, cut]], axis=1)
                    v = jnp.where(alive, v, 0.0)
                    q = v * v
                    total += q[:, :eight] + q[:, eight:]
                    sl[cu % 2, :, pl.ds(r * blocks + start, 2 * eight), to] = v.astype(jnp.bfloat16)
            squares[a0 : a0 + per] = total
            return 0

        lax.fori_loop(0, blocks // (2 * eight * SLANT_UNROLL), body, 0)

    def select_rows():
        lanes = round_up(2 * blocks, LANES)
        rest = jnp.full((eight, lanes - LANES), -1, jnp.int32)
        a_row = jnp.concatenate([jnp.broadcast_to(mine[0:1], (eight, LANES)), rest], axis=1)
        b_row = jnp.concatenate([jnp.broadcast_to(theirs[0:1], (eight, LANES)), rest], axis=1)
        b_row = pltpu.roll(b_row, blocks, 1)
        lane = lax.broadcasted_iota(jnp.int32, a_row.shape, 1)
        row = jnp.where(lane < blocks, a_row, b_row)
        mask = y * (img_dev * grp) + g * img_dev
        row = lax.bitwise_xor(row, jnp.full(row.shape, 0, jnp.int32) + mask)
        number = lax.broadcasted_iota(jnp.int32, (images, lanes), 0)
        hit = jnp.where(number == row[0:1], 1.0, 0.0).astype(jnp.bfloat16)
        onehot[...] = hit[:, : 2 * blocks]

    def stack(cu, tiles=(0, 1)):
        near = slice(tiles[0] * LANES, (tiles[-1] + 1) * LANES)

        def body(i, _):
            for o in range(STACK_UNROLL):
                m = i * STACK_UNROLL + o
                ys = [
                    jnp.dot(onehot[...], sl[cu % 2, 2 * m + k, :, near], preferred_element_type=jnp.float32)
                    for k in range(2)
                ]
                for n, l in enumerate(tiles):
                    p = 2 * cu + l
                    cut = slice(n * LANES, (n + 1) * LANES)
                    for t in range(planes):
                        for ry in range(2):
                            for rx in range(2):
                                r = ((t * 2 + ry) * 2 + rx) * eight
                                v = [ys[k][r : r + eight, cut] for k in range(2)]
                                v = jnp.concatenate(v, axis=0)
                                one, two = (rx, ry) if l == 0 else (ry, rx)
                                if one == 0:
                                    own[p, t, two, m] = v
                                else:
                                    part[p, t, two, m] = v.astype(jnp.bfloat16)
            return 0

        lax.fori_loop(0, pairs // STACK_UNROLL, body, 0)

    def late(cu):
        return kinds[cu] == "vz"

    def s1(cu, l, t):
        p = 2 * cu + l
        return remote(part.at[p, t], rx1.at[p, t], s1s.at[0], s1r.at[cu, t], first_peer[l])

    def across_slot(cu, t):
        return early // 2 + (cu - early // 2) * planes + t if late(cu) else cu

    def across(cu, l, t, source):
        p, slot = 2 * cu + l, across_slot(cu, t)
        kind = 1 if late(cu) else 0
        return remote(source, rxv.at[p, t], vs.at[kind], vr.at[slot], second_peer[l])

    def arrived(region, sem):
        remote(region, region, ms.at[0], sem, core_peer).wait_recv()

    def messages(cu):
        return [(0,), (1,)] if late(cu) else [(0, 1)]

    def hop(cu, tiles, way, s, source):
        p, n = pl.ds(2 * cu + tiles[0], len(tiles)), pl.ds(0, 1 if late(cu) else 2)
        kind = 1 if late(cu) else 0
        slot = early // 2 + 2 * (cu - early // 2) + tiles[0] if late(cu) else cu
        return remote(
            source, held.at[p, way, s, n], zs.at[kind, way, s], zr.at[slot, way, s],
            device(step=1 - 2 * way),
        )

    def begin(cu, t):
        for tiles in messages(cu):
            p = pl.ds(2 * cu + tiles[0], len(tiles))
            source = rx1.at[p, t, pl.ds(0, 1 if late(cu) else 2)]
            if t > 0:
                @pl.when(z == 0)
                def _(tiles=tiles, source=source):
                    hop(cu, tiles, 0, planes - 1 - t, source).start()
            if t < planes - 1:
                @pl.when(z == planes - 1)
                def _(tiles=tiles, source=source):
                    hop(cu, tiles, 1, t, source).start()

    def start(cu, tiles=(0, 1)):
        for t in far_first(planes):
            for l in tiles:
                s1(cu, l, t).start()

    def first(cu, t):
        arrived(rx1.at[pl.ds(2 * cu, 2), t], s1r.at[cu, t])
        for l in range(2):
            p = 2 * cu + l
            for k in (1, 0):
                total = own[p, t, k] + rx1[p, t, k].astype(jnp.float32)
                own[p, t, k] = total
                rx1[p, t, k] = total.astype(jnp.bfloat16)
            if late(cu):
                across(cu, l, t, rx1.at[p, t, 1]).start()
        if not late(cu):
            begin(cu, t)

    def second(cu, t):
        arrived(rxv.at[pl.ds(2 * cu, 2), t], vr.at[across_slot(cu, t)])
        for l in range(2):
            p = 2 * cu + l
            total = own[p, t, 0] + rxv[p, t].astype(jnp.float32)
            own[p, t, 0] = total
            rx1[p, t, 0] = total.astype(jnp.bfloat16)
        begin(cu, t)

    def tick(cu, tau, way):
        here = z if way == 0 else planes - 1 - z
        s = tau - here
        target = planes - 1 - s if way == 0 else s
        n = 1 if late(cu) else 2

        @pl.when((here >= 1) & (s >= 0))
        def _():
            for tiles in messages(cu):
                p = pl.ds(2 * cu + tiles[0], len(tiles))
                message = held.at[p, way, s, pl.ds(0, n)]
                hop(cu, tiles, way, s, message).wait_recv()
                for l in tiles:
                    p = 2 * cu + l
                    for k in range(n):
                        value = held[p, way, s, k].astype(jnp.float32) + own[p, target, k]
                        if tau < planes - 1:
                            held[p, way, s, k] = value.astype(jnp.bfloat16)
                        else:
                            own[p, target, k] = value
                if tau < planes - 1:
                    hop(cu, tiles, way, s, message).start()

    def third(cu):
        for l in range(2):
            p = 2 * cu + l
            rx1[p, z, 1] = own[p, z, 1].astype(jnp.bfloat16)
            across(cu, l, 0, rx1.at[p, z, 1]).start()

    def leave(line, lanes):
        row = pl.multiple_of(c * angles + line.start, per)
        view = out.at[:, pl.ds(row, line.size), pl.ds(lanes.start, lanes.size)]
        return remote(fin.at[:, line, lanes], view, fs.at[0], fr.at[0], core_peer)

    def finish(cu):
        if not late(cu):
            arrived(rxv.at[pl.ds(2 * cu, 2), 0], vr.at[across_slot(cu, 0)])
        a0, lane0 = cu % groups * per, cu // groups * wide
        for l in range(2):
            p = 2 * cu + l
            total = own[p, z, 0]
            if not late(cu):
                total += rxv[p, 0].astype(jnp.float32)
            ft[l] = total.reshape(per * eight, LANES)
            lanes = slice(lane0 + l * LANES, lane0 + (l + 1) * LANES)
            for r in range(eight):
                v = ft[l, pl.ds(r, per, stride=eight)] * gains[a0 : a0 + per]
                if r < img_dev:
                    row = pl.multiple_of(c * angles + a0, per)
                    out[r, pl.ds(row, per), lanes] = v.astype(jnp.bfloat16)
                else:
                    fin[r - img_dev, a0 : a0 + per, lanes] = v.astype(jnp.bfloat16)
        leave(pl.ds(a0, per), pl.ds(lane0, wide)).start()

    def moment(stage):
        peer = (core_peer, x_peer, y_peer)[stage]
        return remote(sums.at[stage], pin.at[stage], ms.at[stage], mr.at[stage], peer)

    def passing(way):
        n = 3 + way
        return remote(sums.at[n + 1], pin.at[n], ms.at[n], mr.at[n], device(step=1 - 2 * way))

    def moments(stage):
        if stage == 0:
            total = jnp.sum(jnp.sum(squares[...], axis=1), axis=1, keepdims=True)
            count = jnp.sum(live[...].astype(jnp.float32), axis=1, keepdims=True)
            lane = lax.broadcasted_iota(jnp.int32, (angles, LANES), 1)
            both = jnp.where(lane == 0, total, jnp.where(lane == 1, count, 0.0))
            both = jnp.concatenate([both, jnp.zeros((LANES - angles, LANES), jnp.float32)], axis=0)
            sums[0] = both.T[:eight]
            moment(0).start()
            return
        if stage <= 3:
            moment(stage - 1).wait_recv()
            sums[stage] = sums[stage - 1] + pin[stage - 1]
            if stage < 3:
                moment(stage).start()
                return
            sums[6] = sums[3]
        tau = stage - 3
        if tau < planes:
            for way in range(2):
                here = z if way == 0 else planes - 1 - z

                @pl.when(here == tau)
                def _(way=way):
                    if tau > 0:
                        passing(way).wait_recv()
                        sums[6] = sums[6] + pin[3 + way]
                        sums[4 + way] = sums[3] + pin[3 + way]
                    else:
                        sums[4 + way] = sums[3]
                    if tau < planes - 1:
                        passing(way).start()
        else:
            total = sums[6]
            gain = lax.rsqrt(total[0:1] / (depth * total[1:2]) + 1e-06)
            gains[...] = jnp.broadcast_to(gain, (LANES, LANES)).T[:angles]

    run = {
        "slant": slant, "stack": stack, "start": start, "first": first, "second": second,
        "tick": tick, "third": third, "finish": finish, "moments": moments,
    }
    for action in ordered(planes, kinds):
        run[action[0]](*action[1:])

    meta.wait_send()
    for copy in core_in:
        copy.wait_send()
    remote(part, rx1, s1s.at[0], s1r.at[0, 0], core_peer).wait_send()
    if early:
        region = rxv.at[pl.ds(0, early), 0]
        remote(region, region, vs.at[0], vr.at[0], core_peer).wait_send()
    if late_count:
        region = rxv.at[pl.ds(early, late_count)]
        remote(region, region, vs.at[1], vr.at[0], core_peer).wait_send()
    for way in range(2):
        here = z if way == 0 else planes - 1 - z

        @pl.when(here < planes - 1)
        def _(way=way):
            passing(way).wait_send()

        for s in range(planes - 1):
            @pl.when(here < planes - 1 - s)
            def _(way=way, s=s):
                for kind, region in enumerate(
                    (
                        held.at[pl.ds(0, early), way, s],
                        held.at[pl.ds(early, late_count), way, s, pl.ds(0, 1)],
                    )
                ):
                    if (early, late_count)[kind]:
                        remote(
                            region, region, zs.at[kind, way, s], zr.at[0, way, s], core_peer
                        ).wait_send()
    for stage in range(3):
        moment(stage).wait_send()
    leave(pl.ds(0, angles), pl.ds(0, depth)).wait()


def far_first(planes):
    return [planes - 1 - i // 2 if i % 2 == 0 else i // 2 for i in range(planes)]


ORDERS = {
    (4, 5, 3): (
        ("slant", 0, 0), ("slant", 1, 0), ("slant", 0, 1, (0,)), ("stack", 0, (0,)), ("start", 0, (0,)),
        ("slant", 0, 1, (1,)), ("stack", 0, (1,)), ("start", 0, (1,)), ("slant", 1, 1), ("stack", 1),
        ("start", 1), ("slant", 3, 0), ("slant", 3, 1), ("first", 0, 3), ("tick", 0, 1, 0),
        ("first", 0, 0), ("tick", 0, 1, 1), ("stack", 3), ("first", 0, 2), ("start", 3), ("first", 0, 1),
        ("first", 1, 3), ("slant", 2, 0), ("slant", 2, 1), ("stack", 2), ("start", 2), ("slant", 4, 0),
        ("tick", 0, 2, 0), ("first", 1, 0), ("tick", 0, 2, 1), ("first", 1, 1), ("slant", 5, 0),
        ("tick", 1, 1, 1), ("first", 1, 2), ("slant", 4, 1), ("stack", 4), ("slant", 6, 0), ("start", 4),
        ("slant", 6, 1), ("stack", 6), ("tick", 1, 2, 1), ("first", 3, 3), ("slant", 5, 1),
        ("tick", 1, 1, 0), ("stack", 5), ("start", 5), ("first", 3, 0), ("first", 2, 0), ("tick", 2, 1, 1),
        ("first", 2, 2), ("first", 2, 3), ("first", 4, 0), ("start", 6), ("tick", 2, 1, 0),
        ("tick", 0, 3, 1), ("first", 4, 3), ("first", 4, 1), ("first", 2, 1), ("tick", 4, 1, 0),
        ("slant", 7, 0), ("tick", 2, 2, 0), ("first", 6, 3), ("tick", 4, 1, 1), ("tick", 1, 3, 1),
        ("first", 5, 3), ("tick", 3, 1, 0), ("first", 4, 2), ("first", 3, 1), ("slant", 7, 1),
        ("first", 5, 0), ("first", 6, 0), ("first", 5, 2), ("moments", 0), ("tick", 0, 3, 0),
        ("moments", 1), ("tick", 3, 1, 1), ("stack", 7), ("start", 7), ("tick", 2, 2, 1),
        ("tick", 1, 2, 0), ("moments", 2), ("second", 5, 3), ("tick", 3, 2, 1), ("second", 6, 3),
        ("first", 3, 2), ("tick", 1, 3, 0), ("tick", 4, 2, 1), ("second", 5, 2), ("first", 5, 1),
        ("first", 7, 3), ("first", 7, 0), ("second", 6, 0), ("tick", 4, 2, 0), ("tick", 5, 1, 0),
        ("second", 5, 0), ("tick", 5, 1, 1), ("first", 7, 1), ("moments", 3), ("first", 6, 1),
        ("first", 7, 2), ("second", 5, 1), ("second", 7, 3), ("tick", 3, 2, 0), ("tick", 6, 1, 1),
        ("first", 6, 2), ("tick", 2, 3, 1), ("second", 7, 0), ("tick", 6, 1, 0), ("moments", 4),
        ("tick", 2, 3, 0), ("third", 2), ("third", 1), ("tick", 3, 3, 1), ("tick", 7, 1, 1),
        ("tick", 7, 1, 0), ("tick", 5, 2, 1), ("second", 7, 1), ("tick", 5, 2, 0), ("tick", 4, 3, 1),
        ("second", 6, 1), ("tick", 4, 3, 0), ("third", 0), ("second", 7, 2), ("moments", 5),
        ("tick", 6, 2, 1), ("third", 4), ("second", 6, 2), ("tick", 7, 2, 0), ("tick", 7, 2, 1),
        ("tick", 3, 3, 0), ("third", 3), ("tick", 6, 2, 0), ("tick", 6, 3, 1), ("tick", 5, 3, 1),
        ("moments", 6), ("moments", 7), ("tick", 7, 3, 0), ("finish", 4), ("finish", 2), ("finish", 0),
        ("tick", 5, 3, 0), ("finish", 3), ("finish", 1), ("tick", 7, 3, 1), ("finish", 7), ("finish", 5),
        ("tick", 6, 3, 0), ("finish", 6),
    ),
}


def ordered(planes, kinds):
    early = kinds.count("zv")
    plan = ORDERS.get((planes, early, len(kinds) - early))
    if plan is None:
        plan = [action for _, action in sorted(schedule(planes, kinds), key=lambda e: e[0])]
    return plan


def schedule(planes, kinds):
    compute, spacing, lag, sub = SCHEDULE["compute"], SCHEDULE["first"], SCHEDULE["start"], SCHEDULE["sub"]
    cus = len(kinds)
    events = [(-2.0, ("slant", 0, 0))]
    for l in range(2):
        for n, name in enumerate((("slant", 0, 1), ("stack", 0), ("start", 0))):
            events.append((-1.0 + 0.1 * n + 0.4 * l, name + ((l,),)))
    events.append((-0.3, ("slant", 1, 0)))
    for cu in range(1, cus):
        at = compute * cu
        if cu > 1:
            events.append((at, ("slant", cu, 0)))
        events.append((at + 0.1 * compute, ("slant", cu, 1)))
        events.append((at + 0.2 * compute, ("stack", cu)))
    done = compute * cus
    for stage in range(3 + planes + 1):
        events.append((done + SCHEDULE["moments"] * stage, ("moments", stage)))
    gain = done + SCHEDULE["moments"] * (3 + planes) + 0.1
    now = SCHEDULE["begin"]
    for cu, kind in enumerate(kinds):
        at = now
        if cu > 0:
            events.append((max(compute * cu + 0.3 * compute, at - lag), ("start", cu)))
        at = max(at, compute * cu + 0.3 * compute + 0.1)
        for i, t in enumerate(far_first(planes)):
            events.append((at + i * sub, ("first", cu, t)))
        now += spacing[kind]
        at += (planes - 1) * sub
        if kind == "vz":
            at += SCHEDULE["second"] - (planes - 1) * sub
            for i, t in enumerate(far_first(planes)):
                events.append((at + i * sub, ("second", cu, t)))
            at += (planes - 1) * sub
        for tau in range(1, planes):
            at += SCHEDULE["hop"][kind]
            for way in range(2):
                events.append((at, ("tick", cu, tau, way)))
        if kind == "zv":
            at += SCHEDULE["third"]
            events.append((at, ("third", cu)))
            at += SCHEDULE["finish"]
        events.append((max(at + 0.01, gain), ("finish", cu)))
    return events


def fused(shapes, offsets, slant_weights, live, block_tile, image_slot):
    planes, grp, scratch, kinds = shapes
    blocks = block_tile.shape[0]
    hs, depth = offsets.shape[1:]
    angles = slant_weights.shape[0]
    any_space = pl.BlockSpec(memory_space=pl.ANY)
    return pl.pallas_call(
        functools.partial(fused_kernel, (planes, grp, kinds)),
        out_shape=pltpu.VMEM((IMG_DEV, 2 * angles, depth), jnp.bfloat16),
        in_specs=[any_space] * 5,
        out_specs=pl.BlockSpec(memory_space=pltpu.VMEM),
        scratch_shapes=scratch,
        compiler_params=pltpu.CompilerParams(
            collective_id=2, has_side_effects=True, vmem_limit_bytes=VMEM_LIMIT
        ),
        name="calibrated_stack",
    )(
        offsets.reshape(blocks, 2, hs, depth),
        live.T,
        block_tile.reshape(1, blocks),
        image_slot.reshape(1, blocks),
        slant_weights.T,
    )


def buffers(planes, blocks, hs, depth, angles, images):
    wide, per = 2 * LANES, 16
    cus = (depth // wide) * (angles // per)
    pieces = 2 * cus
    tile = (per // 2, 16, LANES)
    dma = pltpu.SemaphoreType.DMA
    bf, f32, i32 = jnp.bfloat16, jnp.float32, jnp.int32
    early = (5 * cus + 4) // 8
    kinds = ("zv",) * early + ("vz",) * (cus - early)
    memory = [
        ((angles, 2 * blocks), i32),
        ((1, blocks), i32),
        ((1, blocks), i32),
        ((hs, angles), bf),
        ((2, blocks, hs, depth), bf),
        ((angles * 8, 8 * hs), bf),
        ((images, 2 * blocks), bf),
        ((8 + blocks, LANES), i32),
        ((8 + blocks, LANES), i32),
        ((2, blocks, LANES), i32),
        ((angles, 8, LANES), f32),
        ((2, per, 2 * blocks, wide), bf),
        ((pieces, planes, 2) + tile, f32),
        ((pieces, planes, 2) + tile, bf),
        ((pieces, planes, 2) + tile, bf),
        ((pieces, planes) + tile, bf),
        ((pieces, 2, planes - 1, 2) + tile, bf),
        ((2, per * 8, LANES), f32),
        ((IMG_DEV, angles, depth), bf),
        ((7, 8, LANES), f32),
        ((5, 8, LANES), f32),
        ((angles, LANES), f32),
    ]
    size = sum(math.prod(s) * jnp.dtype(d).itemsize for s, d in memory)
    scratch = [pltpu.VMEM(s, d) for s, d in memory]
    depths = depth // wide
    scratch += [
        dma((4,)), dma((depths,)), dma((depths + 1,)), dma((depths + 1,)), dma((1,)), dma((1,)),
        dma((1,)), dma((cus, planes)),
        dma((2,)), dma((early + (cus - early) * planes,)),
        dma((2, 2, planes - 1)), dma((early + 2 * (cus - early), 2, planes - 1)),
        dma((1,)), dma((1,)), dma((5,)), dma((5,)),
    ]
    return size, scratch, kinds


def local(offsets, slant_weights, live, block_tile, image_slot):
    shots, grp = lax.axis_size("shot"), lax.axis_size("grp")
    planes = shots // PAIR
    blocks = block_tile.shape[0]
    hs, depth = offsets.shape[1:]
    angles = slant_weights.shape[0]
    images = shots * IMG_DEV * grp
    size, scratch, kinds = buffers(planes, blocks, hs, depth, angles, images)
    args = (offsets, slant_weights, live, block_tile, image_slot)
    if grp == 4 and size + (2 << 20) <= VMEM_LIMIT:
        return fused((planes, grp, scratch, kinds), *args)
    return staged(*args)


def solution(mesh):
    placed = (
        P(("shot", "grp"), None, None),
        P(),
        P(("shot", "grp"), None),
        P(("shot", "grp"), None),
        P(("shot", "grp")),
    )
    return jax.shard_map(
        local, mesh=mesh, in_specs=placed, out_specs=P(("shot", "grp"), None, None), check_vma=False
    )
```

```python
import functools
import math

import jax
import jax.numpy as jnp
from jax import lax
from jax.experimental import pallas as pl
from jax.experimental.pallas import tpu as pltpu
from jax.sharding import PartitionSpec as P

IMG_DEV = 4
PAIR = 2
LANES = 128
UNROLL = 8
MESH = pl.DeviceIdType.MESH
VMEM_LIMIT = 62 * 1024 * 1024
SLANT_UNROLL = 2
STACK_UNROLL = 4
SCHEDULE = {
    "compute": 3.19, "first": {"zv": 7.98, "vz": 14.69}, "begin": 3.59, "start": 15.93, "sub": 2.8,
    "second": 19.16, "hop": {"zv": 14.36, "vz": 19.05}, "third": 32.32, "finish": 0.39,
    "moments": 16.35,
}


def place(grp):
    shot, g = lax.axis_index("shot"), lax.axis_index("grp")
    return lax.div(shot, PAIR), lax.rem(shot, PAIR) * grp + g


def at(plane, spot, grp):
    return (plane * PAIR + lax.div(spot, grp), lax.rem(spot, grp))


def share(spot, width, depth):
    start = spot * width
    return lax.div(start, depth), pl.multiple_of(lax.rem(start, depth), LANES)


def relative(spot, grp, r):
    mid = grp // 2
    pair, rest = lax.div(spot, grp), lax.rem(spot, grp)
    m, c = lax.div(rest, 2), lax.rem(rest, 2)
    rp, rm, rc = r // grp, (r % grp) // 2, r % 2
    pair, m, c = lax.rem(pair + rp, PAIR), lax.rem(m + rm, mid), lax.rem(c + rc, 2)
    return (pair * mid + m) * 2 + c


def orders(grp):
    size = PAIR * grp
    far = list(range(grp + 2, size))
    side = list(range(grp, grp + 2))
    ahead = list(range(2, grp))
    turn = []
    for i in range(max(len(far), len(ahead))):
        for group in (far, side, ahead):
            turn += group[i : i + 1]
    return [1] + turn


def exchange_kernel(
    grp, off, aux, w_in, part, mom, w, raw, aux_in, codes, acc, seg, send, recv, asend, arecv, lsem
):
    size = PAIR * grp
    plane, spot = place(grp)
    blocks, depth, width = off.shape[0], off.shape[3], raw.shape[3]
    angles, images = w.shape[1], acc.shape[0]
    j, first = share(spot, width, depth)
    mine = pltpu.make_async_copy(off.at[:, j, :, pl.ds(first, width)], raw.at[0], lsem.at[0])
    mine.start()
    own_codes = pltpu.make_async_copy(aux, codes.at[0], lsem.at[1])
    own_codes.start()
    weigh = pltpu.make_async_copy(w_in, w, lsem.at[size + 1])
    weigh.start()
    barrier = pltpu.get_barrier_semaphore()
    for r in range(1, size):
        pl.semaphore_signal(
            barrier, inc=1, device_id=at(plane, relative(spot, grp, r), grp), device_id_type=MESH
        )
    pl.semaphore_wait(barrier, size - 1)
    data, notes = {}, {}
    for r in orders(grp):
        peer = relative(spot, grp, r)
        pj, pfirst = share(peer, width, depth)
        dev = at(plane, peer, grp)
        notes[r] = pltpu.make_async_remote_copy(
            src_ref=aux,
            dst_ref=aux_in.at[r],
            send_sem=asend.at[r - 1],
            recv_sem=arecv.at[r - 1],
            device_id=dev,
            device_id_type=MESH,
        )
        data[r] = pltpu.make_async_remote_copy(
            src_ref=off.at[:, pj, :, pl.ds(pfirst, width)],
            dst_ref=raw.at[r],
            send_sem=send.at[r - 1],
            recv_sem=recv.at[r - 1],
            device_id=dev,
            device_id_type=MESH,
        )
    for r in orders(grp):
        notes[r].start()
    for r in orders(grp):
        data[r].start()

    acc[...] = jnp.zeros_like(acc)
    seg[blocks] = jnp.zeros((angles, width), jnp.float32)
    row = lax.broadcasted_iota(jnp.int32, (angles, width), 0)
    weigh.wait()
    weights = w[...].astype(jnp.float32).T.astype(jnp.bfloat16)
    square = jnp.zeros((angles, width), jnp.float32)
    count = jnp.zeros((angles, width), jnp.float32)
    for r in [0] + orders(grp):
        if r:
            notes[r].wait()
            code = pltpu.make_async_copy(aux_in.at[r], codes.at[r], lsem.at[r + 1])
            code.start()
            code.wait()
            data[r].wait()
        else:
            own_codes.wait()
            mine.wait()

        def slant(i, carry, r=r):
            square, count = carry
            start = i * UNROLL
            x = jnp.concatenate([raw[r, start + t] for t in range(UNROLL)], axis=1)
            y = jnp.dot(weights, x, preferred_element_type=jnp.float32)
            for t in range(UNROLL):
                alive = row < codes[r, 1 + j, start + t]
                slanted = jnp.where(alive, y[:, t * width : (t + 1) * width], 0.0)
                slanted = slanted.astype(jnp.bfloat16).astype(jnp.float32)
                square += slanted * slanted
                count += jnp.where(alive, 1.0, 0.0)
                seg[start + t] = slanted + seg[codes[r, 0, start + t]]
            return square, count

        square, count = lax.fori_loop(0, blocks // UNROLL, slant, (square, count))

        def stack(i, _, r=r):
            start = i * UNROLL
            line, column = lax.div(start, LANES), lax.rem(start, LANES)
            for t in range(UNROLL):
                acc[start + t] += seg[codes[r, 3 + line, column + t]]
            return 0

        lax.fori_loop(0, images // UNROLL, stack, 0)

    def narrow(i, _):
        start = pl.multiple_of(i * UNROLL, UNROLL)
        part[pl.ds(start, UNROLL)] = acc[pl.ds(start, UNROLL)].astype(jnp.bfloat16)
        return 0

    lax.fori_loop(0, images // UNROLL, narrow, 0)
    lane = lax.broadcasted_iota(jnp.int32, (angles, LANES), 1)
    square = jnp.sum(square, axis=1, keepdims=True)
    count = jnp.sum(count, axis=1, keepdims=True)
    both = jnp.where(lane == 0, square, jnp.where(lane == 1, count, 0.0))
    both = jnp.concatenate([both, jnp.zeros((LANES - angles, LANES), jnp.float32)], axis=0)
    mom[...] = both.T[: mom.shape[0]]


def gather_kernel(
    grp, part, mom, out, held, total, fin, pin, qin, half_sum, zs, zr, ps, pr, qs, qr, fs, fr, lsem
):
    size = PAIR * grp
    planes = held.shape[1] + 1
    plane, spot = place(grp)
    pieces, rows, angles, width = held.shape[2:]
    depth = out.shape[2]
    chunk = pieces * rows
    lower = jnp.where(plane < planes // 2, 1, 0)
    barrier = pltpu.get_barrier_semaphore()
    for r in range(1, size):
        pl.semaphore_signal(
            barrier, inc=1, device_id=at(plane, lax.rem(spot + r, size), grp), device_id_type=MESH
        )
    for r in range(1, planes):
        pl.semaphore_signal(
            barrier, inc=1, device_id=at(lax.rem(plane + r, planes), spot, grp), device_id_type=MESH
        )
    pl.semaphore_wait(barrier, size + planes - 2)

    def along(up):
        spot_on_line = plane * up + (planes - 1 - plane) * (1 - up)
        following = lax.rem(plane + 2 * up - 1 + planes, planes)
        return 1 - up, spot_on_line, following

    def rows_of(up, s, h):
        target = (planes - 1 - s) * up + s * (1 - up)
        return target * chunk + h * rows

    def hop(up, s, h, source):
        way, _, following = along(up)
        return pltpu.make_async_remote_copy(
            src_ref=source,
            dst_ref=held.at[way, s, h],
            send_sem=zs.at[way, s, h],
            recv_sem=zr.at[way, s, h],
            device_id=at(following, spot, grp),
            device_id_type=MESH,
        )

    def begin(s):
        @pl.when(along(lower)[1] == 0)
        def _():
            for h in range(pieces):
                hop(lower, s, h, part.at[pl.ds(rows_of(lower, s, h), rows)]).start()

    def step(up, s, h):
        way, here, _ = along(up)
        end = planes - 1 - s

        @pl.when((here > 0) & (here <= end))
        def _():
            hop(up, s, h, held.at[way, s, h]).wait_recv()

        @pl.when((here > 0) & (here < end))
        def _():
            start = rows_of(up, s, h)

            def add(i, _):
                value = held[way, s, h, i].astype(jnp.float32) + part[start + i].astype(jnp.float32)
                held[way, s, h, i] = value.astype(jnp.bfloat16)
                return 0

            lax.fori_loop(0, rows, add, 0)
            hop(up, s, h, held.at[way, s, h]).start()

        @pl.when((here > 0) & (here == end))
        def _():
            def add(i, _):
                total[h * rows + i] += held[way, s, h, i].astype(jnp.float32)
                return 0

            lax.fori_loop(0, rows, add, 0)

    def finish(up, s, h):
        way, here, _ = along(up)

        @pl.when(here < planes - 1 - s)
        def _():
            hop(up, s, h, held.at[way, s, h]).wait_send()

    near = [
        pltpu.make_async_remote_copy(
            src_ref=mom,
            dst_ref=pin.at[r - 1],
            send_sem=ps.at[r - 1],
            recv_sem=pr.at[r - 1],
            device_id=at(plane, lax.rem(spot + r, size), grp),
            device_id_type=MESH,
        )
        for r in range(1, size)
    ]
    for copy in near:
        copy.start()
    begin(0)
    total[...] = part[pl.ds(plane * chunk, chunk)].astype(jnp.float32)
    moments = mom[...]
    for copy in near:
        copy.wait()
    for r in range(1, size):
        moments += pin[r - 1]
    half_sum[...] = moments
    wide = [
        pltpu.make_async_remote_copy(
            src_ref=half_sum,
            dst_ref=qin.at[r - 1],
            send_sem=qs.at[r - 1],
            recv_sem=qr.at[r - 1],
            device_id=at(lax.rem(plane + r, planes), spot, grp),
            device_id_type=MESH,
        )
        for r in range(1, planes)
    ]
    for copy in wide:
        copy.start()
    for s in range(1, planes - 1):
        begin(s)
    for s in range(planes - 1):
        for up in (lower, 1 - lower):
            for h in range(pieces):
                step(up, s, h)
    for copy in wide:
        copy.wait()
    moments = half_sum[...]
    for r in range(1, planes):
        moments += qin[r - 1]
    gain = lax.rsqrt(moments[0:1] / moments[1:2] + 1e-06)
    gain = jnp.broadcast_to(gain, (LANES, LANES)).T[:angles]

    def body(i, _):
        fin[i] = (total[i] * gain).astype(jnp.bfloat16)
        return 0

    lax.fori_loop(0, chunk, body, 0)

    each = chunk // size
    j, first = share(spot, width, depth)
    view = out.at[:, pl.ds(pl.multiple_of(j * angles, angles), angles), pl.ds(first, width)]
    last = pltpu.make_async_copy(fin.at[pl.ds(spot * each, each)], view, lsem.at[1])
    final = []
    for r in range(1, size):
        peer = lax.rem(spot + r, size)
        final.append(
            pltpu.make_async_remote_copy(
                src_ref=fin.at[pl.ds(peer * each, each)],
                dst_ref=view,
                send_sem=fs.at[r - 1],
                recv_sem=fr.at[r - 1],
                device_id=at(plane, peer, grp),
                device_id_type=MESH,
            )
        )
    for copy in final:
        copy.start()
    last.start()
    last.wait()
    for copy in final:
        copy.wait()
    for s in range(planes - 1):
        for up in (lower, 1 - lower):
            for h in range(pieces):
                finish(up, s, h)


def staged(offsets, slant_weights, live, block_tile, image_slot):
    shots, grp = lax.axis_size("shot"), lax.axis_size("grp")
    planes, size = shots // PAIR, PAIR * grp
    blocks = block_tile.shape[0]
    hs, depth = offsets.shape[1:]
    angles = slant_weights.shape[0]
    width = 2 * depth // size
    tile_rows = IMG_DEV * grp
    images = shots * tile_rows
    per_plane = images // planes
    any_space = pl.BlockSpec(memory_space=pl.ANY)
    vmem = pl.BlockSpec(memory_space=pltpu.VMEM)
    dma = pltpu.SemaphoreType.DMA

    cutoff = jnp.sum(live.reshape(blocks, 2, angles), axis=2)
    image = block_tile[:, 0] * tile_rows + image_slot
    index = jnp.arange(blocks, dtype=jnp.int32)
    same = (image[:, None] == image[None, :]) & (index[None, :] < index[:, None])
    before = jnp.max(jnp.where(same, index[None, :], -1), axis=1)
    found = image[None, :] == jnp.arange(images, dtype=jnp.int32)[:, None]
    final = jnp.max(jnp.where(found, index[None, :], -1), axis=1)
    final = jnp.where(final < 0, blocks, final).reshape(images // LANES, LANES)
    before = jnp.where(before < 0, blocks, before)
    aux = jnp.concatenate([before[None], cutoff.T], axis=0)
    aux = jnp.concatenate([jnp.pad(aux, ((0, 0), (0, LANES - blocks))), final], axis=0)
    aux = jnp.pad(aux, ((0, -aux.shape[0] % 8), (0, 0)))

    part, mom = pl.pallas_call(
        functools.partial(exchange_kernel, grp),
        out_shape=(
            jax.ShapeDtypeStruct((images, angles, width), jnp.bfloat16),
            jax.ShapeDtypeStruct((8, LANES), jnp.float32),
        ),
        in_specs=[any_space, vmem, any_space],
        out_specs=(vmem, vmem),
        scratch_shapes=[
            pltpu.VMEM((hs, angles), jnp.bfloat16),
            pltpu.VMEM((size, blocks, hs, width), jnp.bfloat16),
            pltpu.VMEM((size,) + aux.shape, jnp.int32),
            pltpu.SMEM((size,) + aux.shape, jnp.int32),
            pltpu.VMEM((images, angles, width), jnp.float32),
            pltpu.VMEM((blocks + 1, angles, width), jnp.float32),
            dma((size - 1,)),
            dma((size - 1,)),
            dma((size - 1,)),
            dma((size - 1,)),
            dma((size + 2,)),
        ],
        compiler_params=pltpu.CompilerParams(
            collective_id=0, has_side_effects=True, vmem_limit_bytes=62 * 1024 * 1024
        ),
        name="exchange",
    )(offsets.reshape(blocks, 2, hs, depth), aux, slant_weights.T)

    moments = (8, LANES)
    pieces = 4
    lines = (2, planes - 1, pieces)
    return pl.pallas_call(
        functools.partial(gather_kernel, grp),
        out_shape=jax.ShapeDtypeStruct((IMG_DEV, 2 * angles, depth), jnp.bfloat16),
        in_specs=[vmem, vmem],
        out_specs=any_space,
        scratch_shapes=[
            pltpu.VMEM(lines + (per_plane // pieces, angles, width), jnp.bfloat16),
            pltpu.VMEM((per_plane, angles, width), jnp.float32),
            pltpu.VMEM((per_plane, angles, width), jnp.bfloat16),
            pltpu.VMEM((size - 1,) + moments, jnp.float32),
            pltpu.VMEM((planes - 1,) + moments, jnp.float32),
            pltpu.VMEM(moments, jnp.float32),
            dma(lines),
            dma(lines),
            dma((size - 1,)),
            dma((size - 1,)),
            dma((planes - 1,)),
            dma((planes - 1,)),
            dma((size - 1,)),
            dma((size - 1,)),
            dma((2,)),
        ],
        compiler_params=pltpu.CompilerParams(
            collective_id=1, has_side_effects=True, vmem_limit_bytes=60 * 1024 * 1024
        ),
        name="gather",
    )(part, mom)


def round_up(value, unit):
    return -(-value // unit) * unit


def fused_kernel(
    shape, off, live_in, tile_in, slot_in, w_in, out,
    live, tile, slot, weights, raw, wb, onehot, mine, theirs, cuts, squares, sl,
    own, part, rx1, rxv, held, ft, fin, sums, pin, gains,
    load_sem, in_sem, core_s, core_r, meta_s, meta_r, s1s, s1r, vs, vr, zs, zr, fs, fr, ms, mr,
):
    planes, grp, kinds = shape
    shot, g = lax.axis_index("shot"), lax.axis_index("grp")
    z, y = lax.div(shot, PAIR), lax.rem(shot, PAIR)
    x, c = lax.div(g, 2), lax.rem(g, 2)
    blocks, hs, depth = raw.shape[1:]
    angles = live.shape[0]
    images = onehot.shape[0]
    img_dev = out.shape[0]
    per, wide = sl.shape[1], sl.shape[3]
    pairs = per // 2
    depths, groups = depth // wide, angles // per
    cus = depths * groups
    early = 2 * kinds.count("zv")
    late_count = 2 * cus - early

    def device(step=0, fy=False, fx=False, fc=False):
        yy = 1 - y if fy else y
        xx = 1 - x if fx else x
        cc = 1 - c if fc else c
        return ((z + step) * PAIR + yy, xx * 2 + cc)

    core_peer, x_peer, y_peer = device(fc=True), device(fx=True), device(fy=True)
    first_peer = (x_peer, y_peer)
    second_peer = (y_peer, x_peer)

    def remote(src, dst, send_sem, recv_sem, peer):
        return pltpu.make_async_remote_copy(
            src_ref=src, dst_ref=dst, send_sem=send_sem, recv_sem=recv_sem,
            device_id=peer, device_id_type=MESH,
        )

    barrier = pltpu.get_barrier_semaphore()

    def greet(peer):
        pl.semaphore_signal(barrier, inc=1, device_id=peer, device_id_type=MESH)

    for peer in (core_peer, x_peer, y_peer):
        greet(peer)

    @pl.when(z > 0)
    def _():
        greet(device(step=-1))

    @pl.when(z < planes - 1)
    def _():
        greet(device(step=1))

    loads = [
        pltpu.make_async_copy(src, dst, load_sem.at[n])
        for n, (src, dst) in enumerate(
            ((w_in, weights), (live_in, live), (tile_in, tile), (slot_in, slot))
        )
    ]
    for copy in loads:
        copy.start()
    own_in = [
        pltpu.make_async_copy(
            off.at[:, c, :, pl.ds(d * wide, wide)],
            raw.at[0, :, :, pl.ds(d * wide, wide)],
            in_sem.at[d],
        )
        for d in range(depths)
    ]
    for copy in own_in:
        copy.start()
    spans = [(0, LANES), (LANES, wide - LANES)] + [(d * wide, wide) for d in range(1, depths)]
    core_in = [
        remote(
            off.at[:, 1 - c, :, pl.ds(lane, size)],
            raw.at[1, :, :, pl.ds(lane, size)],
            core_s.at[n], core_r.at[n], core_peer,
        )
        for n, (lane, size) in enumerate(spans)
    ]
    meta = remote(mine, theirs, meta_s.at[0], meta_r.at[0], core_peer)

    eight = 8
    for copy in loads:
        copy.wait()
    ones = jnp.ones((angles, LANES), jnp.bfloat16)
    spot = lax.broadcasted_iota(jnp.int32, (blocks, 2 * blocks), 1)
    block = lax.broadcasted_iota(jnp.int32, (blocks, 2 * blocks), 0)

    def cutoff(j):
        pick = jnp.where(spot == 2 * block + j, 1.0, 0.0).astype(jnp.bfloat16)
        flags = lax.dot_general(
            pick, live[...].astype(jnp.float32).astype(jnp.bfloat16),
            (((1,), (1,)), ((), ())), preferred_element_type=jnp.float32,
        )
        total = jnp.dot(flags.astype(jnp.bfloat16), ones, preferred_element_type=jnp.float32)
        return total.astype(jnp.int32)

    mine[0:eight] = jnp.full((eight, LANES), -1, jnp.int32)
    mine[0:1, 0:blocks] = tile[...] * (img_dev * grp) + slot[...]
    mine[eight : eight + blocks] = cutoff(1 - c)
    cuts[0] = cutoff(c)

    ends = jnp.where(z == 0, 1, 0) + jnp.where(z == planes - 1, 1, 0)
    pl.semaphore_wait(barrier, 5 - ends)
    core_in[0].start()
    meta.start()
    for copy in core_in[1:]:
        copy.start()

    rows = angles * eight
    spread = lax.broadcasted_iota(jnp.int32, (rows, angles), 0)
    which = lax.broadcasted_iota(jnp.int32, (rows, angles), 1)
    pick = jnp.where(lax.div(spread, eight) == which, 1.0, 0.0).astype(jnp.bfloat16)
    tall = lax.dot_general(
        pick, weights[...], (((1,), (1,)), ((), ())), preferred_element_type=jnp.float32
    ).astype(jnp.bfloat16)
    line = lax.broadcasted_iota(jnp.int32, (hs, eight * hs), 0)
    column = lax.broadcasted_iota(jnp.int32, (hs, eight * hs), 1)
    copies = jnp.where(lax.rem(column, hs) == line, 1.0, 0.0).astype(jnp.bfloat16)
    full = jnp.dot(tall, copies, preferred_element_type=jnp.float32)
    line = lax.broadcasted_iota(jnp.int32, full.shape, 0)
    column = lax.broadcasted_iota(jnp.int32, full.shape, 1)
    wb[...] = jnp.where(lax.rem(line, eight) == lax.div(column, hs), full, 0.0).astype(jnp.bfloat16)
    squares[...] = jnp.zeros_like(squares)

    def slant(cu, r, tiles=(0, 1)):
        d, a0 = cu // groups, cu % groups * per
        lane0, size = tiles[0] * LANES, len(tiles) * LANES
        if r == 0 and cu % groups == 0:
            own_in[d].wait()
        if r == 1 and cu == 0 and lane0 == 0:
            meta.wait_recv()
            cuts[1] = theirs[eight : eight + blocks]
            select_rows()
        if r == 1 and cu % groups == 0:
            core_in[spans.index((d * wide + lane0, size))].wait_recv()

        def body(i, _):
            lhs = wb[a0 * eight : (a0 + per) * eight]
            lanes = slice(d * wide + lane0, d * wide + lane0 + size)
            a = lax.broadcasted_iota(jnp.int32, (per, 2 * eight, LANES), 0) + a0
            total = squares[a0 : a0 + per]
            for n in range(SLANT_UNROLL):
                start = (i * SLANT_UNROLL + n) * 2 * eight
                alive = cuts[r, pl.ds(start, 2 * eight)][None] > a
                ys = []
                for k in range(2):
                    data = raw[r, pl.ds(start + k * eight, eight), :, lanes]
                    data = data.reshape(eight * hs, size)
                    y = jnp.dot(lhs, data, preferred_element_type=jnp.float32)
                    ys.append(y.reshape(per, eight, size))
                for k in range(len(tiles)):
                    cut = slice(k * LANES, (k + 1) * LANES)
                    to = slice(lane0 + k * LANES, lane0 + (k + 1) * LANES)
                    v = jnp.concatenate([ys[0][:, :, cut], ys[1][:, :, cut]], axis=1)
                    v = jnp.where(alive, v, 0.0)
                    q = v * v
                    total += q[:, :eight] + q[:, eight:]
                    sl[cu % 2, :, pl.ds(r * blocks + start, 2 * eight), to] = v.astype(jnp.bfloat16)
            squares[a0 : a0 + per] = total
            return 0

        lax.fori_loop(0, blocks // (2 * eight * SLANT_UNROLL), body, 0)

    def select_rows():
        lanes = round_up(2 * blocks, LANES)
        rest = jnp.full((eight, lanes - LANES), -1, jnp.int32)
        a_row = jnp.concatenate([jnp.broadcast_to(mine[0:1], (eight, LANES)), rest], axis=1)
        b_row = jnp.concatenate([jnp.broadcast_to(theirs[0:1], (eight, LANES)), rest], axis=1)
        b_row = pltpu.roll(b_row, blocks, 1)
        lane = lax.broadcasted_iota(jnp.int32, a_row.shape, 1)
        row = jnp.where(lane < blocks, a_row, b_row)
        mask = y * (img_dev * grp) + g * img_dev
        row = lax.bitwise_xor(row, jnp.full(row.shape, 0, jnp.int32) + mask)
        number = lax.broadcasted_iota(jnp.int32, (images, lanes), 0)
        hit = jnp.where(number == row[0:1], 1.0, 0.0).astype(jnp.bfloat16)
        onehot[...] = hit[:, : 2 * blocks]

    def stack(cu, tiles=(0, 1)):
        near = slice(tiles[0] * LANES, (tiles[-1] + 1) * LANES)

        def body(i, _):
            for o in range(STACK_UNROLL):
                m = i * STACK_UNROLL + o
                ys = [
                    jnp.dot(onehot[...], sl[cu % 2, 2 * m + k, :, near], preferred_element_type=jnp.float32)
                    for k in range(2)
                ]
                for n, l in enumerate(tiles):
                    p = 2 * cu + l
                    cut = slice(n * LANES, (n + 1) * LANES)
                    for t in range(planes):
                        for ry in range(2):
                            for rx in range(2):
                                r = ((t * 2 + ry) * 2 + rx) * eight
                                v = [ys[k][r : r + eight, cut] for k in range(2)]
                                v = jnp.concatenate(v, axis=0)
                                one, two = (rx, ry) if l == 0 else (ry, rx)
                                if one == 0:
                                    own[p, t, two, m] = v
                                else:
                                    part[p, t, two, m] = v.astype(jnp.bfloat16)
            return 0

        lax.fori_loop(0, pairs // STACK_UNROLL, body, 0)

    def late(cu):
        return kinds[cu] == "vz"

    def s1(cu, l, t):
        p = 2 * cu + l
        return remote(part.at[p, t], rx1.at[p, t], s1s.at[0], s1r.at[cu, t], first_peer[l])

    def across_slot(cu, t):
        return early // 2 + (cu - early // 2) * planes + t if late(cu) else cu

    def across(cu, l, t, source):
        p, slot = 2 * cu + l, across_slot(cu, t)
        kind = 1 if late(cu) else 0
        return remote(source, rxv.at[p, t], vs.at[kind], vr.at[slot], second_peer[l])

    def arrived(region, sem):
        remote(region, region, ms.at[0], sem, core_peer).wait_recv()

    def messages(cu):
        return [(0,), (1,)] if late(cu) else [(0, 1)]

    def hop(cu, tiles, way, s, source):
        p, n = pl.ds(2 * cu + tiles[0], len(tiles)), pl.ds(0, 1 if late(cu) else 2)
        kind = 1 if late(cu) else 0
        slot = early // 2 + 2 * (cu - early // 2) + tiles[0] if late(cu) else cu
        return remote(
            source, held.at[p, way, s, n], zs.at[kind, way, s], zr.at[slot, way, s],
            device(step=1 - 2 * way),
        )

    def begin(cu, t):
        for tiles in messages(cu):
            p = pl.ds(2 * cu + tiles[0], len(tiles))
            source = rx1.at[p, t, pl.ds(0, 1 if late(cu) else 2)]
            if t > 0:
                @pl.when(z == 0)
                def _(tiles=tiles, source=source):
                    hop(cu, tiles, 0, planes - 1 - t, source).start()
            if t < planes - 1:
                @pl.when(z == planes - 1)
                def _(tiles=tiles, source=source):
                    hop(cu, tiles, 1, t, source).start()

    def start(cu, tiles=(0, 1)):
        for t in far_first(planes):
            for l in tiles:
                s1(cu, l, t).start()

    def first(cu, t):
        arrived(rx1.at[pl.ds(2 * cu, 2), t], s1r.at[cu, t])
        for l in range(2):
            p = 2 * cu + l
            for k in (1, 0):
                total = own[p, t, k] + rx1[p, t, k].astype(jnp.float32)
                own[p, t, k] = total
                rx1[p, t, k] = total.astype(jnp.bfloat16)
            if late(cu):
                across(cu, l, t, rx1.at[p, t, 1]).start()
        if not late(cu):
            begin(cu, t)

    def second(cu, t):
        arrived(rxv.at[pl.ds(2 * cu, 2), t], vr.at[across_slot(cu, t)])
        for l in range(2):
            p = 2 * cu + l
            total = own[p, t, 0] + rxv[p, t].astype(jnp.float32)
            own[p, t, 0] = total
            rx1[p, t, 0] = total.astype(jnp.bfloat16)
        begin(cu, t)

    def tick(cu, tau, way):
        here = z if way == 0 else planes - 1 - z
        s = tau - here
        target = planes - 1 - s if way == 0 else s
        n = 1 if late(cu) else 2

        @pl.when((here >= 1) & (s >= 0))
        def _():
            for tiles in messages(cu):
                p = pl.ds(2 * cu + tiles[0], len(tiles))
                message = held.at[p, way, s, pl.ds(0, n)]
                hop(cu, tiles, way, s, message).wait_recv()
                for l in tiles:
                    p = 2 * cu + l
                    for k in range(n):
                        value = held[p, way, s, k].astype(jnp.float32) + own[p, target, k]
                        if tau < planes - 1:
                            held[p, way, s, k] = value.astype(jnp.bfloat16)
                        else:
                            own[p, target, k] = value
                if tau < planes - 1:
                    hop(cu, tiles, way, s, message).start()

    def third(cu):
        for l in range(2):
            p = 2 * cu + l
            rx1[p, z, 1] = own[p, z, 1].astype(jnp.bfloat16)
            across(cu, l, 0, rx1.at[p, z, 1]).start()

    def leave(line, lanes):
        row = pl.multiple_of(c * angles + line.start, per)
        view = out.at[:, pl.ds(row, line.size), pl.ds(lanes.start, lanes.size)]
        return remote(fin.at[:, line, lanes], view, fs.at[0], fr.at[0], core_peer)

    def finish(cu):
        if not late(cu):
            arrived(rxv.at[pl.ds(2 * cu, 2), 0], vr.at[across_slot(cu, 0)])
        a0, lane0 = cu % groups * per, cu // groups * wide
        for l in range(2):
            p = 2 * cu + l
            total = own[p, z, 0]
            if not late(cu):
                total += rxv[p, 0].astype(jnp.float32)
            ft[l] = total.reshape(per * eight, LANES)
            lanes = slice(lane0 + l * LANES, lane0 + (l + 1) * LANES)
            for r in range(eight):
                v = ft[l, pl.ds(r, per, stride=eight)] * gains[a0 : a0 + per]
                if r < img_dev:
                    row = pl.multiple_of(c * angles + a0, per)
                    out[r, pl.ds(row, per), lanes] = v.astype(jnp.bfloat16)
                else:
                    fin[r - img_dev, a0 : a0 + per, lanes] = v.astype(jnp.bfloat16)
        leave(pl.ds(a0, per), pl.ds(lane0, wide)).start()

    def moment(stage):
        peer = (core_peer, x_peer, y_peer)[stage]
        return remote(sums.at[stage], pin.at[stage], ms.at[stage], mr.at[stage], peer)

    def passing(way):
        n = 3 + way
        return remote(sums.at[n + 1], pin.at[n], ms.at[n], mr.at[n], device(step=1 - 2 * way))

    def moments(stage):
        if stage == 0:
            total = jnp.sum(jnp.sum(squares[...], axis=1), axis=1, keepdims=True)
            count = jnp.sum(live[...].astype(jnp.float32), axis=1, keepdims=True)
            lane = lax.broadcasted_iota(jnp.int32, (angles, LANES), 1)
            both = jnp.where(lane == 0, total, jnp.where(lane == 1, count, 0.0))
            both = jnp.concatenate([both, jnp.zeros((LANES - angles, LANES), jnp.float32)], axis=0)
            sums[0] = both.T[:eight]
            moment(0).start()
            return
        if stage <= 3:
            moment(stage - 1).wait_recv()
            sums[stage] = sums[stage - 1] + pin[stage - 1]
            if stage < 3:
                moment(stage).start()
                return
            sums[6] = sums[3]
        tau = stage - 3
        if tau < planes:
            for way in range(2):
                here = z if way == 0 else planes - 1 - z

                @pl.when(here == tau)
                def _(way=way):
                    if tau > 0:
                        passing(way).wait_recv()
                        sums[6] = sums[6] + pin[3 + way]
                        sums[4 + way] = sums[3] + pin[3 + way]
                    else:
                        sums[4 + way] = sums[3]
                    if tau < planes - 1:
                        passing(way).start()
        else:
            total = sums[6]
            gain = lax.rsqrt(total[0:1] / (depth * total[1:2]) + 1e-06)
            gains[...] = jnp.broadcast_to(gain, (LANES, LANES)).T[:angles]

    run = {
        "slant": slant, "stack": stack, "start": start, "first": first, "second": second,
        "tick": tick, "third": third, "finish": finish, "moments": moments,
    }
    for action in ordered(planes, kinds):
        run[action[0]](*action[1:])

    meta.wait_send()
    for copy in core_in:
        copy.wait_send()
    remote(part, rx1, s1s.at[0], s1r.at[0, 0], core_peer).wait_send()
    if early:
        region = rxv.at[pl.ds(0, early), 0]
        remote(region, region, vs.at[0], vr.at[0], core_peer).wait_send()
    if late_count:
        region = rxv.at[pl.ds(early, late_count)]
        remote(region, region, vs.at[1], vr.at[0], core_peer).wait_send()
    for way in range(2):
        here = z if way == 0 else planes - 1 - z

        @pl.when(here < planes - 1)
        def _(way=way):
            passing(way).wait_send()

        for s in range(planes - 1):
            @pl.when(here < planes - 1 - s)
            def _(way=way, s=s):
                for kind, region in enumerate(
                    (
                        held.at[pl.ds(0, early), way, s],
                        held.at[pl.ds(early, late_count), way, s, pl.ds(0, 1)],
                    )
                ):
                    if (early, late_count)[kind]:
                        remote(
                            region, region, zs.at[kind, way, s], zr.at[0, way, s], core_peer
                        ).wait_send()
    for stage in range(3):
        moment(stage).wait_send()
    leave(pl.ds(0, angles), pl.ds(0, depth)).wait()


def far_first(planes):
    return [planes - 1 - i // 2 if i % 2 == 0 else i // 2 for i in range(planes)]


STEPS = ("slant", "stack", "start", "first", "second", "tick", "third", "finish", "moments")
ORDERS = {
    (4, 5, 3): (
        (0, 0, 0), (0, 1, 0), (0, 0, 1, (0,)), (1, 0, (0,)), (2, 0, (0,)),
        (0, 0, 1, (1,)), (1, 0, (1,)), (2, 0, (1,)), (0, 1, 1), (1, 1),
        (2, 1), (0, 3, 0), (0, 3, 1), (3, 0, 3), (5, 0, 1, 0),
        (3, 0, 0), (5, 0, 1, 1), (1, 3), (3, 0, 2), (2, 3), (3, 0, 1),
        (3, 1, 3), (0, 2, 0), (0, 2, 1), (1, 2), (2, 2), (0, 4, 0),
        (5, 0, 2, 0), (3, 1, 0), (5, 0, 2, 1), (3, 1, 1), (0, 5, 0),
        (5, 1, 1, 1), (3, 1, 2), (0, 4, 1), (1, 4), (0, 6, 0), (2, 4),
        (0, 6, 1), (1, 6), (5, 1, 2, 1), (3, 3, 3), (0, 5, 1),
        (5, 1, 1, 0), (1, 5), (2, 5), (3, 3, 0), (3, 2, 0), (5, 2, 1, 1),
        (3, 2, 2), (3, 2, 3), (3, 4, 0), (2, 6), (5, 2, 1, 0),
        (5, 0, 3, 1), (3, 4, 3), (3, 4, 1), (3, 2, 1), (5, 4, 1, 0),
        (0, 7, 0), (5, 2, 2, 0), (3, 6, 3), (5, 4, 1, 1), (5, 1, 3, 1),
        (3, 5, 3), (5, 3, 1, 0), (3, 4, 2), (3, 3, 1), (0, 7, 1),
        (3, 5, 0), (3, 6, 0), (3, 5, 2), (8, 0), (5, 0, 3, 0),
        (8, 1), (5, 3, 1, 1), (1, 7), (2, 7), (5, 2, 2, 1),
        (5, 1, 2, 0), (8, 2), (4, 5, 3), (5, 3, 2, 1), (4, 6, 3),
        (3, 3, 2), (5, 1, 3, 0), (5, 4, 2, 1), (4, 5, 2), (3, 5, 1),
        (3, 7, 3), (3, 7, 0), (4, 6, 0), (5, 4, 2, 0), (5, 5, 1, 0),
        (4, 5, 0), (5, 5, 1, 1), (3, 7, 1), (8, 3), (3, 6, 1),
        (3, 7, 2), (4, 5, 1), (4, 7, 3), (5, 3, 2, 0), (5, 6, 1, 1),
        (3, 6, 2), (5, 2, 3, 1), (4, 7, 0), (5, 6, 1, 0), (8, 4),
        (5, 2, 3, 0), (6, 2), (6, 1), (5, 3, 3, 1), (5, 7, 1, 1),
        (5, 7, 1, 0), (5, 5, 2, 1), (4, 7, 1), (5, 5, 2, 0), (5, 4, 3, 1),
        (4, 6, 1), (5, 4, 3, 0), (6, 0), (4, 7, 2), (8, 5),
        (5, 6, 2, 1), (6, 4), (4, 6, 2), (5, 7, 2, 0), (5, 7, 2, 1),
        (5, 3, 3, 0), (6, 3), (5, 6, 2, 0), (5, 6, 3, 1), (5, 5, 3, 1),
        (8, 6), (8, 7), (5, 7, 3, 0), (7, 4), (7, 2), (7, 0),
        (5, 5, 3, 0), (7, 3), (7, 1), (5, 7, 3, 1), (7, 7), (7, 5),
        (5, 6, 3, 0), (7, 6),
    ),
}


def ordered(planes, kinds):
    early = kinds.count("zv")
    plan = ORDERS.get((planes, early, len(kinds) - early))
    if plan is None:
        return [action for _, action in sorted(schedule(planes, kinds), key=lambda e: e[0])]
    return [(STEPS[step[0]],) + step[1:] for step in plan]


def schedule(planes, kinds):
    compute, spacing, lag, sub = SCHEDULE["compute"], SCHEDULE["first"], SCHEDULE["start"], SCHEDULE["sub"]
    cus = len(kinds)
    events = [(-2.0, ("slant", 0, 0))]
    for l in range(2):
        for n, name in enumerate((("slant", 0, 1), ("stack", 0), ("start", 0))):
            events.append((-1.0 + 0.1 * n + 0.4 * l, name + ((l,),)))
    events.append((-0.3, ("slant", 1, 0)))
    for cu in range(1, cus):
        at = compute * cu
        if cu > 1:
            events.append((at, ("slant", cu, 0)))
        events.append((at + 0.1 * compute, ("slant", cu, 1)))
        events.append((at + 0.2 * compute, ("stack", cu)))
    done = compute * cus
    for stage in range(3 + planes + 1):
        events.append((done + SCHEDULE["moments"] * stage, ("moments", stage)))
    gain = done + SCHEDULE["moments"] * (3 + planes) + 0.1
    now = SCHEDULE["begin"]
    for cu, kind in enumerate(kinds):
        at = now
        if cu > 0:
            events.append((max(compute * cu + 0.3 * compute, at - lag), ("start", cu)))
        at = max(at, compute * cu + 0.3 * compute + 0.1)
        for i, t in enumerate(far_first(planes)):
            events.append((at + i * sub, ("first", cu, t)))
        now += spacing[kind]
        at += (planes - 1) * sub
        if kind == "vz":
            at += SCHEDULE["second"] - (planes - 1) * sub
            for i, t in enumerate(far_first(planes)):
                events.append((at + i * sub, ("second", cu, t)))
            at += (planes - 1) * sub
        for tau in range(1, planes):
            at += SCHEDULE["hop"][kind]
            for way in range(2):
                events.append((at, ("tick", cu, tau, way)))
        if kind == "zv":
            at += SCHEDULE["third"]
            events.append((at, ("third", cu)))
            at += SCHEDULE["finish"]
        events.append((max(at + 0.01, gain), ("finish", cu)))
    return events


def fused(shapes, offsets, slant_weights, live, block_tile, image_slot):
    planes, grp, scratch, kinds = shapes
    blocks = block_tile.shape[0]
    hs, depth = offsets.shape[1:]
    angles = slant_weights.shape[0]
    any_space = pl.BlockSpec(memory_space=pl.ANY)
    return pl.pallas_call(
        functools.partial(fused_kernel, (planes, grp, kinds)),
        out_shape=pltpu.VMEM((IMG_DEV, 2 * angles, depth), jnp.bfloat16),
        in_specs=[any_space] * 5,
        out_specs=pl.BlockSpec(memory_space=pltpu.VMEM),
        scratch_shapes=scratch,
        compiler_params=pltpu.CompilerParams(
            collective_id=2, has_side_effects=True, vmem_limit_bytes=VMEM_LIMIT
        ),
        name="calibrated_stack",
    )(
        offsets.reshape(blocks, 2, hs, depth),
        live.T,
        block_tile.reshape(1, blocks),
        image_slot.reshape(1, blocks),
        slant_weights.T,
    )


def buffers(planes, blocks, hs, depth, angles, images):
    wide, per = 2 * LANES, 16
    cus = (depth // wide) * (angles // per)
    pieces = 2 * cus
    tile = (per // 2, 16, LANES)
    dma = pltpu.SemaphoreType.DMA
    bf, f32, i32 = jnp.bfloat16, jnp.float32, jnp.int32
    early = (5 * cus + 4) // 8
    kinds = ("zv",) * early + ("vz",) * (cus - early)
    memory = [
        ((angles, 2 * blocks), i32),
        ((1, blocks), i32),
        ((1, blocks), i32),
        ((hs, angles), bf),
        ((2, blocks, hs, depth), bf),
        ((angles * 8, 8 * hs), bf),
        ((images, 2 * blocks), bf),
        ((8 + blocks, LANES), i32),
        ((8 + blocks, LANES), i32),
        ((2, blocks, LANES), i32),
        ((angles, 8, LANES), f32),
        ((2, per, 2 * blocks, wide), bf),
        ((pieces, planes, 2) + tile, f32),
        ((pieces, planes, 2) + tile, bf),
        ((pieces, planes, 2) + tile, bf),
        ((pieces, planes) + tile, bf),
        ((pieces, 2, planes - 1, 2) + tile, bf),
        ((2, per * 8, LANES), f32),
        ((IMG_DEV, angles, depth), bf),
        ((7, 8, LANES), f32),
        ((5, 8, LANES), f32),
        ((angles, LANES), f32),
    ]
    size = sum(math.prod(s) * jnp.dtype(d).itemsize for s, d in memory)
    scratch = [pltpu.VMEM(s, d) for s, d in memory]
    depths = depth // wide
    scratch += [
        dma((4,)), dma((depths,)), dma((depths + 1,)), dma((depths + 1,)), dma((1,)), dma((1,)),
        dma((1,)), dma((cus, planes)),
        dma((2,)), dma((early + (cus - early) * planes,)),
        dma((2, 2, planes - 1)), dma((early + 2 * (cus - early), 2, planes - 1)),
        dma((1,)), dma((1,)), dma((5,)), dma((5,)),
    ]
    return size, scratch, kinds


def local(offsets, slant_weights, live, block_tile, image_slot):
    shots, grp = lax.axis_size("shot"), lax.axis_size("grp")
    planes = shots // PAIR
    blocks = block_tile.shape[0]
    hs, depth = offsets.shape[1:]
    angles = slant_weights.shape[0]
    images = shots * IMG_DEV * grp
    size, scratch, kinds = buffers(planes, blocks, hs, depth, angles, images)
    args = (offsets, slant_weights, live, block_tile, image_slot)
    if grp == 4 and size + (2 << 20) <= VMEM_LIMIT:
        return fused((planes, grp, scratch, kinds), *args)
    return staged(*args)


def solution(mesh):
    placed = (
        P(("shot", "grp"), None, None),
        P(),
        P(("shot", "grp"), None),
        P(("shot", "grp"), None),
        P(("shot", "grp")),
    )
    return jax.shard_map(
        local, mesh=mesh, in_specs=placed, out_specs=P(("shot", "grp"), None, None), check_vma=False
    )
```
